512 devices in a mesh: chain: 64 (over x, z, core), rep: 8 (over y).
Axes of the slice: x: 4, y: 8, z: 8, core: 2. Of those that a mesh axis runs over, the one named last changes fastest.
Arguments:
- spins: bfloat16 [98304, 256], P('chain'), may hold values from -1 to 1, as said below
- energies: bfloat16 [98304], P('chain'), may hold values from -150 to -70
- counts: int32 [64], P('chain'), may hold values from 1 to 1536, 49152 in all
- accepted: int32 [64, 1536], P('chain'), may hold values from 0 to 1535, each once within a row
- hidden_bias: bfloat16 [4096], P('rep'), may hold values from -3 to 3
- weights: bfloat16 [256, 4096], P(None, 'rep'), may hold values from -0.375 to 0.375
Outputs:
- update_visible: float32 [256], P('rep')
- update_hidden: float32 [4096], P('rep')
- update_weights: float32 [256, 4096], P('chain', 'rep')
The draws below stay inside these ranges and needn't reach their ends.
Inputs may be any that keep to these rules, and one draw needn't show every extreme that they name: `spins`: every entry is -1 or 1. The counts sum to 49152; at least one index of chain has 1536. Each row is a permutation of the slot numbers; its first counts entries name that index's accepted slots.
All inputs are finite; a program needn't handle non-finite values. No bound on the sum of `counts` on one device may be relied on, other than what follows from the above.
Results may differ from the reference program's by a relative error of at most 0.02.
Values may be sent and summed in bfloat16 or wider, within the bound.
No kernel may reach another device: no remote copies, remote signals or barrier semaphores. Data moves between devices by JAX's collectives and lax.ppermute only.
A program may use at most 64 MiB of HBM per device.

```python
import math
import jax
import jax.numpy as jnp
import numpy as np
from jax import lax

N_SITES = 256
HIDDEN_SIZE = 4096
KEEP_DEV = 768
ITERS = 3
SLOTS_DEV = 1536
SLOTS_ALL = 98304
TOTAL = 49152
N_CHAIN = 64


def draw_spins(key, part):
    coin_flips = jax.random.randint(key, (SLOTS_ALL, N_SITES), 0, 2)
    return (2 * coin_flips - 1).astype(jnp.bfloat16)


def steps_of(stream_key, extent, split, smallest, largest):
    def one(dim, parts):
        steps = jax.random.uniform(jax.random.fold_in(jax.random.fold_in(stream_key, 6), dim), (parts,), jnp.float32, smallest / len(split), largest / len(split))
        return jnp.repeat(jnp.exp(steps), extent[dim] // parts).reshape((-1,) + (1,) * (len(extent) - dim - 1))

    level = one(*split[0])
    for cut in split[1:]:
        level = level * one(*cut)
    return level


def length_profile(amount, total, bound, slope):
    loads = [(1 << 20) // math.isqrt(grade ** slope) + 1 for grade in range(2, amount + 1)]
    rest, holding = total - bound - (amount - 1), [1] * (amount - 1)
    while rest > 0:
        movable = [i for i in range(amount - 1) if holding[i] < bound]
        whole, remaining = sum([loads[i] for i in movable]), rest
        for i in movable:
            more = min(bound - holding[i], max(1, remaining * loads[i] // whole), rest)
            holding[i] = holding[i] + more
            rest = rest - more
    return np.array([bound] + holding)


def uneven(stream_key, number_of, total, bound, skew):
    if number_of == 2:
        one = jax.random.randint(stream_key, (), max(1, total - bound), min(bound, total - 1) + 1)
        return jnp.stack([one, total - one])
    lengths = jnp.asarray(length_profile(number_of, total, bound, skew), jnp.int32)
    pairs = (number_of - 1) // 2
    giver, sink = lengths[1:1 + 2 * pairs:2], lengths[2:2 + 2 * pairs:2]
    room = jnp.minimum(giver - 1, bound - sink)
    passed = jax.random.randint(jax.random.fold_in(stream_key, 1), (pairs,), 0, 1 << 20) % (room + 1)
    lengths = lengths.at[1:1 + 2 * pairs:2].set(giver - passed).at[2:2 + 2 * pairs:2].set(sink + passed)
    return lengths[jax.random.permutation(jax.random.fold_in(stream_key, 2), number_of)]


def bell_draw(key, shape, deviation, most, cuts=(), held_as=jnp.bfloat16):
    gain = steps_of(key, shape, cuts, -0.22, 0.18) if cuts else 1.0
    entries = jax.random.normal(key, shape, jnp.float32) * deviation * gain
    return jnp.minimum(jnp.maximum(entries, -most), most).astype(held_as)


def setup_inputs(seed: int = 0) -> dict:
    keys = jax.random.split(jax.random.key(seed), 7)
    return {
        "spins": draw_spins(jax.random.fold_in(keys[6], 71), 0),
        "energies": jnp.clip(-150.0 + 80.0 * jax.random.uniform(keys[1], (SLOTS_ALL,), jnp.float32) ** steps_of(keys[1], (SLOTS_ALL,), ((0, 64),), -0.2, 0.2), -150.0, -70.0).astype(jnp.bfloat16),
        "counts": uneven(keys[2], N_CHAIN, TOTAL, SLOTS_DEV, 2).astype(jnp.int32),
        "accepted": jax.vmap(lambda own: jax.random.permutation(own, SLOTS_DEV))(jax.random.split(keys[3], N_CHAIN)).reshape((N_CHAIN, SLOTS_DEV)).astype(jnp.int32),
        "hidden_bias": bell_draw(keys[4], (HIDDEN_SIZE,), 0.5, 3.0, ((0, 8),)),
        "weights": bell_draw(keys[5], (N_SITES, HIDDEN_SIZE), N_SITES ** -0.5, 0.375, ((1, 8),)),
    }


PRECISE = lax.Precision.HIGHEST
DIAG_SHIFT = 0.05
EPSILON = 1e-06

def activations(block_spins, hidden_bias, weights):
    preact = hidden_bias.astype(jnp.float32) + jnp.dot(block_spins, weights, preferred_element_type=jnp.float32)
    return jnp.tanh(preact).astype(jnp.bfloat16)

def combine(base_vec, extra_vec, factor):
    return tuple((first + factor * second for first, second in zip(base_vec, extra_vec)))

def inner(first_vec, second_vec):
    return jnp.sum(first_vec[0] * second_vec[0]) + jnp.sum(first_vec[1] * second_vec[1]) + jnp.sum(first_vec[2] * second_vec[2])

def reference(spins, energies, counts, accepted, hidden_bias, weights):
    sample_total = KEEP_DEV * N_CHAIN
    counts = counts.astype(jnp.int32)
    offsets = (jnp.cumsum(counts) - counts).astype(jnp.int32)
    global_rows = jnp.arange(sample_total, dtype=jnp.int32)
    owner_chain = (lax.optimization_barrier(jnp.sum((offsets[None, :] <= global_rows[:, None]).astype(jnp.int32), axis=1)) - 1).astype(jnp.int32)
    within = global_rows - offsets[owner_chain]
    local_slot = accepted[owner_chain, within].astype(jnp.int32)
    source_slot = owner_chain * SLOTS_DEV + local_slot
    samples = spins[source_slot]
    energy = energies[source_slot].astype(jnp.float32)
    centered = energy - jnp.mean(energy)
    block_rows = math.gcd(sample_total, 512)
    block_count = sample_total // block_rows
    blocks = samples.reshape(block_count, block_rows, N_SITES)

    def pull(row_weight):
        weight_blocks = row_weight.reshape(block_count, block_rows)

        def block_sums(running, block_item):
            block_spins, weight_rows = block_item
            hidden_acts = activations(block_spins, hidden_bias, weights).astype(jnp.float32)
            spins_float = block_spins.astype(jnp.float32)
            weighted = hidden_acts * weight_rows[:, None]
            grad_vis = jnp.dot(weight_rows, spins_float, precision=PRECISE)
            grad_hid = lax.optimization_barrier(jnp.sum(weighted, axis=0))
            grad_mat = jnp.dot(spins_float.T, weighted, precision=PRECISE)
            return ((running[0] + grad_vis, running[1] + grad_hid, running[2] + grad_mat), None)
        initial = (jnp.zeros((N_SITES,), jnp.float32), jnp.zeros((HIDDEN_SIZE,), jnp.float32), jnp.zeros((N_SITES, HIDDEN_SIZE), jnp.float32))
        results, unused = lax.scan(block_sums, initial, (blocks, weight_blocks))
        return tuple((member / sample_total for member in results))

    def forward(vector):
        vis_part, hid_part, mat_part = vector

        def block_values(running, block_spins):
            hidden_acts = activations(block_spins, hidden_bias, weights).astype(jnp.float32)
            spins_float = block_spins.astype(jnp.float32)
            mixture = jnp.dot(spins_float, mat_part, precision=PRECISE)
            values = lax.optimization_barrier(jnp.sum(mixture * hidden_acts, axis=1)) + jnp.dot(hidden_acts, hid_part, precision=PRECISE) + jnp.dot(spins_float, vis_part, precision=PRECISE)
            return (running, values)
        unused, results = lax.scan(block_values, jnp.zeros((), jnp.float32), blocks)
        row_values = results.reshape(sample_total)
        return row_values - jnp.mean(row_values)
    force = pull(centered)
    solution = tuple((jnp.zeros_like(member) for member in force))
    residual = force
    direction = force
    resid_sq = inner(residual, residual)
    for iteration in range(ITERS):
        image = combine(pull(forward(direction)), direction, DIAG_SHIFT)
        step_size = resid_sq / inner(direction, image)
        solution = combine(solution, direction, step_size)
        residual = combine(residual, image, -step_size)
        if iteration + 1 < ITERS:
            resid_next = inner(residual, residual)
            direction = combine(residual, direction, resid_next / resid_sq)
            resid_sq = resid_next
    param_total = N_SITES * HIDDEN_SIZE + HIDDEN_SIZE + N_SITES
    scale = 1.0 / jnp.sqrt(inner(solution, solution) / param_total + EPSILON)
    return (solution[0] * scale, solution[1] * scale, solution[2] * scale)
```

```python
import jax
import jax.numpy as jnp
from jax import lax
from jax.experimental import pallas as pl
from jax.experimental.pallas import tpu as pltpu
from jax.sharding import Mesh
from jax.sharding import PartitionSpec as P

KEEP_DEV = 768
SHIFT = 0.05
EPSILON = 1e-06
ENERGY_MID = -110.0
CHAIN = ("chain_0", "chain_1", "chain_2")
F32 = jnp.float32
BF16 = jnp.bfloat16
HIGH = lax.Precision.HIGHEST

SITES = 256
HIDDEN = 512
OWNERS = 64
ROWS = 4
TAIL = 128
WIDE = HIDDEN + TAIL
SLOTS = 1536
TOTAL = float(KEEP_DEV * OWNERS)
SCALARS = 8


def iota(shape, dim):
    return lax.broadcasted_iota(jnp.int32, shape, dim)


def dot(a, b, dims=((1,), (0,)), precision=None):
    return lax.dot_general(a, b, (dims, ((), ())), precision=precision, preferred_element_type=F32)


def by_lanes(a, b):
    return dot(a, b, ((1,), (1,)))


def eye(n):
    return jnp.where(iota((n, n), 0) == iota((n, n), 1), 1.0, 0.0).astype(BF16)


def two(x):
    high = x.astype(BF16)
    return high, (x - high.astype(F32)).astype(BF16)


def total(x):
    return jnp.sum(x, keepdims=True)


def scalar_lanes(scalars):
    lane = iota((1, TAIL), 1)
    out = jnp.zeros((1, TAIL), F32)
    for i, value in enumerate(scalars):
        one = value.astype(BF16).astype(F32)
        second = (value - one).astype(BF16).astype(F32)
        third = value - one - second
        for k, piece in enumerate((one, second, third)):
            out = jnp.where(lane == 32 + 3 * i + k, piece, out)
    return out


def own_hidden(shape):
    row, col = iota(shape, 0), iota(shape, 1)
    return row == ROWS * (col >> 3)


def pull(weights, st, tt):
    high, low = two(weights)
    spins = st.astype(F32)
    grad = by_lanes((spins * high.astype(F32)).astype(BF16), tt)
    grad = grad + by_lanes((spins * low.astype(F32)).astype(BF16), tt)
    sub = iota((16, SLOTS), 0)
    pair = jnp.where(sub == 0, high.astype(F32), jnp.where(sub == 1, low.astype(F32), 0.0)).astype(BF16)
    both = by_lanes(pair, tt)
    return grad, both[0:1, :] + both[1:2, :]


def tail_of(grad, hidden, scalars):
    visible = grad[:, HIDDEN : HIDDEN + 1]
    v_high = visible.astype(BF16).astype(F32)
    lane, row = iota((SITES, TAIL), 1), iota((SITES, TAIL), 0)
    tail = jnp.where(lane == 0, v_high, jnp.where(lane == 1, visible - v_high, 0.0))
    h_high, h_low = two(hidden[:, :HIDDEN])
    mine = own_hidden((SITES, HIDDEN))
    j, l = iota((HIDDEN, TAIL), 0) & 7, iota((HIDDEN, TAIL), 1)
    for piece, base in ((h_high, 8), (h_low, 16)):
        spread = jnp.where(mine, piece.astype(F32), 0.0).astype(BF16)
        tail = tail + dot(spread, jnp.where(l == base + j, 1.0, 0.0).astype(BF16))
    return tail + jnp.where((row & 3) == 1, scalar_lanes(scalars), 0.0)


def store_rows(out_ref, first, grad, tail):
    for c in range(OWNERS):
        rows = slice(ROWS * c, ROWS * (c + 1))
        out_ref[c, first : first + ROWS, 0:HIDDEN] = grad[rows, 0:HIDDEN].astype(BF16)
        out_ref[c, first : first + ROWS, HIDDEN:WIDE] = tail[rows, :].astype(BF16)


def combined(tail):
    a, b = iota((TAIL, TAIL), 0), iota((TAIL, TAIL), 1)
    take = (b == 0) & (a < 2)
    take = take | ((b >= 8) & (b < 16) & ((a == b) | (a == b + 8)))
    first = 32 + 3 * (b - 64)
    take = take | ((b >= 64) & (b < 64 + SCALARS) & (a >= first) & (a < first + 3))
    return dot(tail, jnp.where(take, 1.0, 0.0).astype(F32), precision=HIGH)


def store_copies(out_ref, rows):
    lane = iota((ROWS, TAIL), 1)
    tail = rows[:, HIDDEN:WIDE]
    tail = jnp.where(lane == 0, tail * 0.125, jnp.where((lane >= 8) & (lane < 16), tail, 0.0))
    high = tail.astype(BF16).astype(F32)
    a, b = iota((TAIL, TAIL), 0), iota((TAIL, TAIL), 1)
    move = ((a == 0) & (b == 1)) | ((a >= 8) & (a < 16) & (b == a + 8))
    low = dot(tail - high, jnp.where(move, 1.0, 0.0).astype(F32), precision=HIGH)
    packed = (high + low).astype(BF16)
    coupling = rows[:, 0:HIDDEN].astype(BF16)
    for c in range(OWNERS):
        out_ref[c, :, 0:HIDDEN] = coupling
        out_ref[c, :, HIDDEN:WIDE] = packed


def setup_kernel(count_ref, spins_ref, energy_ref, accepted_ref, weights_ref, bias_ref, st_ref, tt_ref, vec_ref, out_ref):
    accepted = accepted_ref[...]
    live = iota((16, SLOTS), 1) < count_ref[0]
    major = jnp.where((iota((16, SLOTS), 0) == (accepted >> 7)) & live, 1.0, 0.0).astype(BF16)
    minor = jnp.where(iota((TAIL, SLOTS), 0) == (accepted & 127), 1.0, 0.0).astype(BF16)
    table = by_lanes(major, minor)
    mask = jnp.concatenate([table[h : h + 1, :] for h in range(SLOTS // TAIL)], axis=1)
    spins = spins_ref[...]
    st_ref[...] = by_lanes(eye(SITES), spins).astype(BF16)
    turned = by_lanes(eye(HIDDEN), weights_ref[...]).astype(BF16)
    bias = by_lanes(eye(HIDDEN), jnp.broadcast_to(bias_ref[...].astype(F32), (16, HIDDEN)).astype(BF16))
    preact = bias[:, 0:1] + dot(turned, st_ref[...])
    tt_ref[0:HIDDEN, :] = jnp.tanh(preact).astype(BF16)
    sub = iota((TAIL, SLOTS), 0)
    tt_ref[HIDDEN:WIDE, :] = jnp.where(sub < 2, 1.0, 0.0).astype(BF16)
    energy = (energy_ref[...].astype(F32) - ENERGY_MID) * mask
    vec_ref[0:1, :] = mask
    vec_ref[1:2, :] = energy
    vec_ref[2:8, :] = jnp.zeros((6, SLOTS), F32)
    st, tt = st_ref[...], tt_ref[...]
    for first, row, scalars in ((0, energy, (total(energy),)), (ROWS, mask, ())):
        grad, hidden = pull(row, st, tt)
        store_rows(out_ref, first, grad, tail_of(grad, hidden, scalars))


def arrived(in_ref, first):
    rows = slice(first, first + ROWS)
    acc = [in_ref[c, rows, :].astype(F32) for c in range(4)]
    for c in range(4, OWNERS):
        acc[c % 4] = acc[c % 4] + in_ref[c, rows, :].astype(F32)
    acc = (acc[0] + acc[1]) + (acc[2] + acc[3])
    tail = combined(acc[:, HIDDEN:WIDE])
    scalars = [tail[1:2, 64 + i : 65 + i] for i in range(SCALARS)]
    return acc[:, 0:HIDDEN], tail, scalars


def lanes_of(values):
    lane = iota((8, TAIL), 1)
    out = jnp.zeros((8, TAIL), F32)
    for i, value in enumerate(values):
        out = jnp.where(lane == i, value, out)
    return out


def first_own_kernel(in_ref, vec_ref, res_ref, ones_ref, vec_out_ref, copies_ref):
    energy, energy_tail, scalars = arrived(in_ref, 0)
    ones, ones_tail, _ = arrived(in_ref, ROWS)
    mean = scalars[0] / TOTAL
    res_ref[:, 0:HIDDEN] = energy - mean * ones
    res_ref[:, HIDDEN:WIDE] = energy_tail - mean * ones_tail
    ones_ref[:, 0:HIDDEN] = ones
    ones_ref[:, HIDDEN:WIDE] = ones_tail
    mask, raw = vec_ref[0:1, :], vec_ref[1:2, :]
    vec_out_ref[0:1, :] = mask
    vec_out_ref[1:2, :] = raw - mean * mask
    vec_out_ref[2:8, :] = jnp.zeros((6, SLOTS), F32)
    store_copies(copies_ref, res_ref[...])


def push_kernel(in_ref, st_ref, tt_ref, parts_ref, bias_ref, rows_ref):
    for c in range(OWNERS):
        rows_ref[ROWS * c : ROWS * (c + 1), :] = in_ref[c].astype(F32)
    tail = rows_ref[:, HIDDEN:WIDE].astype(BF16)
    mine = own_hidden((SITES, HIDDEN))
    l, j = iota((TAIL, HIDDEN), 0), iota((TAIL, HIDDEN), 1) & 7
    spread = dot(tail, jnp.where((l == 8 + j) | (l == 16 + j), 1.0, 0.0).astype(BF16))
    hidden = jnp.sum(jnp.where(mine, spread, 0.0), axis=0, keepdims=True)
    pick = jnp.where((iota((16, TAIL), 0) == 0) & (iota((16, TAIL), 1) < 2), 8.0, 0.0).astype(BF16)
    visible = by_lanes(pick, tail)
    bias_ref[...] = jnp.zeros((8, HIDDEN), F32)
    bias_ref[0:1, :] = hidden
    bias_ref[1:2, 0:SITES] = visible[0:1, :]
    h_high, h_low = two(hidden)
    sub = iota((16, HIDDEN), 0)
    pair = jnp.where(sub == 0, h_high.astype(F32), jnp.where(sub == 1, h_low.astype(F32), 0.0)).astype(BF16)
    tt = tt_ref[...]
    side = dot(pair, tt[0:HIDDEN, :])
    turned = jnp.transpose(rows_ref[...]).astype(BF16)
    mixture = dot(turned, st_ref[...])
    values = jnp.sum(mixture * tt.astype(F32), axis=0, keepdims=True)
    values = (values + side[0:1, :] + side[1:2, :]) * (1.0 / TOTAL)
    for y in range(parts_ref.shape[0]):
        parts_ref[y] = values


def row_sum(parts_ref, mask):
    values = parts_ref[0]
    for y in range(1, parts_ref.shape[0]):
        values = values + parts_ref[y]
    return values * mask


def iteration_scalars(vec_ref, values):
    res, before, o_before, start = (vec_ref[i : i + 1, :] for i in (1, 2, 3, 4))
    return (
        total(res * values),
        total(values * values),
        total(values),
        total(values * o_before),
        total(values * before),
        total(res * o_before),
        total(values * start),
    )


def pull_kernel(parts_ref, vec_ref, st_ref, tt_ref, vec_out_ref, out_ref):
    values = row_sum(parts_ref, vec_ref[0:1, :])
    vec_out_ref[...] = vec_ref[...]
    vec_out_ref[5:6, :] = values
    grad, hidden = pull(values, st_ref[...], tt_ref[...])
    store_rows(out_ref, 0, grad, tail_of(grad, hidden, iteration_scalars(vec_ref, values)))


def conjugate(scalars, past):
    r_zr, zr_zr, zr_sum, zr_zd, zr_d, r_zd, zr_start = scalars[:7]
    if past is None:
        beta, zd_sum, zd_zd, zd_d = None, zr_sum, zr_zr, r_zr
    else:
        rr, sum_before, zz_before, zd_before = past
        beta = r_zr / rr
        zd_sum = zr_sum + beta * sum_before
        zd_zd = zr_zr + 2.0 * beta * zr_zd + beta * beta * zz_before
        zd_d = r_zr + beta * (zr_d + r_zd) + beta * beta * zd_before
    step = r_zr / (zd_zd - zd_sum * zd_sum / TOTAL + SHIFT * zd_d)
    return beta, step, (r_zr, zd_sum, zd_zd, zd_d)


def own_kernel(first, *refs):
    if first:
        in_ref, vec_ref, res_ref, ones_ref, sc_out, vec_out, res_out, dir_out, img_out, copies_ref = refs
    else:
        (in_ref, vec_ref, res_ref, ones_ref, sc_ref, dir_ref, img_ref,
         sc_out, vec_out, res_out, dir_out, img_out, copies_ref) = refs
    grad, tail, scalars = arrived(in_ref, 0)
    past = None if first else tuple(sc_ref[0:1, i : i + 1] for i in range(4))
    beta, step, now = conjugate(scalars, past)
    mean = scalars[2] / TOTAL
    zd_mean = now[1] / TOTAL
    if first:
        kept = (step, now[3])
    else:
        d0_zd1 = scalars[6] + beta * sc_ref[0:1, 5:6]
        kept = (sc_ref[0:1, 4:5], sc_ref[0:1, 5:6], step, now[3], d0_zd1, beta)
    sc_out[...] = lanes_of(now + kept)
    for part, new in ((slice(0, HIDDEN), grad), (slice(HIDDEN, WIDE), tail)):
        image, direction = new - mean * ones_ref[:, part], res_ref[:, part]
        if not first:
            image = image + beta * img_ref[:, part]
            direction = direction + beta * dir_ref[:, part]
        img_out[:, part] = image
        dir_out[:, part] = direction
        res_out[:, part] = res_ref[:, part] - step * (image + SHIFT * direction)
    mask, res, o_res = vec_ref[0:1, :], vec_ref[1:2, :], vec_ref[5:6, :]
    direction, o_dir = res, o_res
    if not first:
        direction = direction + beta * vec_ref[2:3, :]
        o_dir = o_dir + beta * vec_ref[3:4, :]
    vec_out[0:1, :] = mask
    vec_out[1:2, :] = res - step * (o_dir - zd_mean * mask + SHIFT * direction)
    vec_out[2:3, :] = direction
    vec_out[3:4, :] = o_dir
    vec_out[4:5, :] = direction if first else vec_ref[4:5, :]
    vec_out[5:8, :] = jnp.zeros((3, SLOTS), F32)
    store_copies(copies_ref, res_out[...])


def last_scalars_kernel(parts_ref, vec_ref, out_ref):
    values = row_sum(parts_ref, vec_ref[0:1, :])
    lane = iota((OWNERS, TAIL), 1)
    out = jnp.zeros((OWNERS, TAIL), F32)
    for i, value in enumerate(iteration_scalars(vec_ref, values)):
        out = jnp.where(lane == i, value, out)
    out_ref[...] = out


def last_kernel(rep_ref, in_ref, sc_ref, dir0_ref, dir1_ref, res2_ref, b0_ref, b1_ref, b2_ref, vis_ref, hid_ref, mat_ref):
    summed = jnp.sum(in_ref[...], axis=0, keepdims=True)
    scalars = [summed[:, i : i + 1] for i in range(SCALARS)]
    keep = [sc_ref[0:1, i : i + 1] for i in range(9)]
    beta2, step2, now = conjugate(scalars, tuple(keep[0:4]))
    step0, d0_zd0, step1, d1_zd1, d0_zd1 = keep[4:9]
    d0_zd2 = scalars[6] + beta2 * d0_zd1
    d1_zd2 = scalars[4] + beta2 * d1_zd1
    norm = step0 * step0 * d0_zd0 + step1 * step1 * d1_zd1 + step2 * step2 * now[3]
    norm = norm + 2.0 * (step0 * step1 * d0_zd1 + step0 * step2 * d0_zd2 + step1 * step2 * d1_zd2)
    params = float(SITES * HIDDEN * 8 + HIDDEN * 8 + SITES)
    scale = lax.rsqrt(norm / (TOTAL * params) + EPSILON) / TOTAL
    beta1 = sc_ref[0:1, 9:10]
    w0, w1, w2 = scale * step0, scale * (step1 + step2 * beta2), scale * step2
    mat_ref[...] = w0 * dir0_ref[:, 0:HIDDEN] + w1 * dir1_ref[:, 0:HIDDEN] + w2 * res2_ref[:, 0:HIDDEN]
    small = (w0 + w1 * beta1) * b0_ref[...] + w1 * b1_ref[...] + w2 * b2_ref[...]
    hid_ref[...] = small
    a, b = iota((SITES, TAIL), 0), iota((SITES, TAIL), 1)
    pick = jnp.where(a == 32 * rep_ref[0] + b, 1.0, 0.0).astype(F32)
    vis_ref[...] = dot(small[:, 0:SITES], pick, precision=HIGH)


def shape(dims, dtype=F32):
    return jax.ShapeDtypeStruct(dims, dtype)


def call(kernel, outs, name, n_in, smem=(), scratch=()):
    vmem = pl.BlockSpec(memory_space=pltpu.VMEM)
    scalar = pl.BlockSpec(memory_space=pltpu.SMEM)
    return pl.pallas_call(
        kernel,
        out_shape=outs,
        in_specs=[scalar if i in smem else vmem for i in range(n_in)],
        out_specs=[vmem] * len(outs),
        scratch_shapes=list(scratch),
        name=name,
    )


def over_chain(blocks):
    return lax.all_to_all(blocks, CHAIN, split_axis=0, concat_axis=0, tiled=True)


def per_device(spins, energies, counts, accepted, hidden_bias, weights):
    reps = lax.axis_size("rep")
    rows = shape((OWNERS, ROWS, WIDE), BF16)
    own = shape((ROWS, WIDE))
    vec_shape = shape((8, SLOTS))
    st, tt, vec, blocks = call(
        setup_kernel,
        [shape((SITES, SLOTS), BF16), shape((WIDE, SLOTS), BF16), vec_shape, shape((OWNERS, 2 * ROWS, WIDE), BF16)],
        "setup", 6, smem=(0,),
    )(counts, spins, energies[None, :], accepted, weights, hidden_bias[None, :])
    res, ones, vec, copies = call(first_own_kernel, [own, own, vec_shape, rows], "first_own", 2)(over_chain(blocks), vec)

    def push(copies):
        parts, small = call(
            push_kernel, [shape((reps, 1, SLOTS)), shape((8, HIDDEN))], "push", 3,
            scratch=[pltpu.VMEM((SITES, WIDE), F32)],
        )(over_chain(copies), st, tt)
        return lax.all_to_all(parts, "rep", split_axis=0, concat_axis=0, tiled=True), small

    state, smalls, directions = (), [], []
    for iteration in range(2):
        parts, small = push(copies)
        vec, blocks = call(pull_kernel, [vec_shape, rows], "pull", 4)(parts, vec, st, tt)
        sc, vec, res, direction, image, copies = call(
            lambda *refs, first=iteration == 0: own_kernel(first, *refs),
            [shape((8, TAIL)), vec_shape, own, own, own, rows], "own", 4 + len(state),
        )(over_chain(blocks), vec, res, ones, *state)
        state = (sc, direction, image)
        smalls.append(small)
        directions.append(direction)
    parts, small = push(copies)
    smalls.append(small)
    (sums,) = call(last_scalars_kernel, [shape((OWNERS, TAIL))], "last_scalars", 2)(parts, vec)
    vis, hid, mat = call(
        last_kernel, [shape((8, TAIL)), shape((8, HIDDEN)), shape((ROWS, HIDDEN))], "last", 9, smem=(0,)
    )(lax.axis_index("rep")[None].astype(jnp.int32), over_chain(sums), sc, *directions, res, *smalls)
    return vis[1, :32], hid[0], mat


def solution(mesh):
    split = Mesh(
        mesh.devices.reshape(4, 8, 2, mesh.shape["rep"]), ("chain_0", "chain_1", "chain_2", "rep")
    )
    in_specs = (P(CHAIN, None), P(CHAIN), P(CHAIN), P(CHAIN, None), P("rep"), P(None, "rep"))
    out_specs = (P("rep"), P("rep"), P(CHAIN, "rep"))
    return jax.shard_map(
        per_device, mesh=split, in_specs=in_specs, out_specs=out_specs, check_vma=False
    )
```

```python
import jax
import jax.numpy as jnp
from jax import lax
from jax.experimental import pallas as pl
from jax.experimental.pallas import tpu as pltpu
from jax.sharding import Mesh
from jax.sharding import PartitionSpec as P

KEEP_DEV = 768
SHIFT = 0.05
EPSILON = 1e-06
ENERGY_MID = -110.0
CHAIN = ("chain_0", "chain_1", "chain_2")
F32 = jnp.float32
BF16 = jnp.bfloat16
HIGH = lax.Precision.HIGHEST

SITES = 256
HIDDEN = 512
OWNERS = 64
ROWS = 4
TAIL = 128
WIDE = HIDDEN + TAIL
SLOTS = 1536
TOTAL = float(KEEP_DEV * OWNERS)
SCALARS = 8
VMEM_LIMIT = 24 * 2**20


def iota(shape, dim):
    return lax.broadcasted_iota(jnp.int32, shape, dim)


def dot(a, b, dims=((1,), (0,)), precision=None):
    return lax.dot_general(a, b, (dims, ((), ())), precision=precision, preferred_element_type=F32)


def by_lanes(a, b):
    return dot(a, b, ((1,), (1,)))


def eye(n):
    return jnp.where(iota((n, n), 0) == iota((n, n), 1), 1.0, 0.0).astype(BF16)


def two(x):
    high = x.astype(BF16)
    return high, (x - high.astype(F32)).astype(BF16)


def total(x):
    return jnp.sum(x, keepdims=True)


def scalar_lanes(scalars):
    lane = iota((1, TAIL), 1)
    out = jnp.zeros((1, TAIL), F32)
    for i, value in enumerate(scalars):
        one = value.astype(BF16).astype(F32)
        second = (value - one).astype(BF16).astype(F32)
        third = value - one - second
        for k, piece in enumerate((one, second, third)):
            out = jnp.where(lane == 32 + 3 * i + k, piece, out)
    return out


def own_hidden(shape):
    row, col = iota(shape, 0), iota(shape, 1)
    return row == ROWS * (col >> 3)


def row_pair(high, low):
    sub = iota((16, high.shape[1]), 0)
    return jnp.where(sub == 0, high.astype(F32), jnp.where(sub == 1, low.astype(F32), 0.0)).astype(BF16)


def pull(weights, st, tt):
    high, low = two(weights)
    spins = st.astype(F32)
    visible = jnp.sum(spins * weights, axis=1, keepdims=True)
    both = jnp.concatenate([(spins * high.astype(F32)).astype(BF16), (spins * low.astype(F32)).astype(BF16)], axis=0)
    grad = by_lanes(both, tt)
    hidden = by_lanes(row_pair(high, low), tt)
    return grad[:SITES] + grad[SITES:], visible, hidden[0:1, :] + hidden[1:2, :]


def tail_of(visible, hidden, scalars):
    v_high = visible.astype(BF16).astype(F32)
    lane, row = iota((SITES, TAIL), 1), iota((SITES, TAIL), 0)
    tail = jnp.where(lane == 0, v_high, jnp.where(lane == 1, visible - v_high, 0.0))
    h_high, h_low = two(hidden)
    mine = own_hidden((SITES, HIDDEN))
    j, l = iota((HIDDEN, TAIL), 0) & 7, iota((HIDDEN, TAIL), 1)
    for piece, base in ((h_high, 8), (h_low, 16)):
        spread = jnp.where(mine, piece.astype(F32), 0.0).astype(BF16)
        tail = tail + dot(spread, jnp.where(l == base + j, 1.0, 0.0).astype(BF16))
    return tail + jnp.where((row & 3) == 1, scalar_lanes(scalars), 0.0)


def store_rows(out_ref, first, grad, tail):
    for c in range(OWNERS):
        rows = slice(ROWS * c, ROWS * (c + 1))
        out_ref[c, first : first + ROWS, 0:HIDDEN] = grad[rows, :].astype(BF16)
        out_ref[c, first : first + ROWS, HIDDEN:WIDE] = tail[rows, :].astype(BF16)


def to_left(x, count):
    return pltpu.roll(x, TAIL - count, 1)


def combined(tail):
    lane = iota((ROWS, TAIL), 1)
    one = to_left(tail, 1)
    second = jnp.where(lane >= 32, one + to_left(tail, 2), jnp.where(lane >= 8, to_left(tail, 8), one))
    return tail + second


def store_copies(out_ref, rows):
    lane = iota((ROWS, TAIL), 1)
    tail = rows[:, HIDDEN:WIDE]
    tail = jnp.where(lane == 0, tail * 0.125, jnp.where((lane >= 8) & (lane < 16), tail, 0.0))
    high = tail.astype(BF16).astype(F32)
    low = tail - high
    packed = high + jnp.where(lane == 1, pltpu.roll(low, 1, 1), jnp.where(lane >= 16, pltpu.roll(low, 8, 1), 0.0))
    packed = packed.astype(BF16)
    coupling = rows[:, 0:HIDDEN].astype(BF16)
    for c in range(OWNERS):
        out_ref[c, :, 0:HIDDEN] = coupling
        out_ref[c, :, HIDDEN:WIDE] = packed


def setup_kernel(count_ref, spins_ref, energy_ref, accepted_ref, weights_ref, bias_ref, st_ref, tt_ref, vec_ref, out_ref):
    accepted = accepted_ref[...]
    live = iota((16, SLOTS), 1) < count_ref[0]
    major = jnp.where((iota((16, SLOTS), 0) == (accepted >> 7)) & live, 1.0, 0.0).astype(BF16)
    minor = jnp.where(iota((TAIL, SLOTS), 0) == (accepted & 127), 1.0, 0.0).astype(BF16)
    table = by_lanes(major, minor)
    mask = jnp.concatenate([table[h : h + 1, :] for h in range(SLOTS // TAIL)], axis=1)
    spins = spins_ref[...]
    st_ref[...] = by_lanes(eye(SITES), spins).astype(BF16)
    turned = by_lanes(eye(HIDDEN), weights_ref[...]).astype(BF16)
    bias = by_lanes(eye(HIDDEN), jnp.broadcast_to(bias_ref[...].astype(F32).reshape(1, HIDDEN), (16, HIDDEN)).astype(BF16))
    preact = bias[:, 0:1] + dot(turned, st_ref[...])
    tt_ref[...] = jnp.tanh(preact).astype(BF16)
    energy = (energy_ref[...].astype(F32).reshape(1, SLOTS) - ENERGY_MID) * mask
    vec_ref[0:1, :] = mask
    vec_ref[1:2, :] = energy
    vec_ref[2:8, :] = jnp.zeros((6, SLOTS), F32)
    st, tt = st_ref[...], tt_ref[...]
    spins = st.astype(F32)
    both = jnp.concatenate([(spins * energy).astype(BF16), (spins * mask).astype(BF16)], axis=0)
    grad = by_lanes(both, tt)
    hidden = by_lanes(row_pair(energy.astype(BF16), mask.astype(BF16)), tt)
    for k, (row, scalars) in enumerate(((energy, (total(energy),)), (mask, ()))):
        visible = jnp.sum(spins * row, axis=1, keepdims=True)
        store_rows(out_ref, ROWS * k, grad[SITES * k : SITES * (k + 1)], tail_of(visible, hidden[k : k + 1], scalars))


def arrived(in_ref, first):
    rows = slice(first, first + ROWS)
    acc = [in_ref[c, rows, :].astype(F32) for c in range(4)]
    for c in range(4, OWNERS):
        acc[c % 4] = acc[c % 4] + in_ref[c, rows, :].astype(F32)
    acc = (acc[0] + acc[1]) + (acc[2] + acc[3])
    tail = combined(acc[:, HIDDEN:WIDE])
    scalars = [tail[1:2, 32 + 3 * i : 33 + 3 * i] for i in range(SCALARS)]
    return acc[:, 0:HIDDEN], tail, scalars


def lanes_of(values):
    lane = iota((8, TAIL), 1)
    out = jnp.zeros((8, TAIL), F32)
    for i, value in enumerate(values):
        out = jnp.where(lane == i, value, out)
    return out


def first_own_kernel(in_ref, vec_ref, res_ref, ones_ref, vec_out_ref, copies_ref):
    energy, energy_tail, scalars = arrived(in_ref, 0)
    ones, ones_tail, _ = arrived(in_ref, ROWS)
    mean = scalars[0] / TOTAL
    res_ref[:, 0:HIDDEN] = energy - mean * ones
    res_ref[:, HIDDEN:WIDE] = energy_tail - mean * ones_tail
    ones_ref[:, 0:HIDDEN] = ones
    ones_ref[:, HIDDEN:WIDE] = ones_tail
    mask, raw = vec_ref[0:1, :], vec_ref[1:2, :]
    vec_out_ref[0:1, :] = mask
    vec_out_ref[1:2, :] = raw - mean * mask
    vec_out_ref[2:8, :] = jnp.zeros((6, SLOTS), F32)
    store_copies(copies_ref, res_ref[...])


def push_kernel(in_ref, st_ref, tt_ref, parts_ref, bias_ref, rows_ref):
    for c in range(OWNERS):
        rows_ref[ROWS * c : ROWS * (c + 1), :] = in_ref[c].astype(F32)
    tail = rows_ref[:, HIDDEN:WIDE].astype(BF16)
    mine = own_hidden((SITES, HIDDEN))
    l, j = iota((TAIL, HIDDEN), 0), iota((TAIL, HIDDEN), 1) & 7
    spread = dot(tail, jnp.where((l == 8 + j) | (l == 16 + j), 1.0, 0.0).astype(BF16))
    hidden = jnp.sum(jnp.where(mine, spread, 0.0), axis=0, keepdims=True)
    pick = jnp.where((iota((16, TAIL), 0) == 0) & (iota((16, TAIL), 1) < 2), 8.0, 0.0).astype(BF16)
    visible = by_lanes(pick, tail)
    bias_ref[...] = jnp.zeros((8, HIDDEN), F32)
    bias_ref[0:1, :] = hidden
    bias_ref[1:2, 0:SITES] = visible[0:1, :]
    tt, st = tt_ref[...], st_ref[...]
    pick = jnp.where((iota((16, TAIL), 0) == iota((16, TAIL), 1)) & (iota((16, TAIL), 1) < 2), 1.0, 0.0)
    side = dot(row_pair(*two(hidden)), tt) + dot(by_lanes(pick.astype(BF16), tail).astype(BF16), st)
    turned = jnp.transpose(rows_ref[:, 0:HIDDEN]).astype(BF16)
    mixture = dot(turned, st)
    values = jnp.sum(mixture * tt.astype(F32), axis=0, keepdims=True)
    values = (values + side[0:1, :] + side[1:2, :]) * (1.0 / TOTAL)
    for y in range(parts_ref.shape[0]):
        parts_ref[y] = values


def row_sum(parts_ref, mask):
    values = parts_ref[0]
    for y in range(1, parts_ref.shape[0]):
        values = values + parts_ref[y]
    return values * mask


def iteration_scalars(vec_ref, values):
    res, before, o_before, start = (vec_ref[i : i + 1, :] for i in (1, 2, 3, 4))
    return (
        total(res * values),
        total(values * values),
        total(values),
        total(values * o_before),
        total(values * before),
        total(res * o_before),
        total(values * start),
    )


def pull_kernel(parts_ref, vec_ref, st_ref, tt_ref, vec_out_ref, out_ref):
    values = row_sum(parts_ref, vec_ref[0:1, :])
    vec_out_ref[...] = vec_ref[...]
    vec_out_ref[5:6, :] = values
    grad, visible, hidden = pull(values, st_ref[...], tt_ref[...])
    store_rows(out_ref, 0, grad, tail_of(visible, hidden, iteration_scalars(vec_ref, values)))


def conjugate(scalars, past):
    r_zr, zr_zr, zr_sum, zr_zd, zr_d, r_zd, zr_start = scalars[:7]
    if past is None:
        beta, zd_sum, zd_zd, zd_d = None, zr_sum, zr_zr, r_zr
    else:
        rr, sum_before, zz_before, zd_before = past
        beta = r_zr / rr
        zd_sum = zr_sum + beta * sum_before
        zd_zd = zr_zr + 2.0 * beta * zr_zd + beta * beta * zz_before
        zd_d = r_zr + beta * (zr_d + r_zd) + beta * beta * zd_before
    step = r_zr / (zd_zd - zd_sum * zd_sum / TOTAL + SHIFT * zd_d)
    return beta, step, (r_zr, zd_sum, zd_zd, zd_d)


def own_kernel(first, *refs):
    if first:
        in_ref, vec_ref, res_ref, ones_ref, sc_out, vec_out, res_out, dir_out, img_out, copies_ref = refs
    else:
        (in_ref, vec_ref, res_ref, ones_ref, sc_ref, dir_ref, img_ref,
         sc_out, vec_out, res_out, dir_out, img_out, copies_ref) = refs
    grad, tail, scalars = arrived(in_ref, 0)
    past = None if first else tuple(sc_ref[0:1, i : i + 1] for i in range(4))
    beta, step, now = conjugate(scalars, past)
    mean = scalars[2] / TOTAL
    zd_mean = now[1] / TOTAL
    if first:
        kept = (step, now[3])
    else:
        d0_zd1 = scalars[6] + beta * sc_ref[0:1, 5:6]
        kept = (sc_ref[0:1, 4:5], sc_ref[0:1, 5:6], step, now[3], d0_zd1, beta)
    sc_out[...] = lanes_of(now + kept)
    for part, new in ((slice(0, HIDDEN), grad), (slice(HIDDEN, WIDE), tail)):
        image, direction = new - mean * ones_ref[:, part], res_ref[:, part]
        if not first:
            image = image + beta * img_ref[:, part]
            direction = direction + beta * dir_ref[:, part]
        img_out[:, part] = image
        dir_out[:, part] = direction
        res_out[:, part] = res_ref[:, part] - step * (image + SHIFT * direction)
    mask, res, o_res = vec_ref[0:1, :], vec_ref[1:2, :], vec_ref[5:6, :]
    direction, o_dir = res, o_res
    if not first:
        direction = direction + beta * vec_ref[2:3, :]
        o_dir = o_dir + beta * vec_ref[3:4, :]
    vec_out[0:1, :] = mask
    vec_out[1:2, :] = res - step * (o_dir - zd_mean * mask + SHIFT * direction)
    vec_out[2:3, :] = direction
    vec_out[3:4, :] = o_dir
    vec_out[4:5, :] = direction if first else vec_ref[4:5, :]
    vec_out[5:8, :] = jnp.zeros((3, SLOTS), F32)
    store_copies(copies_ref, res_out[...])


def last_scalars_kernel(parts_ref, vec_ref, out_ref):
    values = row_sum(parts_ref, vec_ref[0:1, :])
    lane = iota((OWNERS, TAIL), 1)
    out = jnp.zeros((OWNERS, TAIL), F32)
    for i, value in enumerate(iteration_scalars(vec_ref, values)):
        out = jnp.where(lane == i, value, out)
    out_ref[...] = out


def last_kernel(rep_ref, in_ref, sc_ref, dir0_ref, dir1_ref, res2_ref, b0_ref, b1_ref, b2_ref, vis_ref, hid_ref, mat_ref):
    summed = jnp.sum(in_ref[...], axis=0, keepdims=True)
    scalars = [summed[:, i : i + 1] for i in range(SCALARS)]
    keep = [sc_ref[0:1, i : i + 1] for i in range(9)]
    beta2, step2, now = conjugate(scalars, tuple(keep[0:4]))
    step0, d0_zd0, step1, d1_zd1, d0_zd1 = keep[4:9]
    d0_zd2 = scalars[6] + beta2 * d0_zd1
    d1_zd2 = scalars[4] + beta2 * d1_zd1
    norm = step0 * step0 * d0_zd0 + step1 * step1 * d1_zd1 + step2 * step2 * now[3]
    norm = norm + 2.0 * (step0 * step1 * d0_zd1 + step0 * step2 * d0_zd2 + step1 * step2 * d1_zd2)
    params = float(SITES * HIDDEN * 8 + HIDDEN * 8 + SITES)
    scale = lax.rsqrt(norm / (TOTAL * params) + EPSILON) / TOTAL
    beta1 = sc_ref[0:1, 9:10]
    w0, w1, w2 = scale * step0, scale * (step1 + step2 * beta2), scale * step2
    mat_ref[...] = w0 * dir0_ref[:, 0:HIDDEN] + w1 * dir1_ref[:, 0:HIDDEN] + w2 * res2_ref[:, 0:HIDDEN]
    small = (w0 + w1 * beta1) * b0_ref[...] + w1 * b1_ref[...] + w2 * b2_ref[...]
    hid_ref[...] = small[0]
    a, b = iota((SITES, TAIL), 0), iota((SITES, TAIL), 1)
    pick = jnp.where(a == 32 * rep_ref[0] + b, 1.0, 0.0).astype(F32)
    vis_ref[...] = dot(small[:, 0:SITES], pick, precision=HIGH)[1, 0:32]


def shape(dims, dtype=F32):
    return jax.ShapeDtypeStruct(dims, dtype)


def call(kernel, outs, name, n_in, smem=(), scratch=()):
    vmem = pl.BlockSpec(memory_space=pltpu.VMEM)
    scalar = pl.BlockSpec(memory_space=pltpu.SMEM)
    return pl.pallas_call(
        kernel,
        out_shape=outs,
        in_specs=[scalar if i in smem else vmem for i in range(n_in)],
        out_specs=[vmem] * len(outs),
        scratch_shapes=list(scratch),
        name=name,
        compiler_params=pltpu.CompilerParams(vmem_limit_bytes=VMEM_LIMIT),
    )


def over_chain(blocks):
    return lax.all_to_all(blocks, CHAIN, split_axis=0, concat_axis=0, tiled=True)


def per_device(spins, energies, counts, accepted, hidden_bias, weights):
    reps = lax.axis_size("rep")
    rows = shape((OWNERS, ROWS, WIDE), BF16)
    own = shape((ROWS, WIDE))
    vec_shape = shape((8, SLOTS))
    st, tt, vec, blocks = call(
        setup_kernel,
        [shape((SITES, SLOTS), BF16), shape((HIDDEN, SLOTS), BF16), vec_shape, shape((OWNERS, 2 * ROWS, WIDE), BF16)],
        "setup", 6, smem=(0,),
    )(counts, *(pltpu.with_memory_space_constraint(a, pltpu.HBM) for a in (spins, energies, accepted, weights, hidden_bias)))
    res, ones, vec, copies = call(first_own_kernel, [own, own, vec_shape, rows], "first_own", 2)(over_chain(blocks), vec)

    def push(copies):
        parts, small = call(
            push_kernel, [shape((reps, 1, SLOTS)), shape((8, HIDDEN))], "push", 3,
            scratch=[pltpu.VMEM((SITES, WIDE), F32)],
        )(over_chain(copies), st, tt)
        return lax.all_to_all(parts, "rep", split_axis=0, concat_axis=0, tiled=True), small

    state, smalls, directions = (), [], []
    for iteration in range(2):
        parts, small = push(copies)
        vec, blocks = call(pull_kernel, [vec_shape, rows], "pull", 4)(parts, vec, st, tt)
        sc, vec, res, direction, image, copies = call(
            lambda *refs, first=iteration == 0: own_kernel(first, *refs),
            [shape((8, TAIL)), vec_shape, own, own, own, rows], "own", 4 + len(state),
        )(over_chain(blocks), vec, res, ones, *state)
        state = (sc, direction, image)
        smalls.append(small)
        directions.append(direction)
    parts, small = push(copies)
    smalls.append(small)
    (sums,) = call(last_scalars_kernel, [shape((OWNERS, TAIL))], "last_scalars", 2)(parts, vec)
    vis, hid, mat = call(
        last_kernel, [shape((32,)), shape((HIDDEN,)), shape((ROWS, HIDDEN))], "last", 9, smem=(0,)
    )(lax.axis_index("rep")[None].astype(jnp.int32), over_chain(sums), sc, *directions, res, *smalls)
    return vis, hid, mat


def solution(mesh):
    split = Mesh(
        mesh.devices.reshape(4, 8, 2, mesh.shape["rep"]), ("chain_0", "chain_1", "chain_2", "rep")
    )
    in_specs = (P(CHAIN, None), P(CHAIN), P(CHAIN), P(CHAIN, None), P("rep"), P(None, "rep"))
    out_specs = (P("rep"), P("rep"), P(CHAIN, "rep"))
    return jax.shard_map(
        per_device, mesh=split, in_specs=in_specs, out_specs=out_specs, check_vma=False
    )
```

```python
import jax
import jax.numpy as jnp
from jax import lax
from jax.experimental import pallas as pl
from jax.experimental.pallas import tpu as pltpu
from jax.sharding import Mesh
from jax.sharding import PartitionSpec as P

KEEP_DEV = 768
SHIFT = 0.05
EPSILON = 1e-06
ENERGY_MID = -110.0
CHAIN = ("chain_0", "chain_1", "chain_2")
CHIPS = ("chain_0", "chain_1")
UNITS = ("chain_2", "rep")
F32 = jnp.float32
BF16 = jnp.bfloat16
HIGH = lax.Precision.HIGHEST

SITES = 256
CORES = 2
REPS = 8
HIDDEN = 256
OWNERS = 32
ROWS = 4
COUPLING = 2 * HIDDEN
TAIL = 128
WIDE = COUPLING + TAIL
OWN_SLOTS = 1536
SLOTS = CORES * OWN_SLOTS
SIDE = SITES + 16
PART = SLOTS + ROWS * HIDDEN + HIDDEN
TOTAL = float(KEEP_DEV * OWNERS * CORES)
SCALARS = 8
VMEM_LIMIT = 24 * 2**20


def iota(shape, dim):
    return lax.broadcasted_iota(jnp.int32, shape, dim)


def dot(a, b, dims=((1,), (0,)), precision=None):
    return lax.dot_general(a, b, (dims, ((), ())), precision=precision, preferred_element_type=F32)


def by_lanes(a, b):
    return dot(a, b, ((1,), (1,)))


def eye(n):
    return jnp.where(iota((n, n), 0) == iota((n, n), 1), 1.0, 0.0).astype(BF16)


def two(x):
    high = x.astype(BF16)
    return high, (x - high.astype(F32)).astype(BF16)


def total(x):
    return jnp.sum(x, keepdims=True)


def scalar_lanes(scalars):
    lane = iota((1, TAIL), 1)
    out = jnp.zeros((1, TAIL), F32)
    for i, value in enumerate(scalars):
        one = value.astype(BF16).astype(F32)
        second = (value - one).astype(BF16).astype(F32)
        third = value - one - second
        for k, piece in enumerate((one, second, third)):
            out = jnp.where(lane == 32 + 3 * i + k, piece, out)
    return out


def own_hidden(shape):
    row, col = iota(shape, 0), iota(shape, 1)
    return row == 8 * (col >> 3)


def row_pair(high, low):
    sub = iota((16, high.shape[1]), 0)
    return jnp.where(sub == 0, high.astype(F32), jnp.where(sub == 1, low.astype(F32), 0.0)).astype(BF16)


def pull(weights, st, tt):
    high, low = two(weights)
    spins = st.astype(F32)
    visible = jnp.sum(spins * weights, axis=1, keepdims=True)
    both = jnp.concatenate([(spins * high.astype(F32)).astype(BF16), (spins * low.astype(F32)).astype(BF16)], axis=0)
    grad = by_lanes(both, tt)
    hidden = by_lanes(row_pair(high, low), tt)
    return grad[:SITES] + grad[SITES:], visible, hidden[0:1, :] + hidden[1:2, :]


def tail_of(visible, hidden, scalars):
    v_high = visible.astype(BF16).astype(F32)
    lane, row = iota((SITES, TAIL), 1), iota((SITES, TAIL), 0)
    first = (row & 4) >> 1
    tail = jnp.where(lane == first, v_high, jnp.where(lane == first + 1, visible - v_high, 0.0))
    h_high, h_low = two(hidden)
    mine = own_hidden((SITES, HIDDEN))
    j, l = iota((HIDDEN, TAIL), 0) & 7, iota((HIDDEN, TAIL), 1)
    for piece, base in ((h_high, 8), (h_low, 16)):
        spread = jnp.where(mine, piece.astype(F32), 0.0).astype(BF16)
        tail = tail + dot(spread, jnp.where(l == base + j, 1.0, 0.0).astype(BF16))
    return tail + jnp.where((row & 7) == 1, scalar_lanes(scalars), 0.0)


def store_rows(out_ref, first, grad, tail):
    for c in range(OWNERS):
        near, far = slice(8 * c, 8 * c + ROWS), slice(8 * c + ROWS, 8 * c + 8)
        out_ref[c, first : first + ROWS, 0:HIDDEN] = grad[near, :].astype(BF16)
        out_ref[c, first : first + ROWS, HIDDEN:COUPLING] = grad[far, :].astype(BF16)
        out_ref[c, first : first + ROWS, COUPLING:WIDE] = (tail[near, :] + tail[far, :]).astype(BF16)


def to_left(x, count):
    return pltpu.roll(x, TAIL - count, 1)


def combined(tail):
    lane = iota((ROWS, TAIL), 1)
    one = to_left(tail, 1)
    second = jnp.where(lane >= 32, one + to_left(tail, 2), jnp.where(lane >= 8, to_left(tail, 8), one))
    return tail + second


def store_copies(out_ref, rows):
    lane = iota((ROWS, TAIL), 1)
    tail = rows[:, COUPLING:WIDE]
    tail = jnp.where((lane == 0) | (lane == 2), tail * (1.0 / (CORES * REPS)), jnp.where((lane >= 8) & (lane < 16), tail, 0.0))
    high = tail.astype(BF16).astype(F32)
    low = tail - high
    packed = high + jnp.where(lane < 8, pltpu.roll(low, 1, 1), jnp.where(lane >= 16, pltpu.roll(low, 8, 1), 0.0))
    packed = packed.astype(BF16)
    coupling = rows[:, 0:COUPLING].astype(BF16)
    for c in range(OWNERS):
        out_ref[c, :, 0:COUPLING] = coupling
        out_ref[c, :, COUPLING:WIDE] = packed


def share_kernel(count_ref, core_ref, rep_ref, spins_ref, energy_ref, accepted_ref, out_ref):
    accepted = accepted_ref[...]
    live = iota((16, OWN_SLOTS), 1) < count_ref[0]
    major = jnp.where((iota((16, OWN_SLOTS), 0) == (accepted >> 7)) & live, 1.0, 0.0).astype(BF16)
    minor = jnp.where(iota((TAIL, OWN_SLOTS), 0) == (accepted & 127), 1.0, 0.0).astype(BF16)
    table = by_lanes(major, minor)
    mask = jnp.concatenate([table[h : h + 1, :] for h in range(OWN_SLOTS // TAIL)], axis=1)
    energy = (energy_ref[...].astype(F32).reshape(1, OWN_SLOTS) - ENERGY_MID) * mask
    sites = by_lanes(eye(SITES), spins_ref[...]).astype(BF16)
    extra = row_pair(energy.astype(BF16), mask.astype(BF16))
    for core in range(CORES):
        out_ref[core, 0:SITES, :] = sites
        out_ref[core, SITES:SIDE, :] = extra


def setup_kernel(core_ref, shared_ref, weights_ref, bias_ref, st_ref, tt_ref, vec_ref, out_ref):
    upper = core_ref[0] == 1
    weights = jnp.where(upper, weights_ref[:, HIDDEN:], weights_ref[:, 0:HIDDEN])
    bias_row = bias_ref[...].astype(F32).reshape(1, CORES * HIDDEN)
    bias_row = jnp.where(upper, bias_row[:, HIDDEN:], bias_row[:, 0:HIDDEN])
    turned = by_lanes(eye(HIDDEN), weights).astype(BF16)
    bias = by_lanes(eye(HIDDEN), jnp.broadcast_to(bias_row, (16, HIDDEN)).astype(BF16))
    vec_ref[...] = jnp.zeros((8, SLOTS), F32)
    for core in range(CORES):
        half = slice(core * OWN_SLOTS, (core + 1) * OWN_SLOTS)
        sites = shared_ref[core, 0:SITES, :]
        extra = shared_ref[core, SITES:SIDE, :].astype(F32)
        st_ref[:, half] = sites
        tt_ref[:, half] = jnp.tanh(bias[:, 0:1] + dot(turned, sites)).astype(BF16)
        vec_ref[0:1, half] = extra[1:2, :]
        vec_ref[1:2, half] = extra[0:1, :]
    mask, energy = vec_ref[0:1, :], vec_ref[1:2, :]
    st, tt = st_ref[...], tt_ref[...]
    spins = st.astype(F32)
    both = jnp.concatenate([(spins * energy).astype(BF16), (spins * mask).astype(BF16)], axis=0)
    grad = by_lanes(both, tt)
    hidden = by_lanes(row_pair(energy.astype(BF16), mask.astype(BF16)), tt)
    for k, (row, scalars) in enumerate(((energy, (total(energy),)), (mask, ()))):
        visible = jnp.sum(spins * row, axis=1, keepdims=True)
        store_rows(out_ref, ROWS * k, grad[SITES * k : SITES * (k + 1)], tail_of(visible, hidden[k : k + 1], scalars))


def arrived(in_ref, first):
    rows = slice(first, first + ROWS)
    acc = [in_ref[c, rows, :].astype(F32) for c in range(4)]
    for c in range(4, OWNERS):
        acc[c % 4] = acc[c % 4] + in_ref[c, rows, :].astype(F32)
    acc = (acc[0] + acc[1]) + (acc[2] + acc[3])
    tail = combined(acc[:, COUPLING:WIDE])
    scalars = [tail[1:2, 32 + 3 * i : 33 + 3 * i] for i in range(SCALARS)]
    return acc[:, 0:COUPLING], tail, scalars


def lanes_of(values):
    lane = iota((8, TAIL), 1)
    out = jnp.zeros((8, TAIL), F32)
    for i, value in enumerate(values):
        out = jnp.where(lane == i, value, out)
    return out


def first_own_kernel(in_ref, vec_ref, res_ref, ones_ref, vec_out_ref, copies_ref):
    energy, energy_tail, scalars = arrived(in_ref, 0)
    ones, ones_tail, _ = arrived(in_ref, ROWS)
    mean = scalars[0] / TOTAL
    res_ref[:, 0:COUPLING] = energy - mean * ones
    res_ref[:, COUPLING:WIDE] = energy_tail - mean * ones_tail
    ones_ref[:, 0:COUPLING] = ones
    ones_ref[:, COUPLING:WIDE] = ones_tail
    mask, raw = vec_ref[0:1, :], vec_ref[1:2, :]
    vec_out_ref[0:1, :] = mask
    vec_out_ref[1:2, :] = raw - mean * mask
    vec_out_ref[2:8, :] = jnp.zeros((6, SLOTS), F32)
    store_copies(copies_ref, res_ref[...])


def push_kernel(in_ref, res_ref, st_ref, tt_ref, parts_ref, visible_ref, rows_ref, tail_ref):
    for c in range(OWNERS):
        near, far = slice(8 * c, 8 * c + ROWS), slice(8 * c + ROWS, 8 * c + 8)
        block = in_ref[c].astype(F32)
        rows_ref[near, :] = block[:, 0:HIDDEN]
        rows_ref[far, :] = block[:, HIDDEN:COUPLING]
        tail_ref[near, :] = block[:, COUPLING:WIDE]
        tail_ref[far, :] = block[:, COUPLING:WIDE]
    lane, row = iota((SITES, TAIL), 1), iota((SITES, TAIL), 0)
    tail = tail_ref[...]
    l, j = iota((TAIL, HIDDEN), 0), iota((TAIL, HIDDEN), 1) & 7
    spread = dot(tail.astype(BF16), jnp.where((l == 8 + j) | (l == 16 + j), 1.0, 0.0).astype(BF16))
    hidden = jnp.sum(jnp.where(own_hidden((SITES, HIDDEN)), spread, 0.0), axis=0, keepdims=True)
    seen = jnp.where((lane < 4) & ((lane & 2) == ((row & 4) >> 1)), tail, 0.0).astype(BF16)
    a, b = iota((16, TAIL), 0), iota((16, TAIL), 1)
    pair = by_lanes(jnp.where((b < 4) & ((b & 1) == a), 1.0, 0.0).astype(BF16), seen)
    visible_ref[...] = jnp.zeros((8, SITES), F32)
    visible_ref[0:1, :] = (pair[0:1, :] + pair[1:2, :]) * float(CORES * REPS)
    tt, st = tt_ref[...], st_ref[...]
    side = dot(row_pair(*two(hidden)), tt) + dot(pair.astype(BF16), st)
    turned = jnp.transpose(rows_ref[...]).astype(BF16)
    mixture = dot(turned, st)
    values = jnp.sum(mixture * tt.astype(F32), axis=0, keepdims=True)
    values = (values + side[0:1, :] + side[1:2, :]) * (1.0 / TOTAL)
    for p in range(CORES * REPS):
        parts_ref[p, :, 0:SLOTS] = values
        first = HIDDEN * (p // REPS)
        for r in range(ROWS):
            start = SLOTS + HIDDEN * r
            parts_ref[p, :, start : start + HIDDEN] = res_ref[r : r + 1, first : first + HIDDEN]
        parts_ref[p, :, PART - HIDDEN : PART] = hidden


def row_sum(parts_ref, mask):
    values = parts_ref[0, :, 0:SLOTS]
    for p in range(1, CORES * REPS):
        values = values + parts_ref[p, :, 0:SLOTS]
    return values * mask


def iteration_scalars(vec_ref, values):
    res, before, o_before, start = (vec_ref[i : i + 1, :] for i in (1, 2, 3, 4))
    return (
        total(res * values),
        total(values * values),
        total(values),
        total(values * o_before),
        total(values * before),
        total(res * o_before),
        total(values * start),
    )


def pull_kernel(parts_ref, vec_ref, st_ref, tt_ref, vec_out_ref, out_ref):
    values = row_sum(parts_ref, vec_ref[0:1, :])
    vec_out_ref[...] = vec_ref[...]
    vec_out_ref[5:6, :] = values
    grad, visible, hidden = pull(values, st_ref[...], tt_ref[...])
    store_rows(out_ref, 0, grad, tail_of(visible, hidden, iteration_scalars(vec_ref, values)))


def conjugate(scalars, past):
    r_zr, zr_zr, zr_sum, zr_zd, zr_d, r_zd, zr_start = scalars[:7]
    if past is None:
        beta, zd_sum, zd_zd, zd_d = None, zr_sum, zr_zr, r_zr
    else:
        rr, sum_before, zz_before, zd_before = past
        beta = r_zr / rr
        zd_sum = zr_sum + beta * sum_before
        zd_zd = zr_zr + 2.0 * beta * zr_zd + beta * beta * zz_before
        zd_d = r_zr + beta * (zr_d + r_zd) + beta * beta * zd_before
    step = r_zr / (zd_zd - zd_sum * zd_sum / TOTAL + SHIFT * zd_d)
    return beta, step, (r_zr, zd_sum, zd_zd, zd_d)


def own_kernel(first, *refs):
    if first:
        in_ref, vec_ref, res_ref, ones_ref, sc_out, vec_out, res_out, dir_out, img_out, copies_ref = refs
    else:
        (in_ref, vec_ref, res_ref, ones_ref, sc_ref, dir_ref, img_ref,
         sc_out, vec_out, res_out, copies_ref) = refs
    grad, tail, scalars = arrived(in_ref, 0)
    past = None if first else tuple(sc_ref[0:1, i : i + 1] for i in range(4))
    beta, step, now = conjugate(scalars, past)
    mean = scalars[2] / TOTAL
    zd_mean = now[1] / TOTAL
    if first:
        kept = (step, now[3])
    else:
        d0_zd1 = scalars[6] + beta * sc_ref[0:1, 5:6]
        kept = (sc_ref[0:1, 4:5], sc_ref[0:1, 5:6], step, now[3], d0_zd1, beta)
    sc_out[...] = lanes_of(now + kept)
    for part, new in ((slice(0, COUPLING), grad), (slice(COUPLING, WIDE), tail)):
        image, direction = new - mean * ones_ref[:, part], res_ref[:, part]
        if not first:
            image = image + beta * img_ref[:, part]
            direction = direction + beta * dir_ref[:, part]
        if first:
            img_out[:, part] = image
            dir_out[:, part] = direction
        res_out[:, part] = res_ref[:, part] - step * (image + SHIFT * direction)
    mask, res, o_res = vec_ref[0:1, :], vec_ref[1:2, :], vec_ref[5:6, :]
    direction, o_dir = res, o_res
    if not first:
        direction = direction + beta * vec_ref[2:3, :]
        o_dir = o_dir + beta * vec_ref[3:4, :]
    vec_out[0:1, :] = mask
    vec_out[1:2, :] = res - step * (o_dir - zd_mean * mask + SHIFT * direction)
    vec_out[2:3, :] = direction
    vec_out[3:4, :] = o_dir
    vec_out[4:5, :] = direction if first else vec_ref[4:5, :]
    vec_out[5:8, :] = jnp.zeros((3, SLOTS), F32)
    store_copies(copies_ref, res_out[...])


def last_scalars_kernel(parts_ref, vec_ref, out_ref):
    values = row_sum(parts_ref, vec_ref[0:1, :])
    lane = iota((OWNERS, TAIL), 1)
    out = jnp.zeros((OWNERS, TAIL), F32)
    for i, value in enumerate(iteration_scalars(vec_ref, values)):
        out = jnp.where(lane == i, value, out)
    out_ref[...] = out


def last_kernel(rep_ref, in_ref, sc_ref, p0_ref, p1_ref, p2_ref, v0_ref, v1_ref, v2_ref, vis_ref, hid_ref, mat_ref):
    summed = jnp.sum(in_ref[...], axis=0, keepdims=True)
    scalars = [summed[:, i : i + 1] for i in range(SCALARS)]
    keep = [sc_ref[0:1, i : i + 1] for i in range(10)]
    beta2, step2, now = conjugate(scalars, tuple(keep[0:4]))
    step0, d0_zd0, step1, d1_zd1, d0_zd1, beta1 = keep[4:10]
    d0_zd2 = scalars[6] + beta2 * d0_zd1
    d1_zd2 = scalars[4] + beta2 * d1_zd1
    norm = step0 * step0 * d0_zd0 + step1 * step1 * d1_zd1 + step2 * step2 * now[3]
    norm = norm + 2.0 * (step0 * step1 * d0_zd1 + step0 * step2 * d0_zd2 + step1 * step2 * d1_zd2)
    params = float(SITES * HIDDEN * CORES * REPS + HIDDEN * CORES * REPS + SITES)
    scale = lax.rsqrt(norm / (TOTAL * params) + EPSILON) / TOTAL
    w1 = scale * (step1 + step2 * beta2)
    weights = (scale * step0 + w1 * beta1, w1, scale * step2)
    hidden = []
    for core in range(CORES):
        at = core * REPS + rep_ref[0]
        both = sum(w * ref[at][:, SLOTS:PART] for w, ref in zip(weights, (p0_ref, p1_ref, p2_ref)))
        for r in range(ROWS):
            mat_ref[r : r + 1, core * HIDDEN : (core + 1) * HIDDEN] = both[:, HIDDEN * r : HIDDEN * (r + 1)]
        hidden.append(both[:, ROWS * HIDDEN :])
    hid_ref[...] = jnp.concatenate(hidden, axis=1)[0]
    visible = sum(w * ref[...] for w, ref in zip(weights, (v0_ref, v1_ref, v2_ref)))
    a, b = iota((SITES, TAIL), 0), iota((SITES, TAIL), 1)
    pick = jnp.where(a == 32 * rep_ref[0] + b, 1.0, 0.0).astype(F32)
    vis_ref[...] = dot(visible, pick, precision=HIGH)[0, 0:32]


def shape(dims, dtype=F32):
    return jax.ShapeDtypeStruct(dims, dtype)


def call(kernel, outs, name, n_in, smem=(), scratch=()):
    vmem = pl.BlockSpec(memory_space=pltpu.VMEM)
    scalar = pl.BlockSpec(memory_space=pltpu.SMEM)
    return pl.pallas_call(
        kernel,
        out_shape=outs,
        in_specs=[scalar if i in smem else vmem for i in range(n_in)],
        out_specs=[vmem] * len(outs),
        scratch_shapes=list(scratch),
        name=name,
        compiler_params=pltpu.CompilerParams(vmem_limit_bytes=VMEM_LIMIT),
    )


def exchanged(blocks, axes):
    return lax.all_to_all(blocks, axes, split_axis=0, concat_axis=0, tiled=True)


def place(axis):
    return lax.axis_index(axis)[None].astype(jnp.int32)


def in_hbm(*arrays):
    return [pltpu.with_memory_space_constraint(a, pltpu.HBM) for a in arrays]


def per_device(spins, energies, counts, accepted, hidden_bias, weights):
    rows = shape((OWNERS, ROWS, WIDE), BF16)
    own = shape((ROWS, WIDE))
    vec_shape = shape((8, SLOTS))
    core, rep = place("chain_2"), place("rep")
    (shared,) = call(share_kernel, [shape((CORES, SIDE, OWN_SLOTS), BF16)], "share", 6, smem=(0, 1, 2))(
        counts, core, rep, *in_hbm(spins, energies, accepted)
    )
    st, tt, vec, blocks = call(
        setup_kernel,
        [shape((SITES, SLOTS), BF16), shape((HIDDEN, SLOTS), BF16), vec_shape, shape((OWNERS, 2 * ROWS, WIDE), BF16)],
        "setup", 4, smem=(0,),
    )(core, exchanged(shared, "chain_2"), *in_hbm(weights, hidden_bias))
    res, ones, vec, copies = call(first_own_kernel, [own, own, vec_shape, rows], "first_own", 2)(
        exchanged(blocks, CHIPS), vec
    )

    def push(copies, res):
        parts, visible = call(
            push_kernel, [shape((CORES * REPS, 1, PART)), shape((8, SITES))], "push", 4,
            scratch=[pltpu.VMEM((SITES, HIDDEN), F32), pltpu.VMEM((SITES, TAIL), F32)],
        )(exchanged(copies, CHIPS), res, st, tt)
        return exchanged(parts, UNITS), visible

    state, seen = (), []
    for iteration in range(2):
        seen.append(push(copies, res))
        vec, blocks = call(pull_kernel, [vec_shape, rows], "pull", 4)(seen[-1][0], vec, st, tt)
        first = iteration == 0
        sc, vec, res, *state, copies = call(
            lambda *refs, first=first: own_kernel(first, *refs),
            [shape((8, TAIL)), vec_shape, own, *([own, own] if first else []), rows], "own", 4 + len(state),
        )(exchanged(blocks, CHIPS), vec, res, ones, *state)
        state = (sc, *state)
    seen.append(push(copies, res))
    (sums,) = call(last_scalars_kernel, [shape((OWNERS, TAIL))], "last_scalars", 2)(seen[-1][0], vec)
    return call(
        last_kernel, [shape((32,)), shape((CORES * HIDDEN,)), shape((ROWS, CORES * HIDDEN))], "last", 9, smem=(0,)
    )(rep, exchanged(sums, CHIPS), sc, *(p for p, _ in seen), *(v for _, v in seen))


def solution(mesh):
    split = Mesh(
        mesh.devices.reshape(4, 8, 2, mesh.shape["rep"]), ("chain_0", "chain_1", "chain_2", "rep")
    )
    in_specs = (P(CHAIN, None), P(CHAIN), P(CHAIN), P(CHAIN, None), P("rep"), P(None, "rep"))
    out_specs = (P("rep"), P("rep"), P(CHAIN, "rep"))
    return jax.shard_map(
        per_device, mesh=split, in_specs=in_specs, out_specs=out_specs, check_vma=False
    )
```

```python
import jax
import jax.numpy as jnp
from jax import lax
from jax.experimental import pallas as pl
from jax.experimental.pallas import tpu as pltpu
from jax.sharding import Mesh
from jax.sharding import PartitionSpec as P

KEEP_DEV = 768
SHIFT = 0.05
EPSILON = 1e-06
ENERGY_MID = -110.0
CHAIN = ("chain_0", "chain_1", "chain_2")
CHIPS = ("chain_0", "chain_1")
UNITS = ("chain_2", "rep")
F32 = jnp.float32
BF16 = jnp.bfloat16
HIGH = lax.Precision.HIGHEST

SITES = 256
CORES = 2
REPS = 8
HIDDEN = 512
OWNERS = 32
ROWS = 4
HALF = OWNERS * ROWS
TAIL = 128
WIDE = HIDDEN + TAIL
FIRST = 40
OWN_SLOTS = 1536
SLOTS = CORES * OWN_SLOTS
SIDE = SITES + 16
TOTAL = float(KEEP_DEV * OWNERS * CORES)
SCALARS = 8
VMEM_LIMIT = 24 * 2**20


def iota(shape, dim):
    return lax.broadcasted_iota(jnp.int32, shape, dim)


def dot(a, b, dims=((1,), (0,)), precision=None):
    return lax.dot_general(a, b, (dims, ((), ())), precision=precision, preferred_element_type=F32)


def by_lanes(a, b):
    return dot(a, b, ((1,), (1,)))


def eye(n):
    return jnp.where(iota((n, n), 0) == iota((n, n), 1), 1.0, 0.0).astype(BF16)


def two(x):
    high = x.astype(BF16)
    return high, (x - high.astype(F32)).astype(BF16)


def total(x):
    return jnp.sum(x, keepdims=True)


def scalar_lanes(scalars):
    lane = iota((1, TAIL), 1)
    out = jnp.zeros((1, TAIL), F32)
    for i, value in enumerate(scalars):
        one = value.astype(BF16).astype(F32)
        second = (value - one).astype(BF16).astype(F32)
        third = value - one - second
        for k, piece in enumerate((one, second, third)):
            out = jnp.where(lane == FIRST + 3 * i + k, piece, out)
    return out


def own_hidden(shape):
    row, col = iota(shape, 0), iota(shape, 1)
    return row == 8 * (col >> 4)


def row_pair(high, low):
    sub = iota((16, high.shape[1]), 0)
    return jnp.where(sub == 0, high.astype(F32), jnp.where(sub == 1, low.astype(F32), 0.0)).astype(BF16)


def pull(weights, st, half, tt):
    high, low = two(weights)
    spins = half.astype(F32)
    both = jnp.concatenate([(spins * high.astype(F32)).astype(BF16), (spins * low.astype(F32)).astype(BF16)], axis=0)
    grad = by_lanes(both, tt)
    pair = row_pair(high, low)
    visible, hidden = by_lanes(st, pair), by_lanes(pair, tt)
    return grad[:HALF] + grad[HALF:], visible[:, 0:1] + visible[:, 1:2], hidden[0:1, :] + hidden[1:2, :]


def tail_of(visible, hidden, scalars):
    v_high = visible.astype(BF16).astype(F32)
    lane, row = iota((SITES, TAIL), 1), iota((SITES, TAIL), 0)
    first = (row & 4) >> 1
    tail = jnp.where(lane == first, v_high, jnp.where(lane == first + 1, visible - v_high, 0.0))
    h_high, h_low = two(hidden)
    mine = own_hidden((SITES, HIDDEN))
    j, l = iota((HIDDEN, TAIL), 0) & 15, iota((HIDDEN, TAIL), 1)
    for piece, base in ((h_high, 8), (h_low, 24)):
        spread = jnp.where(mine, piece.astype(F32), 0.0).astype(BF16)
        tail = tail + dot(spread, jnp.where(l == base + j, 1.0, 0.0).astype(BF16))
    return tail + jnp.where((row & 7) == 1, scalar_lanes(scalars), 0.0)


def store_rows(out_ref, first, grad, tail):
    for c in range(OWNERS):
        near, far = slice(8 * c, 8 * c + ROWS), slice(8 * c + ROWS, 8 * c + 8)
        out_ref[c, first : first + ROWS, 0:HIDDEN] = grad[ROWS * c : ROWS * (c + 1), :].astype(BF16)
        out_ref[c, first : first + ROWS, HIDDEN:WIDE] = (tail[near, :] + tail[far, :]).astype(BF16)


def to_left(x, count):
    return pltpu.roll(x, TAIL - count, 1)


def combined(tail):
    lane = iota((ROWS, TAIL), 1)
    one = to_left(tail, 1)
    second = jnp.where(lane >= FIRST, one + to_left(tail, 2), jnp.where(lane >= 8, to_left(tail, 16), one))
    return tail + second


def store_copies(out_ref, rows):
    lane = iota((ROWS, TAIL), 1)
    tail = rows[:, HIDDEN:WIDE]
    tail = jnp.where((lane == 0) | (lane == 2), tail * (1.0 / (CORES * REPS)), jnp.where((lane >= 8) & (lane < 24), tail * (1.0 / CORES), 0.0))
    high = tail.astype(BF16).astype(F32)
    low = tail - high
    packed = high + jnp.where(lane < 8, pltpu.roll(low, 1, 1), jnp.where(lane >= 24, pltpu.roll(low, 16, 1), 0.0))
    packed = packed.astype(BF16)
    coupling = rows[:, 0:HIDDEN].astype(BF16)
    for c in range(OWNERS):
        out_ref[c, :, 0:HIDDEN] = coupling
        out_ref[c, :, HIDDEN:WIDE] = packed


def share_kernel(count_ref, core_ref, rep_ref, spins_ref, energy_ref, accepted_ref, out_ref):
    accepted = accepted_ref[...]
    live = iota((16, OWN_SLOTS), 1) < count_ref[0]
    major = jnp.where((iota((16, OWN_SLOTS), 0) == (accepted >> 7)) & live, 1.0, 0.0).astype(BF16)
    minor = jnp.where(iota((TAIL, OWN_SLOTS), 0) == (accepted & 127), 1.0, 0.0).astype(BF16)
    table = by_lanes(major, minor)
    mask = jnp.concatenate([table[h : h + 1, :] for h in range(OWN_SLOTS // TAIL)], axis=1)
    energy = (energy_ref[...].astype(F32).reshape(1, OWN_SLOTS) - ENERGY_MID) * mask
    sites = by_lanes(eye(SITES), spins_ref[...]).astype(BF16)
    extra = row_pair(energy.astype(BF16), mask.astype(BF16))
    for core in range(CORES):
        out_ref[core, 0:SITES, :] = sites
        out_ref[core, SITES:SIDE, :] = extra


def setup_kernel(core_ref, shared_ref, weights_ref, bias_ref, st_ref, half_ref, tt_ref, vec_ref, out_ref):
    turned = by_lanes(eye(HIDDEN), weights_ref[...]).astype(BF16)
    bias_row = jnp.broadcast_to(bias_ref[...].astype(F32).reshape(1, HIDDEN), (16, HIDDEN))
    bias = by_lanes(eye(HIDDEN), bias_row.astype(BF16))
    row, site = iota((HALF, SITES), 0), iota((HALF, SITES), 1)
    mine = jnp.where(site == 8 * (row >> 2) + 4 * core_ref[0] + (row & 3), 1.0, 0.0).astype(BF16)
    vec_ref[...] = jnp.zeros((8, SLOTS), F32)
    for core in range(CORES):
        part = slice(core * OWN_SLOTS, (core + 1) * OWN_SLOTS)
        sites = shared_ref[core, 0:SITES, :]
        extra = shared_ref[core, SITES:SIDE, :].astype(F32)
        st_ref[:, part] = sites
        half_ref[:, part] = dot(mine, sites).astype(BF16)
        tt_ref[:, part] = jnp.tanh(bias[:, 0:1] + dot(turned, sites)).astype(BF16)
        vec_ref[0:1, part] = extra[1:2, :]
        vec_ref[1:2, part] = extra[0:1, :]
    mask, energy = vec_ref[0:1, :], vec_ref[1:2, :]
    spins = half_ref[...].astype(F32)
    both = jnp.concatenate([(spins * energy).astype(BF16), (spins * mask).astype(BF16)], axis=0)
    tt = tt_ref[...]
    grad = by_lanes(both, tt)
    pair = row_pair(energy.astype(BF16), mask.astype(BF16))
    visible, hidden = by_lanes(st_ref[...], pair), by_lanes(pair, tt)
    for k, scalars in enumerate(((total(energy),), ())):
        tail = tail_of(visible[:, k : k + 1], hidden[k : k + 1], scalars)
        store_rows(out_ref, ROWS * k, grad[HALF * k : HALF * (k + 1)], tail)


def arrived(in_ref, first):
    rows = slice(first, first + ROWS)
    acc = [in_ref[c, rows, :].astype(F32) for c in range(4)]
    for c in range(4, OWNERS):
        acc[c % 4] = acc[c % 4] + in_ref[c, rows, :].astype(F32)
    acc = (acc[0] + acc[1]) + (acc[2] + acc[3])
    tail = combined(acc[:, HIDDEN:WIDE])
    scalars = [tail[1:2, FIRST + 3 * i : FIRST + 3 * i + 1] for i in range(SCALARS)]
    return acc[:, 0:HIDDEN], tail, scalars


def lanes_of(values):
    lane = iota((8, TAIL), 1)
    out = jnp.zeros((8, TAIL), F32)
    for i, value in enumerate(values):
        out = jnp.where(lane == i, value, out)
    return out


def first_own_kernel(in_ref, vec_ref, res_ref, ones_ref, vec_out_ref, copies_ref):
    energy, energy_tail, scalars = arrived(in_ref, 0)
    ones, ones_tail, _ = arrived(in_ref, ROWS)
    mean = scalars[0] / TOTAL
    res_ref[:, 0:HIDDEN] = energy - mean * ones
    res_ref[:, HIDDEN:WIDE] = energy_tail - mean * ones_tail
    ones_ref[:, 0:HIDDEN] = ones
    ones_ref[:, HIDDEN:WIDE] = ones_tail
    mask, raw = vec_ref[0:1, :], vec_ref[1:2, :]
    vec_out_ref[0:1, :] = mask
    vec_out_ref[1:2, :] = raw - mean * mask
    vec_out_ref[2:8, :] = jnp.zeros((6, SLOTS), F32)
    store_copies(copies_ref, res_ref[...])


def push_kernel(in_ref, st_ref, half_ref, tt_ref, parts_ref, small_ref, rows_ref, tail_ref):
    for c in range(OWNERS):
        block = in_ref[c].astype(F32)
        rows_ref[ROWS * c : ROWS * (c + 1), :] = block[:, 0:HIDDEN]
        tail_ref[8 * c : 8 * c + ROWS, :] = block[:, HIDDEN:WIDE]
        tail_ref[8 * c + ROWS : 8 * c + 8, :] = block[:, HIDDEN:WIDE]
    lane, row = iota((SITES, TAIL), 1), iota((SITES, TAIL), 0)
    tail = tail_ref[...]
    l, j = iota((TAIL, HIDDEN), 0), iota((TAIL, HIDDEN), 1) & 15
    spread = dot(tail.astype(BF16), jnp.where((l == 8 + j) | (l == 24 + j), 1.0, 0.0).astype(BF16))
    hidden = jnp.sum(jnp.where(own_hidden((SITES, HIDDEN)), spread, 0.0), axis=0, keepdims=True)
    seen = jnp.where((lane < 4) & ((lane & 2) == ((row & 4) >> 1)), tail, 0.0).astype(BF16)
    a, b = iota((16, TAIL), 0), iota((16, TAIL), 1)
    pair = by_lanes(jnp.where((b < 4) & ((b & 1) == a), 1.0, 0.0).astype(BF16), seen)
    small_ref[...] = jnp.zeros((8, HIDDEN), F32)
    small_ref[0:1, :] = hidden * float(CORES)
    small_ref[1:2, 0:SITES] = (pair[0:1, :] + pair[1:2, :]) * float(CORES * REPS)
    tt = tt_ref[...]
    side = dot(row_pair(*two(hidden)), tt) + dot(pair.astype(BF16), st_ref[...])
    turned = jnp.transpose(rows_ref[...]).astype(BF16)
    mixture = dot(turned, half_ref[...])
    values = jnp.sum(mixture * tt.astype(F32), axis=0, keepdims=True)
    values = (values + side[0:1, :] + side[1:2, :]) * (1.0 / TOTAL)
    packed = jnp.concatenate([values[:, 0:OWN_SLOTS], values[:, OWN_SLOTS:]], axis=0).astype(BF16)
    for p in range(CORES * REPS):
        parts_ref[p] = packed


def row_sum(parts_ref, mask):
    values = parts_ref[0].astype(F32)
    for p in range(1, CORES * REPS):
        values = values + parts_ref[p].astype(F32)
    return jnp.concatenate([values[0:1, :], values[1:2, :]], axis=1) * mask


def iteration_scalars(vec_ref, values):
    res, before, o_before, start = (vec_ref[i : i + 1, :] for i in (1, 2, 3, 4))
    return (
        total(res * values),
        total(values * values),
        total(values),
        total(values * o_before),
        total(values * before),
        total(res * o_before),
        total(values * start),
    )


def pull_kernel(parts_ref, vec_ref, st_ref, half_ref, tt_ref, vec_out_ref, out_ref):
    values = row_sum(parts_ref, vec_ref[0:1, :])
    vec_out_ref[...] = vec_ref[...]
    vec_out_ref[5:6, :] = values
    grad, visible, hidden = pull(values, st_ref[...], half_ref[...], tt_ref[...])
    store_rows(out_ref, 0, grad, tail_of(visible, hidden, iteration_scalars(vec_ref, values)))


def conjugate(scalars, past):
    r_zr, zr_zr, zr_sum, zr_zd, zr_d, r_zd, zr_start = scalars[:7]
    if past is None:
        beta, zd_sum, zd_zd, zd_d = None, zr_sum, zr_zr, r_zr
    else:
        rr, sum_before, zz_before, zd_before = past
        beta = r_zr / rr
        zd_sum = zr_sum + beta * sum_before
        zd_zd = zr_zr + 2.0 * beta * zr_zd + beta * beta * zz_before
        zd_d = r_zr + beta * (zr_d + r_zd) + beta * beta * zd_before
    step = r_zr / (zd_zd - zd_sum * zd_sum / TOTAL + SHIFT * zd_d)
    return beta, step, (r_zr, zd_sum, zd_zd, zd_d)


def own_kernel(first, *refs):
    if first:
        in_ref, vec_ref, res_ref, ones_ref, sc_out, vec_out, res_out, dir_out, img_out, copies_ref = refs
    else:
        (in_ref, vec_ref, res_ref, ones_ref, sc_ref, dir_ref, img_ref,
         sc_out, vec_out, res_out, copies_ref) = refs
    grad, tail, scalars = arrived(in_ref, 0)
    past = None if first else tuple(sc_ref[0:1, i : i + 1] for i in range(4))
    beta, step, now = conjugate(scalars, past)
    mean = scalars[2] / TOTAL
    zd_mean = now[1] / TOTAL
    if first:
        kept = (step, now[3])
    else:
        d0_zd1 = scalars[6] + beta * sc_ref[0:1, 5:6]
        kept = (sc_ref[0:1, 4:5], sc_ref[0:1, 5:6], step, now[3], d0_zd1, beta)
    sc_out[...] = lanes_of(now + kept)
    for part, new in ((slice(0, HIDDEN), grad), (slice(HIDDEN, WIDE), tail)):
        image, direction = new - mean * ones_ref[:, part], res_ref[:, part]
        if not first:
            image = image + beta * img_ref[:, part]
            direction = direction + beta * dir_ref[:, part]
        if first:
            img_out[:, part] = image
            dir_out[:, part] = direction
        res_out[:, part] = res_ref[:, part] - step * (image + SHIFT * direction)
    mask, res, o_res = vec_ref[0:1, :], vec_ref[1:2, :], vec_ref[5:6, :]
    direction, o_dir = res, o_res
    if not first:
        direction = direction + beta * vec_ref[2:3, :]
        o_dir = o_dir + beta * vec_ref[3:4, :]
    vec_out[0:1, :] = mask
    vec_out[1:2, :] = res - step * (o_dir - zd_mean * mask + SHIFT * direction)
    vec_out[2:3, :] = direction
    vec_out[3:4, :] = o_dir
    vec_out[4:5, :] = direction if first else vec_ref[4:5, :]
    vec_out[5:8, :] = jnp.zeros((3, SLOTS), F32)
    store_copies(copies_ref, res_out[...])


def last_scalars_kernel(parts_ref, vec_ref, out_ref):
    values = row_sum(parts_ref, vec_ref[0:1, :])
    lane = iota((OWNERS, TAIL), 1)
    out = jnp.zeros((OWNERS, TAIL), F32)
    for i, value in enumerate(iteration_scalars(vec_ref, values)):
        out = jnp.where(lane == i, value, out)
    out_ref[...] = out


def last_kernel(rep_ref, in_ref, sc_ref, r0_ref, r1_ref, r2_ref, v0_ref, v1_ref, v2_ref, vis_ref, hid_ref, mat_ref):
    summed = jnp.sum(in_ref[...], axis=0, keepdims=True)
    scalars = [summed[:, i : i + 1] for i in range(SCALARS)]
    keep = [sc_ref[0:1, i : i + 1] for i in range(10)]
    beta2, step2, now = conjugate(scalars, tuple(keep[0:4]))
    step0, d0_zd0, step1, d1_zd1, d0_zd1, beta1 = keep[4:10]
    d0_zd2 = scalars[6] + beta2 * d0_zd1
    d1_zd2 = scalars[4] + beta2 * d1_zd1
    norm = step0 * step0 * d0_zd0 + step1 * step1 * d1_zd1 + step2 * step2 * now[3]
    norm = norm + 2.0 * (step0 * step1 * d0_zd1 + step0 * step2 * d0_zd2 + step1 * step2 * d1_zd2)
    params = float(SITES * HIDDEN * REPS + HIDDEN * REPS + SITES)
    scale = lax.rsqrt(norm / (TOTAL * params) + EPSILON) / TOTAL
    w1 = scale * (step1 + step2 * beta2)
    weights = (scale * step0 + w1 * beta1, w1, scale * step2)
    mat_ref[...] = sum(w * ref[:, 0:HIDDEN] for w, ref in zip(weights, (r0_ref, r1_ref, r2_ref)))
    small = sum(w * ref[...] for w, ref in zip(weights, (v0_ref, v1_ref, v2_ref)))
    hid_ref[...] = small[0]
    a, b = iota((SITES, TAIL), 0), iota((SITES, TAIL), 1)
    pick = jnp.where(a == 32 * rep_ref[0] + b, 1.0, 0.0).astype(F32)
    vis_ref[...] = dot(small[:, 0:SITES], pick, precision=HIGH)[1, 0:32]


def shape(dims, dtype=F32):
    return jax.ShapeDtypeStruct(dims, dtype)


def call(kernel, outs, name, n_in, smem=(), scratch=()):
    vmem = pl.BlockSpec(memory_space=pltpu.VMEM)
    scalar = pl.BlockSpec(memory_space=pltpu.SMEM)
    return pl.pallas_call(
        kernel,
        out_shape=outs,
        in_specs=[scalar if i in smem else vmem for i in range(n_in)],
        out_specs=[vmem] * len(outs),
        scratch_shapes=list(scratch),
        name=name,
        compiler_params=pltpu.CompilerParams(vmem_limit_bytes=VMEM_LIMIT),
    )


def exchanged(blocks, axes):
    return lax.all_to_all(blocks, axes, split_axis=0, concat_axis=0, tiled=True)


def place(axis):
    return lax.axis_index(axis)[None].astype(jnp.int32)


def in_hbm(*arrays):
    return [pltpu.with_memory_space_constraint(a, pltpu.HBM) for a in arrays]


def per_device(spins, energies, counts, accepted, hidden_bias, weights):
    rows = shape((OWNERS, ROWS, WIDE), BF16)
    own = shape((ROWS, WIDE))
    vec_shape = shape((8, SLOTS))
    core, rep = place("chain_2"), place("rep")
    (shared,) = call(share_kernel, [shape((CORES, SIDE, OWN_SLOTS), BF16)], "share", 6, smem=(0, 1, 2))(
        counts, core, rep, *in_hbm(spins, energies, accepted)
    )
    spins_and_acts = [shape((n, SLOTS), BF16) for n in (SITES, HALF, HIDDEN)]
    *operands, vec, blocks = call(
        setup_kernel,
        [*spins_and_acts, vec_shape, shape((OWNERS, 2 * ROWS, WIDE), BF16)],
        "setup", 4, smem=(0,),
    )(core, exchanged(shared, "chain_2"), *in_hbm(weights, hidden_bias))
    res, ones, vec, copies = call(first_own_kernel, [own, own, vec_shape, rows], "first_own", 2)(
        exchanged(blocks, CHIPS), vec
    )

    def push(copies):
        parts, small = call(
            push_kernel, [shape((CORES * REPS, 2, OWN_SLOTS), BF16), shape((8, HIDDEN))], "push", 4,
            scratch=[pltpu.VMEM((HALF, HIDDEN), F32), pltpu.VMEM((SITES, TAIL), F32)],
        )(exchanged(copies, CHIPS), *operands)
        return exchanged(parts, UNITS), small

    state, smalls, residuals = (), [], [res]
    for iteration in range(2):
        parts, small = push(copies)
        vec, blocks = call(pull_kernel, [vec_shape, rows], "pull", 5)(parts, vec, *operands)
        first = iteration == 0
        sc, vec, res, *state, copies = call(
            lambda *refs, first=first: own_kernel(first, *refs),
            [shape((8, TAIL)), vec_shape, own, *([own, own] if first else []), rows], "own", 4 + len(state),
        )(exchanged(blocks, CHIPS), vec, res, ones, *state)
        state = (sc, *state)
        smalls.append(small)
        residuals.append(res)
    parts, small = push(copies)
    smalls.append(small)
    (sums,) = call(last_scalars_kernel, [shape((OWNERS, TAIL))], "last_scalars", 2)(parts, vec)
    return call(
        last_kernel, [shape((32,)), shape((HIDDEN,)), shape((ROWS, HIDDEN))], "last", 9, smem=(0,)
    )(rep, exchanged(sums, CHIPS), sc, *residuals, *smalls)


def solution(mesh):
    split = Mesh(
        mesh.devices.reshape(4, 8, 2, mesh.shape["rep"]), ("chain_0", "chain_1", "chain_2", "rep")
    )
    in_specs = (P(CHAIN, None), P(CHAIN), P(CHAIN), P(CHAIN, None), P("rep"), P(None, "rep"))
    out_specs = (P("rep"), P("rep"), P(CHAIN, "rep"))
    return jax.shard_map(
        per_device, mesh=split, in_specs=in_specs, out_specs=out_specs, check_vma=False
    )
```

```python
import jax
import jax.numpy as jnp
from jax import lax
from jax.experimental import pallas as pl
from jax.experimental.pallas import tpu as pltpu
from jax.sharding import Mesh
from jax.sharding import PartitionSpec as P

KEEP_DEV = 768
SHIFT = 0.05
EPSILON = 1e-06
ENERGY_MID = -110.0
CHAIN = ("chain_0", "chain_1", "chain_2")
CHIPS = ("chain_0", "chain_1")
UNITS = ("chain_2", "rep")
F32 = jnp.float32
BF16 = jnp.bfloat16
HIGH = lax.Precision.HIGHEST

SITES = 256
CORES = 2
REPS = 8
HIDDEN = 512
OWNERS = 32
ROWS = 4
HALF = OWNERS * ROWS
TAIL = 128
WIDE = HIDDEN + TAIL
FIRST = 40
OWN_SLOTS = 1536
SLOTS = CORES * OWN_SLOTS
SIDE = SITES + 16
TOTAL = float(KEEP_DEV * OWNERS * CORES)
SCALARS = 8
VMEM_LIMIT = 24 * 2**20


def iota(shape, dim):
    return lax.broadcasted_iota(jnp.int32, shape, dim)


def dot(a, b, dims=((1,), (0,)), precision=None):
    return lax.dot_general(a, b, (dims, ((), ())), precision=precision, preferred_element_type=F32)


def by_lanes(a, b):
    return dot(a, b, ((1,), (1,)))


def eye(n):
    return jnp.where(iota((n, n), 0) == iota((n, n), 1), 1.0, 0.0).astype(BF16)


def two(x):
    high = x.astype(BF16)
    return high, (x - high.astype(F32)).astype(BF16)


def total(x):
    return jnp.sum(x, keepdims=True)


def scalar_lanes(scalars):
    lane = iota((1, TAIL), 1)
    out = jnp.zeros((1, TAIL), F32)
    for i, value in enumerate(scalars):
        one = value.astype(BF16).astype(F32)
        second = (value - one).astype(BF16).astype(F32)
        third = value - one - second
        for k, piece in enumerate((one, second, third)):
            out = jnp.where(lane == FIRST + 3 * i + k, piece, out)
    return out


def own_hidden(shape):
    row, col = iota(shape, 0), iota(shape, 1)
    return row == 8 * (col >> 4)


def row_pair(high, low):
    sub = iota((16, high.shape[1]), 0)
    return jnp.where(sub == 0, high.astype(F32), jnp.where(sub == 1, low.astype(F32), 0.0)).astype(BF16)


def pull(weights, st, half, tt):
    high, low = two(weights)
    spins = half.astype(F32)
    pair = row_pair(high, low)
    rows = [(spins * high.astype(F32)).astype(BF16), (spins * low.astype(F32)).astype(BF16), pair]
    grad = by_lanes(jnp.concatenate(rows, axis=0), tt)
    visible = by_lanes(st, pair)
    hidden = grad[2 * HALF : 2 * HALF + 1] + grad[2 * HALF + 1 : 2 * HALF + 2]
    return grad[:HALF] + grad[HALF : 2 * HALF], visible[:, 0:1] + visible[:, 1:2], hidden


def tail_of(visible, hidden, scalars):
    v_high = visible.astype(BF16).astype(F32)
    lane, row = iota((SITES, TAIL), 1), iota((SITES, TAIL), 0)
    first = (row & 4) >> 1
    tail = jnp.where(lane == first, v_high, jnp.where(lane == first + 1, visible - v_high, 0.0))
    h_high, h_low = two(hidden)
    mine = own_hidden((SITES, HIDDEN))
    j, l = iota((HIDDEN, TAIL), 0) & 15, iota((HIDDEN, TAIL), 1)
    for piece, base in ((h_high, 8), (h_low, 24)):
        spread = jnp.where(mine, piece.astype(F32), 0.0).astype(BF16)
        tail = tail + dot(spread, jnp.where(l == base + j, 1.0, 0.0).astype(BF16))
    return tail + jnp.where((row & 7) == 1, scalar_lanes(scalars), 0.0)


def store_rows(out_ref, first, grad, tail):
    for c in range(OWNERS):
        near, far = slice(8 * c, 8 * c + ROWS), slice(8 * c + ROWS, 8 * c + 8)
        out_ref[c, first : first + ROWS, 0:HIDDEN] = grad[ROWS * c : ROWS * (c + 1), :].astype(BF16)
        out_ref[c, first : first + ROWS, HIDDEN:WIDE] = (tail[near, :] + tail[far, :]).astype(BF16)


def to_left(x, count):
    return pltpu.roll(x, TAIL - count, 1)


def combined(tail):
    lane = iota((ROWS, TAIL), 1)
    one = to_left(tail, 1)
    second = jnp.where(lane >= FIRST, one + to_left(tail, 2), jnp.where(lane >= 8, to_left(tail, 16), one))
    return tail + second


def store_copies(out_ref, rows):
    lane = iota((ROWS, TAIL), 1)
    tail = rows[:, HIDDEN:WIDE]
    tail = jnp.where((lane == 0) | (lane == 2), tail * (1.0 / (CORES * REPS)), jnp.where((lane >= 8) & (lane < 24), tail * (1.0 / CORES), 0.0))
    high = tail.astype(BF16).astype(F32)
    low = tail - high
    packed = high + jnp.where(lane < 8, pltpu.roll(low, 1, 1), jnp.where(lane >= 24, pltpu.roll(low, 16, 1), 0.0))
    packed = packed.astype(BF16)
    coupling = rows[:, 0:HIDDEN].astype(BF16)
    for c in range(OWNERS):
        out_ref[c, :, 0:HIDDEN] = coupling
        out_ref[c, :, HIDDEN:WIDE] = packed


def share_kernel(
    count_ref, core_ref, rep_ref, spins_ref, energy_ref, accepted_ref, weights_ref, bias_ref, out_ref, turned_ref
):
    accepted = accepted_ref[...]
    live = iota((16, OWN_SLOTS), 1) < count_ref[0]
    major = jnp.where((iota((16, OWN_SLOTS), 0) == (accepted >> 7)) & live, 1.0, 0.0).astype(BF16)
    minor = jnp.where(iota((TAIL, OWN_SLOTS), 0) == (accepted & 127), 1.0, 0.0).astype(BF16)
    table = by_lanes(major, minor)
    mask = jnp.concatenate([table[h : h + 1, :] for h in range(OWN_SLOTS // TAIL)], axis=1)
    energy = (energy_ref[...].astype(F32).reshape(1, OWN_SLOTS) - ENERGY_MID) * mask
    sites = by_lanes(eye(SITES), spins_ref[...]).astype(BF16)
    extra = row_pair(energy.astype(BF16), mask.astype(BF16))
    for core in range(CORES):
        out_ref[core, 0:SITES, :] = sites
        out_ref[core, SITES:SIDE, :] = extra
    bias_row = jnp.broadcast_to(bias_ref[...].astype(F32).reshape(1, HIDDEN), (16, HIDDEN))
    turned_ref[:, 0:SITES] = by_lanes(eye(HIDDEN), weights_ref[...]).astype(BF16)
    turned_ref[:, SITES:SIDE] = by_lanes(eye(HIDDEN), bias_row.astype(BF16)).astype(BF16)


def setup_kernel(core_ref, shared_ref, turned_ref, st_ref, half_ref, tt_ref, vec_ref, out_ref):
    turned = turned_ref[:, 0:SITES]
    bias = turned_ref[:, SITES : SITES + 1].astype(F32)
    row, site = iota((HALF, SITES), 0), iota((HALF, SITES), 1)
    mine = jnp.where(site == 8 * (row >> 2) + 4 * core_ref[0] + (row & 3), 1.0, 0.0).astype(BF16)
    vec_ref[...] = jnp.zeros((8, SLOTS), F32)
    for core in range(CORES):
        part = slice(core * OWN_SLOTS, (core + 1) * OWN_SLOTS)
        sites = shared_ref[core, 0:SITES, :]
        extra = shared_ref[core, SITES:SIDE, :].astype(F32)
        st_ref[:, part] = sites
        half_ref[0:HALF, part] = dot(mine, sites).astype(BF16)
        half_ref[HALF:, part] = jnp.ones((16, OWN_SLOTS), BF16)
        tt_ref[:, part] = jnp.tanh(bias + dot(turned, sites)).astype(BF16)
        vec_ref[0:1, part] = extra[1:2, :]
        vec_ref[1:2, part] = extra[0:1, :]
    mask, energy = vec_ref[0:1, :], vec_ref[1:2, :]
    spins = half_ref[0:HALF, :].astype(F32)
    pair = row_pair(energy.astype(BF16), mask.astype(BF16))
    rows = [(spins * energy).astype(BF16), (spins * mask).astype(BF16), pair]
    grad = by_lanes(jnp.concatenate(rows, axis=0), tt_ref[...])
    visible, hidden = by_lanes(st_ref[...], pair), grad[2 * HALF :]
    for k, scalars in enumerate(((total(energy),), ())):
        tail = tail_of(visible[:, k : k + 1], hidden[k : k + 1], scalars)
        store_rows(out_ref, ROWS * k, grad[HALF * k : HALF * (k + 1)], tail)


def arrived(in_ref, first):
    rows = slice(first, first + ROWS)
    acc = [in_ref[c, rows, :].astype(F32) for c in range(4)]
    for c in range(4, OWNERS):
        acc[c % 4] = acc[c % 4] + in_ref[c, rows, :].astype(F32)
    acc = (acc[0] + acc[1]) + (acc[2] + acc[3])
    tail = combined(acc[:, HIDDEN:WIDE])
    scalars = [tail[1:2, FIRST + 3 * i : FIRST + 3 * i + 1] for i in range(SCALARS)]
    return acc[:, 0:HIDDEN], tail, scalars


def lanes_of(values):
    lane = iota((8, TAIL), 1)
    out = jnp.zeros((8, TAIL), F32)
    for i, value in enumerate(values):
        out = jnp.where(lane == i, value, out)
    return out


def first_own_kernel(in_ref, vec_ref, res_ref, ones_ref, vec_out_ref, copies_ref):
    energy, energy_tail, scalars = arrived(in_ref, 0)
    ones, ones_tail, _ = arrived(in_ref, ROWS)
    mean = scalars[0] / TOTAL
    res_ref[:, 0:HIDDEN] = energy - mean * ones
    res_ref[:, HIDDEN:WIDE] = energy_tail - mean * ones_tail
    ones_ref[:, 0:HIDDEN] = ones
    ones_ref[:, HIDDEN:WIDE] = ones_tail
    mask, raw = vec_ref[0:1, :], vec_ref[1:2, :]
    vec_out_ref[0:1, :] = mask
    vec_out_ref[1:2, :] = raw - mean * mask
    vec_out_ref[2:8, :] = jnp.zeros((6, SLOTS), F32)
    store_copies(copies_ref, res_ref[...])


def push_kernel(in_ref, st_ref, half_ref, tt_ref, parts_ref, small_ref, rows_ref, tail_ref):
    for c in range(OWNERS):
        block = in_ref[c].astype(F32)
        rows_ref[ROWS * c : ROWS * (c + 1), :] = block[:, 0:HIDDEN]
        tail_ref[8 * c : 8 * c + ROWS, :] = block[:, HIDDEN:WIDE]
        tail_ref[8 * c + ROWS : 8 * c + 8, :] = block[:, HIDDEN:WIDE]
    lane, row = iota((SITES, TAIL), 1), iota((SITES, TAIL), 0)
    tail = tail_ref[...]
    l, j = iota((TAIL, HIDDEN), 0), iota((TAIL, HIDDEN), 1) & 15
    spread = dot(tail.astype(BF16), jnp.where((l == 8 + j) | (l == 24 + j), 1.0, 0.0).astype(BF16))
    hidden = jnp.sum(jnp.where(own_hidden((SITES, HIDDEN)), spread, 0.0), axis=0, keepdims=True)
    seen = jnp.where((lane < 4) & ((lane & 2) == ((row & 4) >> 1)), tail, 0.0).astype(BF16)
    a, b = iota((16, TAIL), 0), iota((16, TAIL), 1)
    pair = by_lanes(jnp.where((b < 4) & ((b & 1) == a), 1.0, 0.0).astype(BF16), seen)
    small_ref[...] = jnp.zeros((8, HIDDEN), F32)
    small_ref[0:1, :] = hidden * float(CORES)
    small_ref[1:2, 0:SITES] = (pair[0:1, :] + pair[1:2, :]) * float(CORES * REPS)
    side = dot(pair.astype(BF16), st_ref[...])
    turned = jnp.transpose(rows_ref[...]).astype(BF16)
    columns = by_lanes(eye(HIDDEN), row_pair(*two(hidden))).astype(BF16)
    mixture = dot(jnp.concatenate([turned, columns], axis=1), half_ref[...])
    values = jnp.sum(mixture * tt_ref[...].astype(F32), axis=0, keepdims=True)
    values = (values + side[0:1, :] + side[1:2, :]) * (1.0 / TOTAL)
    packed = jnp.concatenate([values[:, 0:OWN_SLOTS], values[:, OWN_SLOTS:]], axis=0).astype(BF16)
    for p in range(CORES * REPS):
        parts_ref[p] = packed


def row_sum(parts_ref, mask):
    values = parts_ref[0].astype(F32)
    for p in range(1, CORES * REPS):
        values = values + parts_ref[p].astype(F32)
    return jnp.concatenate([values[0:1, :], values[1:2, :]], axis=1) * mask


def iteration_scalars(vec_ref, values):
    res, before, o_before, start = (vec_ref[i : i + 1, :] for i in (1, 2, 3, 4))
    return (
        total(res * values),
        total(values * values),
        total(values),
        total(values * o_before),
        total(values * before),
        total(res * o_before),
        total(values * start),
    )


def pull_kernel(parts_ref, vec_ref, st_ref, half_ref, tt_ref, vec_out_ref, out_ref):
    values = row_sum(parts_ref, vec_ref[0:1, :])
    vec_out_ref[...] = vec_ref[...]
    vec_out_ref[5:6, :] = values
    grad, visible, hidden = pull(values, st_ref[...], half_ref[0:HALF, :], tt_ref[...])
    store_rows(out_ref, 0, grad, tail_of(visible, hidden, iteration_scalars(vec_ref, values)))


def conjugate(scalars, past):
    r_zr, zr_zr, zr_sum, zr_zd, zr_d, r_zd, zr_start = scalars[:7]
    if past is None:
        beta, zd_sum, zd_zd, zd_d = None, zr_sum, zr_zr, r_zr
    else:
        rr, sum_before, zz_before, zd_before = past
        beta = r_zr / rr
        zd_sum = zr_sum + beta * sum_before
        zd_zd = zr_zr + 2.0 * beta * zr_zd + beta * beta * zz_before
        zd_d = r_zr + beta * (zr_d + r_zd) + beta * beta * zd_before
    step = r_zr / (zd_zd - zd_sum * zd_sum / TOTAL + SHIFT * zd_d)
    return beta, step, (r_zr, zd_sum, zd_zd, zd_d)


def own_kernel(first, *refs):
    if first:
        in_ref, vec_ref, res_ref, ones_ref, sc_out, vec_out, res_out, dir_out, img_out, copies_ref = refs
    else:
        (in_ref, vec_ref, res_ref, ones_ref, sc_ref, dir_ref, img_ref,
         sc_out, vec_out, res_out, copies_ref) = refs
    grad, tail, scalars = arrived(in_ref, 0)
    past = None if first else tuple(sc_ref[0:1, i : i + 1] for i in range(4))
    beta, step, now = conjugate(scalars, past)
    mean = scalars[2] / TOTAL
    zd_mean = now[1] / TOTAL
    if first:
        kept = (step, now[3])
    else:
        d0_zd1 = scalars[6] + beta * sc_ref[0:1, 5:6]
        kept = (sc_ref[0:1, 4:5], sc_ref[0:1, 5:6], step, now[3], d0_zd1, beta)
    sc_out[...] = lanes_of(now + kept)
    for part, new in ((slice(0, HIDDEN), grad), (slice(HIDDEN, WIDE), tail)):
        image, direction = new - mean * ones_ref[:, part], res_ref[:, part]
        if not first:
            image = image + beta * img_ref[:, part]
            direction = direction + beta * dir_ref[:, part]
        if first:
            img_out[:, part] = image
            dir_out[:, part] = direction
        res_out[:, part] = res_ref[:, part] - step * (image + SHIFT * direction)
    mask, res, o_res = vec_ref[0:1, :], vec_ref[1:2, :], vec_ref[5:6, :]
    direction, o_dir = res, o_res
    if not first:
        direction = direction + beta * vec_ref[2:3, :]
        o_dir = o_dir + beta * vec_ref[3:4, :]
    vec_out[0:1, :] = mask
    vec_out[1:2, :] = res - step * (o_dir - zd_mean * mask + SHIFT * direction)
    vec_out[2:3, :] = direction
    vec_out[3:4, :] = o_dir
    vec_out[4:5, :] = direction if first else vec_ref[4:5, :]
    vec_out[5:8, :] = jnp.zeros((3, SLOTS), F32)
    store_copies(copies_ref, res_out[...])


def last_scalars_kernel(parts_ref, vec_ref, out_ref):
    values = row_sum(parts_ref, vec_ref[0:1, :])
    lane = iota((OWNERS, TAIL), 1)
    out = jnp.zeros((OWNERS, TAIL), F32)
    for i, value in enumerate(iteration_scalars(vec_ref, values)):
        out = jnp.where(lane == i, value, out)
    out_ref[...] = out


def last_kernel(rep_ref, in_ref, sc_ref, r0_ref, r1_ref, r2_ref, v0_ref, v1_ref, v2_ref, vis_ref, hid_ref, mat_ref):
    summed = jnp.sum(in_ref[...], axis=0, keepdims=True)
    scalars = [summed[:, i : i + 1] for i in range(SCALARS)]
    keep = [sc_ref[0:1, i : i + 1] for i in range(10)]
    beta2, step2, now = conjugate(scalars, tuple(keep[0:4]))
    step0, d0_zd0, step1, d1_zd1, d0_zd1, beta1 = keep[4:10]
    d0_zd2 = scalars[6] + beta2 * d0_zd1
    d1_zd2 = scalars[4] + beta2 * d1_zd1
    norm = step0 * step0 * d0_zd0 + step1 * step1 * d1_zd1 + step2 * step2 * now[3]
    norm = norm + 2.0 * (step0 * step1 * d0_zd1 + step0 * step2 * d0_zd2 + step1 * step2 * d1_zd2)
    params = float(SITES * HIDDEN * REPS + HIDDEN * REPS + SITES)
    scale = lax.rsqrt(norm / (TOTAL * params) + EPSILON) / TOTAL
    w1 = scale * (step1 + step2 * beta2)
    weights = (scale * step0 + w1 * beta1, w1, scale * step2)
    mat_ref[...] = sum(w * ref[:, 0:HIDDEN] for w, ref in zip(weights, (r0_ref, r1_ref, r2_ref)))
    small = sum(w * ref[...] for w, ref in zip(weights, (v0_ref, v1_ref, v2_ref)))
    hid_ref[...] = small[0]
    a, b = iota((SITES, TAIL), 0), iota((SITES, TAIL), 1)
    pick = jnp.where(a == 32 * rep_ref[0] + b, 1.0, 0.0).astype(F32)
    vis_ref[...] = dot(small[:, 0:SITES], pick, precision=HIGH)[1, 0:32]


def shape(dims, dtype=F32):
    return jax.ShapeDtypeStruct(dims, dtype)


def call(kernel, outs, name, n_in, smem=(), scratch=()):
    vmem = pl.BlockSpec(memory_space=pltpu.VMEM)
    scalar = pl.BlockSpec(memory_space=pltpu.SMEM)
    return pl.pallas_call(
        kernel,
        out_shape=outs,
        in_specs=[scalar if i in smem else vmem for i in range(n_in)],
        out_specs=[vmem] * len(outs),
        scratch_shapes=list(scratch),
        name=name,
        compiler_params=pltpu.CompilerParams(vmem_limit_bytes=VMEM_LIMIT),
    )


def exchanged(blocks, axes):
    return lax.all_to_all(blocks, axes, split_axis=0, concat_axis=0, tiled=True)


def place(axis):
    return lax.axis_index(axis)[None].astype(jnp.int32)


def in_hbm(*arrays):
    return [pltpu.with_memory_space_constraint(a, pltpu.HBM) for a in arrays]


def per_device(spins, energies, counts, accepted, hidden_bias, weights):
    rows = shape((OWNERS, ROWS, WIDE), BF16)
    own = shape((ROWS, WIDE))
    vec_shape = shape((8, SLOTS))
    core, rep = place("chain_2"), place("rep")
    shared, turned = call(
        share_kernel, [shape((CORES, SIDE, OWN_SLOTS), BF16), shape((HIDDEN, SIDE), BF16)], "share", 8, smem=(0, 1, 2)
    )(counts, core, rep, *in_hbm(spins, energies, accepted, weights, hidden_bias))
    spins_and_acts = [shape((n, SLOTS), BF16) for n in (SITES, HALF + 16, HIDDEN)]
    *operands, vec, blocks = call(
        setup_kernel,
        [*spins_and_acts, vec_shape, shape((OWNERS, 2 * ROWS, WIDE), BF16)],
        "setup", 3, smem=(0,),
    )(core, exchanged(shared, "chain_2"), turned)
    res, ones, vec, copies = call(first_own_kernel, [own, own, vec_shape, rows], "first_own", 2)(
        exchanged(blocks, CHIPS), vec
    )

    def push(copies):
        parts, small = call(
            push_kernel, [shape((CORES * REPS, 2, OWN_SLOTS), BF16), shape((8, HIDDEN))], "push", 4,
            scratch=[pltpu.VMEM((HALF, HIDDEN), F32), pltpu.VMEM((SITES, TAIL), F32)],
        )(exchanged(copies, CHIPS), *operands)
        return exchanged(parts, UNITS), small

    state, smalls, residuals = (), [], [res]
    for iteration in range(2):
        parts, small = push(copies)
        vec, blocks = call(pull_kernel, [vec_shape, rows], "pull", 5)(parts, vec, *operands)
        first = iteration == 0
        sc, vec, res, *state, copies = call(
            lambda *refs, first=first: own_kernel(first, *refs),
            [shape((8, TAIL)), vec_shape, own, *([own, own] if first else []), rows], "own", 4 + len(state),
        )(exchanged(blocks, CHIPS), vec, res, ones, *state)
        state = (sc, *state)
        smalls.append(small)
        residuals.append(res)
    parts, small = push(copies)
    smalls.append(small)
    (sums,) = call(last_scalars_kernel, [shape((OWNERS, TAIL))], "last_scalars", 2)(parts, vec)
    return call(
        last_kernel, [shape((32,)), shape((HIDDEN,)), shape((ROWS, HIDDEN))], "last", 9, smem=(0,)
    )(rep, exchanged(sums, CHIPS), sc, *residuals, *smalls)


def solution(mesh):
    split = Mesh(
        mesh.devices.reshape(4, 8, 2, mesh.shape["rep"]), ("chain_0", "chain_1", "chain_2", "rep")
    )
    in_specs = (P(CHAIN, None), P(CHAIN), P(CHAIN), P(CHAIN, None), P("rep"), P(None, "rep"))
    out_specs = (P("rep"), P("rep"), P(CHAIN, "rep"))
    return jax.shard_map(
        per_device, mesh=split, in_specs=in_specs, out_specs=out_specs, check_vma=False
    )
```

```python
import jax
import jax.numpy as jnp
from jax import lax
from jax.experimental import pallas as pl
from jax.experimental.pallas import tpu as pltpu
from jax.sharding import Mesh
from jax.sharding import PartitionSpec as P

KEEP_DEV = 768
SHIFT = 0.05
EPSILON = 1e-06
ENERGY_MID = -110.0
CHAIN = ("chain_0", "chain_1", "chain_2")
CHIPS = ("chain_0", "chain_1")
UNITS = ("chain_2", "rep")
F32 = jnp.float32
BF16 = jnp.bfloat16
HIGH = lax.Precision.HIGHEST

SITES = 256
CORES = 2
REPS = 8
HIDDEN = 512
OWNERS = 32
ROWS = 4
HALF = OWNERS * ROWS
TAIL = 128
WIDE = HIDDEN + TAIL
FIRST = 40
OWN_SLOTS = 1536
SLOTS = CORES * OWN_SLOTS
SIDE = SITES + 16
TOTAL = float(KEEP_DEV * OWNERS * CORES)
SCALARS = 8
VMEM_LIMIT = 24 * 2**20


def iota(shape, dim):
    return lax.broadcasted_iota(jnp.int32, shape, dim)


def dot(a, b, dims=((1,), (0,)), precision=None):
    return lax.dot_general(a, b, (dims, ((), ())), precision=precision, preferred_element_type=F32)


def by_lanes(a, b):
    return dot(a, b, ((1,), (1,)))


def eye(n):
    return jnp.where(iota((n, n), 0) == iota((n, n), 1), 1.0, 0.0).astype(BF16)


def two(x):
    high = x.astype(BF16)
    return high, (x - high.astype(F32)).astype(BF16)


def total(x):
    return jnp.sum(x, keepdims=True)


def scalar_lanes(scalars):
    lane = iota((1, TAIL), 1)
    out = jnp.zeros((1, TAIL), F32)
    for i, value in enumerate(scalars):
        one = value.astype(BF16).astype(F32)
        second = (value - one).astype(BF16).astype(F32)
        third = value - one - second
        for k, piece in enumerate((one, second, third)):
            out = jnp.where(lane == FIRST + 3 * i + k, piece, out)
    return out


def own_hidden(shape):
    row, col = iota(shape, 0), iota(shape, 1)
    return row == 8 * (col >> 4)


def row_pair(high, low):
    sub = iota((16, high.shape[1]), 0)
    return jnp.where(sub == 0, high.astype(F32), jnp.where(sub == 1, low.astype(F32), 0.0)).astype(BF16)


def pull(weights, st, half, tt):
    high, low = two(weights)
    spins = half.astype(F32)
    pair = row_pair(high, low)
    rows = [(spins * high.astype(F32)).astype(BF16), (spins * low.astype(F32)).astype(BF16), pair]
    grad = by_lanes(jnp.concatenate(rows, axis=0), tt)
    visible = by_lanes(st, pair)
    hidden = grad[2 * HALF : 2 * HALF + 1] + grad[2 * HALF + 1 : 2 * HALF + 2]
    return grad[:HALF] + grad[HALF : 2 * HALF], visible[:, 0:1] + visible[:, 1:2], hidden


def tail_of(visible, hidden, scalars):
    v_high = visible.astype(BF16).astype(F32)
    lane, row = iota((SITES, TAIL), 1), iota((SITES, TAIL), 0)
    first = (row & 4) >> 1
    tail = jnp.where(lane == first, v_high, jnp.where(lane == first + 1, visible - v_high, 0.0))
    h_high, h_low = two(hidden)
    mine = own_hidden((SITES, HIDDEN))
    j, l = iota((HIDDEN, TAIL), 0) & 15, iota((HIDDEN, TAIL), 1)
    for piece, base in ((h_high, 8), (h_low, 24)):
        spread = jnp.where(mine, piece.astype(F32), 0.0).astype(BF16)
        tail = tail + dot(spread, jnp.where(l == base + j, 1.0, 0.0).astype(BF16))
    return tail + jnp.where((row & 7) == 1, scalar_lanes(scalars), 0.0)


def store_rows(out_ref, first, grad, tail):
    for c in range(OWNERS):
        near, far = slice(8 * c, 8 * c + ROWS), slice(8 * c + ROWS, 8 * c + 8)
        out_ref[c, first : first + ROWS, 0:HIDDEN] = grad[ROWS * c : ROWS * (c + 1), :].astype(BF16)
        out_ref[c, first : first + ROWS, HIDDEN:WIDE] = (tail[near, :] + tail[far, :]).astype(BF16)


def to_left(x, count):
    return pltpu.roll(x, TAIL - count, 1)


def combined(tail):
    lane = iota((ROWS, TAIL), 1)
    one = to_left(tail, 1)
    second = jnp.where(lane >= FIRST, one + to_left(tail, 2), jnp.where(lane >= 8, to_left(tail, 16), one))
    return tail + second


def store_copies(out_ref, rows):
    lane = iota((ROWS, TAIL), 1)
    tail = rows[:, HIDDEN:WIDE]
    tail = jnp.where((lane == 0) | (lane == 2), tail * (1.0 / (CORES * REPS)), jnp.where((lane >= 8) & (lane < 24), tail * (1.0 / CORES), 0.0))
    high = tail.astype(BF16).astype(F32)
    low = tail - high
    packed = high + jnp.where(lane < 8, pltpu.roll(low, 1, 1), jnp.where(lane >= 24, pltpu.roll(low, 16, 1), 0.0))
    packed = packed.astype(BF16)
    coupling = rows[:, 0:HIDDEN].astype(BF16)
    for c in range(OWNERS):
        out_ref[c, :, 0:HIDDEN] = coupling
        out_ref[c, :, HIDDEN:WIDE] = packed


def share_kernel(
    count_ref, spins_ref, energy_ref, accepted_ref, weights_ref, bias_ref, out_ref, turned_ref
):
    accepted = accepted_ref[...]
    live = iota((16, OWN_SLOTS), 1) < count_ref[...].reshape(1, 1)
    major = jnp.where((iota((16, OWN_SLOTS), 0) == (accepted >> 7)) & live, 1.0, 0.0).astype(BF16)
    minor = jnp.where(iota((TAIL, OWN_SLOTS), 0) == (accepted & 127), 1.0, 0.0).astype(BF16)
    table = by_lanes(major, minor)
    mask = jnp.concatenate([table[h : h + 1, :] for h in range(OWN_SLOTS // TAIL)], axis=1)
    energy = (energy_ref[...].astype(F32).reshape(1, OWN_SLOTS) - ENERGY_MID) * mask
    sites = by_lanes(eye(SITES), spins_ref[...]).astype(BF16)
    extra = row_pair(energy.astype(BF16), mask.astype(BF16))
    for core in range(CORES):
        out_ref[core, 0:SITES, :] = sites
        out_ref[core, SITES:SIDE, :] = extra
    bias_row = jnp.broadcast_to(bias_ref[...].astype(F32).reshape(1, HIDDEN), (16, HIDDEN))
    turned_ref[:, 0:SITES] = by_lanes(eye(HIDDEN), weights_ref[...]).astype(BF16)
    turned_ref[:, SITES:SIDE] = by_lanes(eye(HIDDEN), bias_row.astype(BF16)).astype(BF16)


def setup_kernel(shared_ref, turned_ref, st_ref, half_ref, tt_ref, vec_ref, out_ref):
    turned = turned_ref[:, 0:SITES]
    bias = turned_ref[:, SITES : SITES + 1].astype(F32)
    row, site = iota((HALF, SITES), 0), iota((HALF, SITES), 1)
    mine = jnp.where(site == 8 * (row >> 2) + 4 * lax.axis_index("chain_2") + (row & 3), 1.0, 0.0).astype(BF16)
    vec_ref[...] = jnp.zeros((8, SLOTS), F32)
    for core in range(CORES):
        part = slice(core * OWN_SLOTS, (core + 1) * OWN_SLOTS)
        sites = shared_ref[core, 0:SITES, :]
        extra = shared_ref[core, SITES:SIDE, :].astype(F32)
        st_ref[:, part] = sites
        half_ref[:, part] = dot(mine, sites).astype(BF16)
        tt_ref[:, part] = jnp.tanh(bias + dot(turned, sites)).astype(BF16)
        vec_ref[0:1, part] = extra[1:2, :]
        vec_ref[1:2, part] = extra[0:1, :]
    mask, energy = vec_ref[0:1, :], vec_ref[1:2, :]
    spins = half_ref[...].astype(F32)
    pair = row_pair(energy.astype(BF16), mask.astype(BF16))
    rows = [(spins * energy).astype(BF16), (spins * mask).astype(BF16), pair]
    grad = by_lanes(jnp.concatenate(rows, axis=0), tt_ref[...])
    visible, hidden = by_lanes(st_ref[...], pair), grad[2 * HALF :]
    for k, scalars in enumerate(((total(energy),), ())):
        tail = tail_of(visible[:, k : k + 1], hidden[k : k + 1], scalars)
        store_rows(out_ref, ROWS * k, grad[HALF * k : HALF * (k + 1)], tail)


def arrived(in_ref, first):
    rows = slice(first, first + ROWS)
    acc = [in_ref[c, rows, :].astype(F32) for c in range(4)]
    for c in range(4, OWNERS):
        acc[c % 4] = acc[c % 4] + in_ref[c, rows, :].astype(F32)
    acc = (acc[0] + acc[1]) + (acc[2] + acc[3])
    tail = combined(acc[:, HIDDEN:WIDE])
    scalars = [tail[1:2, FIRST + 3 * i : FIRST + 3 * i + 1] for i in range(SCALARS)]
    return acc[:, 0:HIDDEN], tail, scalars


def lanes_of(values):
    lane = iota((8, TAIL), 1)
    out = jnp.zeros((8, TAIL), F32)
    for i, value in enumerate(values):
        out = jnp.where(lane == i, value, out)
    return out


def first_own_kernel(in_ref, vec_ref, res_ref, ones_ref, vec_out_ref, copies_ref):
    energy, energy_tail, scalars = arrived(in_ref, 0)
    ones, ones_tail, _ = arrived(in_ref, ROWS)
    mean = scalars[0] / TOTAL
    res_ref[:, 0:HIDDEN] = energy - mean * ones
    res_ref[:, HIDDEN:WIDE] = energy_tail - mean * ones_tail
    ones_ref[:, 0:HIDDEN] = ones
    ones_ref[:, HIDDEN:WIDE] = ones_tail
    mask, raw = vec_ref[0:1, :], vec_ref[1:2, :]
    vec_out_ref[0:1, :] = mask
    vec_out_ref[1:2, :] = raw - mean * mask
    vec_out_ref[2:8, :] = jnp.zeros((6, SLOTS), F32)
    store_copies(copies_ref, res_ref[...])


def push_kernel(in_ref, st_ref, half_ref, tt_ref, parts_ref, small_ref, rows_ref, tail_ref):
    for c in range(OWNERS):
        block = in_ref[c].astype(F32)
        rows_ref[ROWS * c : ROWS * (c + 1), :] = block[:, 0:HIDDEN]
        tail_ref[8 * c : 8 * c + ROWS, :] = block[:, HIDDEN:WIDE]
        tail_ref[8 * c + ROWS : 8 * c + 8, :] = block[:, HIDDEN:WIDE]
    lane, row = iota((SITES, TAIL), 1), iota((SITES, TAIL), 0)
    tail = tail_ref[...]
    l, j = iota((TAIL, HIDDEN), 0), iota((TAIL, HIDDEN), 1) & 15
    spread = dot(tail.astype(BF16), jnp.where((l == 8 + j) | (l == 24 + j), 1.0, 0.0).astype(BF16))
    hidden = jnp.sum(jnp.where(own_hidden((SITES, HIDDEN)), spread, 0.0), axis=0, keepdims=True)
    seen = jnp.where((lane < 4) & ((lane & 2) == ((row & 4) >> 1)), tail, 0.0).astype(BF16)
    a, b = iota((16, TAIL), 0), iota((16, TAIL), 1)
    pair = by_lanes(jnp.where((b < 4) & ((b & 1) == a), 1.0, 0.0).astype(BF16), seen)
    small_ref[...] = jnp.zeros((8, HIDDEN), F32)
    small_ref[0:1, :] = hidden * float(CORES)
    small_ref[1:2, 0:SITES] = (pair[0:1, :] + pair[1:2, :]) * float(CORES * REPS)
    side = dot(pair.astype(BF16), st_ref[...])
    rows = jnp.concatenate([rows_ref[...].astype(BF16), row_pair(*two(hidden))], axis=0)
    mixture = dot(rows, tt_ref[...])
    side = side + mixture[HALF:, :]
    values = jnp.sum(mixture[0:HALF, :] * half_ref[...].astype(F32), axis=0, keepdims=True)
    values = (values + side[0:1, :] + side[1:2, :]) * (1.0 / TOTAL)
    packed = jnp.concatenate([values[:, 0:OWN_SLOTS], values[:, OWN_SLOTS:]], axis=0).astype(BF16)
    for p in range(CORES * REPS):
        parts_ref[p] = packed


def row_sum(parts_ref, mask):
    values = parts_ref[0].astype(F32)
    for p in range(1, CORES * REPS):
        values = values + parts_ref[p].astype(F32)
    return jnp.concatenate([values[0:1, :], values[1:2, :]], axis=1) * mask


def iteration_scalars(vec_ref, values):
    res, before, o_before, start = (vec_ref[i : i + 1, :] for i in (1, 2, 3, 4))
    return (
        total(res * values),
        total(values * values),
        total(values),
        total(values * o_before),
        total(values * before),
        total(res * o_before),
        total(values * start),
    )


def pull_kernel(parts_ref, vec_ref, st_ref, half_ref, tt_ref, vec_out_ref, out_ref):
    values = row_sum(parts_ref, vec_ref[0:1, :])
    vec_out_ref[...] = vec_ref[...]
    vec_out_ref[5:6, :] = values
    grad, visible, hidden = pull(values, st_ref[...], half_ref[...], tt_ref[...])
    store_rows(out_ref, 0, grad, tail_of(visible, hidden, iteration_scalars(vec_ref, values)))


def conjugate(scalars, past):
    r_zr, zr_zr, zr_sum, zr_zd, zr_d, r_zd, zr_start = scalars[:7]
    if past is None:
        beta, zd_sum, zd_zd, zd_d = None, zr_sum, zr_zr, r_zr
    else:
        rr, sum_before, zz_before, zd_before = past
        beta = r_zr / rr
        zd_sum = zr_sum + beta * sum_before
        zd_zd = zr_zr + 2.0 * beta * zr_zd + beta * beta * zz_before
        zd_d = r_zr + beta * (zr_d + r_zd) + beta * beta * zd_before
    step = r_zr / (zd_zd - zd_sum * zd_sum / TOTAL + SHIFT * zd_d)
    return beta, step, (r_zr, zd_sum, zd_zd, zd_d)


def own_kernel(first, *refs):
    if first:
        in_ref, vec_ref, res_ref, ones_ref, sc_out, vec_out, res_out, dir_out, img_out, copies_ref = refs
    else:
        (in_ref, vec_ref, res_ref, ones_ref, sc_ref, dir_ref, img_ref,
         sc_out, vec_out, res_out, copies_ref) = refs
    grad, tail, scalars = arrived(in_ref, 0)
    past = None if first else tuple(sc_ref[0:1, i : i + 1] for i in range(4))
    beta, step, now = conjugate(scalars, past)
    mean = scalars[2] / TOTAL
    zd_mean = now[1] / TOTAL
    if first:
        kept = (step, now[3])
    else:
        d0_zd1 = scalars[6] + beta * sc_ref[0:1, 5:6]
        kept = (sc_ref[0:1, 4:5], sc_ref[0:1, 5:6], step, now[3], d0_zd1, beta)
    sc_out[...] = lanes_of(now + kept)
    for part, new in ((slice(0, HIDDEN), grad), (slice(HIDDEN, WIDE), tail)):
        image, direction = new - mean * ones_ref[:, part], res_ref[:, part]
        if not first:
            image = image + beta * img_ref[:, part]
            direction = direction + beta * dir_ref[:, part]
        if first:
            img_out[:, part] = image
            dir_out[:, part] = direction
        res_out[:, part] = res_ref[:, part] - step * (image + SHIFT * direction)
    mask, res, o_res = vec_ref[0:1, :], vec_ref[1:2, :], vec_ref[5:6, :]
    direction, o_dir = res, o_res
    if not first:
        direction = direction + beta * vec_ref[2:3, :]
        o_dir = o_dir + beta * vec_ref[3:4, :]
    vec_out[0:1, :] = mask
    vec_out[1:2, :] = res - step * (o_dir - zd_mean * mask + SHIFT * direction)
    vec_out[2:3, :] = direction
    vec_out[3:4, :] = o_dir
    vec_out[4:5, :] = direction if first else vec_ref[4:5, :]
    vec_out[5:8, :] = jnp.zeros((3, SLOTS), F32)
    store_copies(copies_ref, res_out[...])


def last_scalars_kernel(parts_ref, vec_ref, out_ref):
    values = row_sum(parts_ref, vec_ref[0:1, :])
    lane = iota((OWNERS, TAIL), 1)
    out = jnp.zeros((OWNERS, TAIL), F32)
    for i, value in enumerate(iteration_scalars(vec_ref, values)):
        out = jnp.where(lane == i, value, out)
    out_ref[...] = out


def last_kernel(in_ref, sc_ref, r0_ref, r1_ref, r2_ref, v0_ref, v1_ref, v2_ref, vis_ref, hid_ref, mat_ref):
    summed = jnp.sum(in_ref[...], axis=0, keepdims=True)
    scalars = [summed[:, i : i + 1] for i in range(SCALARS)]
    keep = [sc_ref[0:1, i : i + 1] for i in range(10)]
    beta2, step2, now = conjugate(scalars, tuple(keep[0:4]))
    step0, d0_zd0, step1, d1_zd1, d0_zd1, beta1 = keep[4:10]
    d0_zd2 = scalars[6] + beta2 * d0_zd1
    d1_zd2 = scalars[4] + beta2 * d1_zd1
    norm = step0 * step0 * d0_zd0 + step1 * step1 * d1_zd1 + step2 * step2 * now[3]
    norm = norm + 2.0 * (step0 * step1 * d0_zd1 + step0 * step2 * d0_zd2 + step1 * step2 * d1_zd2)
    params = float(SITES * HIDDEN * REPS + HIDDEN * REPS + SITES)
    scale = lax.rsqrt(norm / (TOTAL * params) + EPSILON) / TOTAL
    w1 = scale * (step1 + step2 * beta2)
    weights = (scale * step0 + w1 * beta1, w1, scale * step2)
    mat_ref[...] = sum(w * ref[:, 0:HIDDEN] for w, ref in zip(weights, (r0_ref, r1_ref, r2_ref)))
    small = sum(w * ref[...] for w, ref in zip(weights, (v0_ref, v1_ref, v2_ref)))
    hid_ref[...] = small[0]
    a, b = iota((SITES, TAIL), 0), iota((SITES, TAIL), 1)
    pick = jnp.where(a == 32 * lax.axis_index("rep") + b, 1.0, 0.0).astype(F32)
    vis_ref[...] = dot(small[:, 0:SITES], pick, precision=HIGH)[1, 0:32]


def shape(dims, dtype=F32):
    return jax.ShapeDtypeStruct(dims, dtype)


def call(kernel, outs, name, n_in, scratch=()):
    vmem = pl.BlockSpec(memory_space=pltpu.VMEM)
    return pl.pallas_call(
        kernel,
        out_shape=outs,
        in_specs=[vmem] * n_in,
        out_specs=[vmem] * len(outs),
        scratch_shapes=list(scratch),
        name=name,
        compiler_params=pltpu.CompilerParams(vmem_limit_bytes=VMEM_LIMIT),
    )


def exchanged(blocks, axes):
    return lax.all_to_all(blocks, axes, split_axis=0, concat_axis=0, tiled=True)


def in_hbm(*arrays):
    return [pltpu.with_memory_space_constraint(a, pltpu.HBM) for a in arrays]


def per_device(spins, energies, counts, accepted, hidden_bias, weights):
    rows = shape((OWNERS, ROWS, WIDE), BF16)
    own = shape((ROWS, WIDE))
    vec_shape = shape((8, SLOTS))
    shared, turned = call(
        share_kernel, [shape((CORES, SIDE, OWN_SLOTS), BF16), shape((HIDDEN, SIDE), BF16)], "share", 6
    )(counts, *in_hbm(spins, energies, accepted, weights, hidden_bias))
    spins_and_acts = [shape((n, SLOTS), BF16) for n in (SITES, HALF, HIDDEN)]
    *operands, vec, blocks = call(
        setup_kernel,
        [*spins_and_acts, vec_shape, shape((OWNERS, 2 * ROWS, WIDE), BF16)],
        "setup", 2,
    )(exchanged(shared, "chain_2"), turned)
    res, ones, vec, copies = call(first_own_kernel, [own, own, vec_shape, rows], "first_own", 2)(
        exchanged(blocks, CHIPS), vec
    )

    def push(copies):
        parts, small = call(
            push_kernel, [shape((CORES * REPS, 2, OWN_SLOTS), BF16), shape((8, HIDDEN))], "push", 4,
            scratch=[pltpu.VMEM((HALF, HIDDEN), F32), pltpu.VMEM((SITES, TAIL), F32)],
        )(exchanged(copies, CHIPS), *operands)
        return exchanged(parts, UNITS), small

    state, smalls, residuals = (), [], [res]
    for iteration in range(2):
        parts, small = push(copies)
        vec, blocks = call(pull_kernel, [vec_shape, rows], "pull", 5)(parts, vec, *operands)
        first = iteration == 0
        sc, vec, res, *state, copies = call(
            lambda *refs, first=first: own_kernel(first, *refs),
            [shape((8, TAIL)), vec_shape, own, *([own, own] if first else []), rows], "own", 4 + len(state),
        )(exchanged(blocks, CHIPS), vec, res, ones, *state)
        state = (sc, *state)
        smalls.append(small)
        residuals.append(res)
    parts, small = push(copies)
    smalls.append(small)
    (sums,) = call(last_scalars_kernel, [shape((OWNERS, TAIL))], "last_scalars", 2)(parts, vec)
    return call(
        last_kernel, [shape((32,)), shape((HIDDEN,)), shape((ROWS, HIDDEN))], "last", 8
    )(exchanged(sums, CHIPS), sc, *residuals, *smalls)


def solution(mesh):
    split = Mesh(
        mesh.devices.reshape(4, 8, 2, mesh.shape["rep"]), ("chain_0", "chain_1", "chain_2", "rep")
    )
    in_specs = (P(CHAIN, None), P(CHAIN), P(CHAIN), P(CHAIN, None), P("rep"), P(None, "rep"))
    out_specs = (P("rep"), P("rep"), P(CHAIN, "rep"))
    return jax.shard_map(
        per_device, mesh=split, in_specs=in_specs, out_specs=out_specs, check_vma=False
    )
```

```python
import jax
import jax.numpy as jnp
from jax import lax
from jax.experimental import pallas as pl
from jax.experimental.pallas import tpu as pltpu
from jax.sharding import Mesh
from jax.sharding import PartitionSpec as P

KEEP_DEV = 768
SHIFT = 0.05
EPSILON = 1e-06
ENERGY_MID = -110.0
CHAIN = ("chain_0", "chain_1", "chain_2")
CHIPS = ("chain_0", "chain_1")
UNITS = ("chain_2", "rep")
F32 = jnp.float32
BF16 = jnp.bfloat16
HIGH = lax.Precision.HIGHEST

SITES = 256
CORES = 2
REPS = 8
HIDDEN = 512
OWNERS = 32
ROWS = 4
HALF = OWNERS * ROWS
TAIL = 128
WIDE = HIDDEN + TAIL
FIRST = 40
OWN_SLOTS = 1536
SLOTS = CORES * OWN_SLOTS
SIDE = SITES + 16
TOTAL = float(KEEP_DEV * OWNERS * CORES)
SCALARS = 8
VMEM_LIMIT = 24 * 2**20


def iota(shape, dim):
    return lax.broadcasted_iota(jnp.int32, shape, dim)


def dot(a, b, dims=((1,), (0,)), precision=None):
    return lax.dot_general(a, b, (dims, ((), ())), precision=precision, preferred_element_type=F32)


def by_lanes(a, b):
    return dot(a, b, ((1,), (1,)))


def eye(n):
    return jnp.where(iota((n, n), 0) == iota((n, n), 1), 1.0, 0.0).astype(BF16)


def two(x):
    high = x.astype(BF16)
    return high, (x - high.astype(F32)).astype(BF16)


def total(x):
    return jnp.sum(x, keepdims=True)


def scalar_lanes(scalars):
    lane = iota((1, TAIL), 1)
    out = jnp.zeros((1, TAIL), F32)
    for i, value in enumerate(scalars):
        one = value.astype(BF16).astype(F32)
        second = (value - one).astype(BF16).astype(F32)
        third = value - one - second
        for k, piece in enumerate((one, second, third)):
            out = jnp.where(lane == FIRST + 3 * i + k, piece, out)
    return out


def own_hidden(shape):
    row, col = iota(shape, 0), iota(shape, 1)
    return row == 8 * (col >> 4)


def row_pair(high, low):
    sub = iota((16, high.shape[1]), 0)
    return jnp.where(sub == 0, high.astype(F32), jnp.where(sub == 1, low.astype(F32), 0.0)).astype(BF16)


def part_of(core):
    return slice(core * OWN_SLOTS, (core + 1) * OWN_SLOTS)


def pull(weights, operands):
    grad, visible = 0.0, 0.0
    for core, (st_ref, half_ref, tt_ref) in enumerate(operands):
        high, low = two(weights[:, part_of(core)])
        spins = half_ref[...].astype(F32)
        pair = row_pair(high, low)
        rows = [(spins * high.astype(F32)).astype(BF16), (spins * low.astype(F32)).astype(BF16), pair]
        grad = grad + by_lanes(jnp.concatenate(rows, axis=0), tt_ref[...])
        visible = visible + by_lanes(st_ref[0:SITES, :], pair)
    hidden = grad[2 * HALF : 2 * HALF + 1] + grad[2 * HALF + 1 : 2 * HALF + 2]
    return grad[:HALF] + grad[HALF : 2 * HALF], visible[:, 0:1] + visible[:, 1:2], hidden


def tail_of(visible, hidden, scalars):
    v_high = visible.astype(BF16).astype(F32)
    lane, row = iota((SITES, TAIL), 1), iota((SITES, TAIL), 0)
    first = (row & 4) >> 1
    tail = jnp.where(lane == first, v_high, jnp.where(lane == first + 1, visible - v_high, 0.0))
    h_high, h_low = two(hidden)
    mine = own_hidden((SITES, HIDDEN))
    j, l = iota((HIDDEN, TAIL), 0) & 15, iota((HIDDEN, TAIL), 1)
    for piece, base in ((h_high, 8), (h_low, 24)):
        spread = jnp.where(mine, piece.astype(F32), 0.0).astype(BF16)
        tail = tail + dot(spread, jnp.where(l == base + j, 1.0, 0.0).astype(BF16))
    return tail + jnp.where((row & 7) == 1, scalar_lanes(scalars), 0.0)


def store_rows(out_ref, first, grad, tail):
    for c in range(OWNERS):
        near, far = slice(8 * c, 8 * c + ROWS), slice(8 * c + ROWS, 8 * c + 8)
        out_ref[c, first : first + ROWS, 0:HIDDEN] = grad[ROWS * c : ROWS * (c + 1), :].astype(BF16)
        out_ref[c, first : first + ROWS, HIDDEN:WIDE] = (tail[near, :] + tail[far, :]).astype(BF16)


def to_left(x, count):
    return pltpu.roll(x, TAIL - count, 1)


def combined(tail):
    lane = iota((ROWS, TAIL), 1)
    one = to_left(tail, 1)
    second = jnp.where(lane >= FIRST, one + to_left(tail, 2), jnp.where(lane >= 8, to_left(tail, 16), one))
    return tail + second


def store_copies(out_ref, rows):
    lane = iota((ROWS, TAIL), 1)
    tail = rows[:, HIDDEN:WIDE]
    tail = jnp.where((lane == 0) | (lane == 2), tail * (1.0 / (CORES * REPS)), jnp.where((lane >= 8) & (lane < 24), tail * (1.0 / CORES), 0.0))
    high = tail.astype(BF16).astype(F32)
    low = tail - high
    packed = high + jnp.where(lane < 8, pltpu.roll(low, 1, 1), jnp.where(lane >= 24, pltpu.roll(low, 16, 1), 0.0))
    packed = packed.astype(BF16)
    coupling = rows[:, 0:HIDDEN].astype(BF16)
    for c in range(OWNERS):
        out_ref[c, :, 0:HIDDEN] = coupling
        out_ref[c, :, HIDDEN:WIDE] = packed


def share_kernel(
    count_ref, spins_ref, energy_ref, accepted_ref, weights_ref, bias_ref, st_ref, turned_ref
):
    accepted = accepted_ref[...]
    live = iota((16, OWN_SLOTS), 1) < count_ref[...].reshape(1, 1)
    major = jnp.where((iota((16, OWN_SLOTS), 0) == (accepted >> 7)) & live, 1.0, 0.0).astype(BF16)
    minor = jnp.where(iota((TAIL, OWN_SLOTS), 0) == (accepted & 127), 1.0, 0.0).astype(BF16)
    table = by_lanes(major, minor)
    mask = jnp.concatenate([table[h : h + 1, :] for h in range(OWN_SLOTS // TAIL)], axis=1)
    energy = (energy_ref[...].astype(F32).reshape(1, OWN_SLOTS) - ENERGY_MID) * mask
    st_ref[0:SITES, :] = by_lanes(eye(SITES), spins_ref[...]).astype(BF16)
    st_ref[SITES:SIDE, :] = row_pair(energy.astype(BF16), mask.astype(BF16))
    bias_row = jnp.broadcast_to(bias_ref[...].astype(F32).reshape(1, HIDDEN), (16, HIDDEN))
    turned_ref[:, 0:SITES] = by_lanes(eye(HIDDEN), weights_ref[...]).astype(BF16)
    turned_ref[:, SITES:SIDE] = by_lanes(eye(HIDDEN), bias_row.astype(BF16)).astype(BF16)


def acts_kernel(st_ref, turned_ref, half_ref, tt_ref):
    sites = st_ref[0:SITES, :]
    row, site = iota((HALF, SITES), 0), iota((HALF, SITES), 1)
    mine = jnp.where(site == 8 * (row >> 2) + 4 * lax.axis_index("chain_2") + (row & 3), 1.0, 0.0).astype(BF16)
    half_ref[...] = dot(mine, sites).astype(BF16)
    preact = turned_ref[:, SITES : SITES + 1].astype(F32) + dot(turned_ref[:, 0:SITES], sites)
    tt_ref[...] = jnp.tanh(preact).astype(BF16)


def setup_kernel(st0_ref, half0_ref, tt0_ref, st1_ref, turned_ref, half1_ref, tt1_ref, vec_ref, out_ref):
    acts_kernel(st1_ref, turned_ref, half1_ref, tt1_ref)
    vec_ref[...] = jnp.zeros((8, SLOTS), F32)
    grad, visible, sums = 0.0, 0.0, 0.0
    for core, (st_ref, half_ref, tt_ref) in enumerate(((st0_ref, half0_ref, tt0_ref), (st1_ref, half1_ref, tt1_ref))):
        pair = st_ref[SITES:SIDE, :]
        extra = pair.astype(F32)
        energy, mask = extra[0:1, :], extra[1:2, :]
        vec_ref[0:1, part_of(core)] = mask
        vec_ref[1:2, part_of(core)] = energy
        spins = half_ref[...].astype(F32)
        rows = [(spins * energy).astype(BF16), (spins * mask).astype(BF16), pair]
        grad = grad + by_lanes(jnp.concatenate(rows, axis=0), tt_ref[...])
        visible = visible + by_lanes(st_ref[0:SITES, :], pair)
        sums = sums + total(energy)
    hidden = grad[2 * HALF :]
    for k, scalars in enumerate(((sums,), ())):
        tail = tail_of(visible[:, k : k + 1], hidden[k : k + 1], scalars)
        store_rows(out_ref, ROWS * k, grad[HALF * k : HALF * (k + 1)], tail)


def arrived(in_ref, first):
    rows = slice(first, first + ROWS)
    acc = [in_ref[c, rows, :].astype(F32) for c in range(4)]
    for c in range(4, OWNERS):
        acc[c % 4] = acc[c % 4] + in_ref[c, rows, :].astype(F32)
    acc = (acc[0] + acc[1]) + (acc[2] + acc[3])
    tail = combined(acc[:, HIDDEN:WIDE])
    scalars = [tail[1:2, FIRST + 3 * i : FIRST + 3 * i + 1] for i in range(SCALARS)]
    return acc[:, 0:HIDDEN], tail, scalars


def lanes_of(values):
    lane = iota((8, TAIL), 1)
    out = jnp.zeros((8, TAIL), F32)
    for i, value in enumerate(values):
        out = jnp.where(lane == i, value, out)
    return out


def first_own_kernel(in_ref, vec_ref, res_ref, ones_ref, vec_out_ref, copies_ref):
    energy, energy_tail, scalars = arrived(in_ref, 0)
    ones, ones_tail, _ = arrived(in_ref, ROWS)
    mean = scalars[0] / TOTAL
    res_ref[:, 0:HIDDEN] = energy - mean * ones
    res_ref[:, HIDDEN:WIDE] = energy_tail - mean * ones_tail
    ones_ref[:, 0:HIDDEN] = ones
    ones_ref[:, HIDDEN:WIDE] = ones_tail
    mask, raw = vec_ref[0:1, :], vec_ref[1:2, :]
    vec_out_ref[0:1, :] = mask
    vec_out_ref[1:2, :] = raw - mean * mask
    vec_out_ref[2:8, :] = jnp.zeros((6, SLOTS), F32)
    store_copies(copies_ref, res_ref[...])


def push_kernel(in_ref, st0_ref, half0_ref, tt0_ref, st1_ref, half1_ref, tt1_ref, parts_ref, small_ref, rows_ref, tail_ref):
    for c in range(OWNERS):
        block = in_ref[c].astype(F32)
        rows_ref[ROWS * c : ROWS * (c + 1), :] = block[:, 0:HIDDEN]
        tail_ref[8 * c : 8 * c + ROWS, :] = block[:, HIDDEN:WIDE]
        tail_ref[8 * c + ROWS : 8 * c + 8, :] = block[:, HIDDEN:WIDE]
    lane, row = iota((SITES, TAIL), 1), iota((SITES, TAIL), 0)
    tail = tail_ref[...]
    l, j = iota((TAIL, HIDDEN), 0), iota((TAIL, HIDDEN), 1) & 15
    spread = dot(tail.astype(BF16), jnp.where((l == 8 + j) | (l == 24 + j), 1.0, 0.0).astype(BF16))
    hidden = jnp.sum(jnp.where(own_hidden((SITES, HIDDEN)), spread, 0.0), axis=0, keepdims=True)
    seen = jnp.where((lane < 4) & ((lane & 2) == ((row & 4) >> 1)), tail, 0.0).astype(BF16)
    a, b = iota((16, TAIL), 0), iota((16, TAIL), 1)
    pair = by_lanes(jnp.where((b < 4) & ((b & 1) == a), 1.0, 0.0).astype(BF16), seen)
    small_ref[...] = jnp.zeros((8, HIDDEN), F32)
    small_ref[0:1, :] = hidden * float(CORES)
    small_ref[1:2, 0:SITES] = (pair[0:1, :] + pair[1:2, :]) * float(CORES * REPS)
    rows = jnp.concatenate([rows_ref[...].astype(BF16), row_pair(*two(hidden))], axis=0)
    halves = []
    for st_ref, half_ref, tt_ref in ((st0_ref, half0_ref, tt0_ref), (st1_ref, half1_ref, tt1_ref)):
        mixture = dot(rows, tt_ref[...])
        side = dot(pair.astype(BF16), st_ref[0:SITES, :]) + mixture[HALF:, :]
        values = jnp.sum(mixture[0:HALF, :] * half_ref[...].astype(F32), axis=0, keepdims=True)
        halves.append((values + side[0:1, :] + side[1:2, :]) * (1.0 / TOTAL))
    own = lax.axis_index("chain_2")
    straight, swapped = jnp.concatenate(halves, axis=0), jnp.concatenate(halves[::-1], axis=0)
    for core in range(CORES):
        packed = jnp.where(own == core, straight, swapped).astype(BF16)
        for y in range(REPS):
            parts_ref[core * REPS + y] = packed


def row_sum(parts_ref, mask):
    values = parts_ref[0].astype(F32)
    for p in range(1, CORES * REPS):
        values = values + parts_ref[p].astype(F32)
    return jnp.concatenate([values[0:1, :], values[1:2, :]], axis=1) * mask


def iteration_scalars(vec_ref, values):
    res, before, o_before, start = (vec_ref[i : i + 1, :] for i in (1, 2, 3, 4))
    return (
        total(res * values),
        total(values * values),
        total(values),
        total(values * o_before),
        total(values * before),
        total(res * o_before),
        total(values * start),
    )


def pull_kernel(parts_ref, vec_ref, st0_ref, half0_ref, tt0_ref, st1_ref, half1_ref, tt1_ref, vec_out_ref, out_ref):
    values = row_sum(parts_ref, vec_ref[0:1, :])
    vec_out_ref[...] = vec_ref[...]
    vec_out_ref[5:6, :] = values
    grad, visible, hidden = pull(values, ((st0_ref, half0_ref, tt0_ref), (st1_ref, half1_ref, tt1_ref)))
    store_rows(out_ref, 0, grad, tail_of(visible, hidden, iteration_scalars(vec_ref, values)))


def conjugate(scalars, past):
    r_zr, zr_zr, zr_sum, zr_zd, zr_d, r_zd, zr_start = scalars[:7]
    if past is None:
        beta, zd_sum, zd_zd, zd_d = None, zr_sum, zr_zr, r_zr
    else:
        rr, sum_before, zz_before, zd_before = past
        beta = r_zr / rr
        zd_sum = zr_sum + beta * sum_before
        zd_zd = zr_zr + 2.0 * beta * zr_zd + beta * beta * zz_before
        zd_d = r_zr + beta * (zr_d + r_zd) + beta * beta * zd_before
    step = r_zr / (zd_zd - zd_sum * zd_sum / TOTAL + SHIFT * zd_d)
    return beta, step, (r_zr, zd_sum, zd_zd, zd_d)


def own_kernel(first, *refs):
    if first:
        in_ref, vec_ref, res_ref, ones_ref, sc_out, vec_out, res_out, dir_out, img_out, copies_ref = refs
    else:
        (in_ref, vec_ref, res_ref, ones_ref, sc_ref, dir_ref, img_ref,
         sc_out, vec_out, res_out, copies_ref) = refs
    grad, tail, scalars = arrived(in_ref, 0)
    past = None if first else tuple(sc_ref[0:1, i : i + 1] for i in range(4))
    beta, step, now = conjugate(scalars, past)
    mean = scalars[2] / TOTAL
    zd_mean = now[1] / TOTAL
    if first:
        kept = (step, now[3])
    else:
        d0_zd1 = scalars[6] + beta * sc_ref[0:1, 5:6]
        kept = (sc_ref[0:1, 4:5], sc_ref[0:1, 5:6], step, now[3], d0_zd1, beta)
    sc_out[...] = lanes_of(now + kept)
    for part, new in ((slice(0, HIDDEN), grad), (slice(HIDDEN, WIDE), tail)):
        image, direction = new - mean * ones_ref[:, part], res_ref[:, part]
        if not first:
            image = image + beta * img_ref[:, part]
            direction = direction + beta * dir_ref[:, part]
        if first:
            img_out[:, part] = image
            dir_out[:, part] = direction
        res_out[:, part] = res_ref[:, part] - step * (image + SHIFT * direction)
    mask, res, o_res = vec_ref[0:1, :], vec_ref[1:2, :], vec_ref[5:6, :]
    direction, o_dir = res, o_res
    if not first:
        direction = direction + beta * vec_ref[2:3, :]
        o_dir = o_dir + beta * vec_ref[3:4, :]
    vec_out[0:1, :] = mask
    vec_out[1:2, :] = res - step * (o_dir - zd_mean * mask + SHIFT * direction)
    vec_out[2:3, :] = direction
    vec_out[3:4, :] = o_dir
    vec_out[4:5, :] = direction if first else vec_ref[4:5, :]
    vec_out[5:8, :] = jnp.zeros((3, SLOTS), F32)
    store_copies(copies_ref, res_out[...])


def last_scalars_kernel(parts_ref, vec_ref, out_ref):
    values = row_sum(parts_ref, vec_ref[0:1, :])
    lane = iota((OWNERS, TAIL), 1)
    out = jnp.zeros((OWNERS, TAIL), F32)
    for i, value in enumerate(iteration_scalars(vec_ref, values)):
        out = jnp.where(lane == i, value, out)
    out_ref[...] = out


def last_kernel(in_ref, sc_ref, r0_ref, r1_ref, r2_ref, v0_ref, v1_ref, v2_ref, vis_ref, hid_ref, mat_ref):
    summed = jnp.sum(in_ref[...], axis=0, keepdims=True)
    scalars = [summed[:, i : i + 1] for i in range(SCALARS)]
    keep = [sc_ref[0:1, i : i + 1] for i in range(10)]
    beta2, step2, now = conjugate(scalars, tuple(keep[0:4]))
    step0, d0_zd0, step1, d1_zd1, d0_zd1, beta1 = keep[4:10]
    d0_zd2 = scalars[6] + beta2 * d0_zd1
    d1_zd2 = scalars[4] + beta2 * d1_zd1
    norm = step0 * step0 * d0_zd0 + step1 * step1 * d1_zd1 + step2 * step2 * now[3]
    norm = norm + 2.0 * (step0 * step1 * d0_zd1 + step0 * step2 * d0_zd2 + step1 * step2 * d1_zd2)
    params = float(SITES * HIDDEN * REPS + HIDDEN * REPS + SITES)
    scale = lax.rsqrt(norm / (TOTAL * params) + EPSILON) / TOTAL
    w1 = scale * (step1 + step2 * beta2)
    weights = (scale * step0 + w1 * beta1, w1, scale * step2)
    mat_ref[...] = sum(w * ref[:, 0:HIDDEN] for w, ref in zip(weights, (r0_ref, r1_ref, r2_ref)))
    small = sum(w * ref[...] for w, ref in zip(weights, (v0_ref, v1_ref, v2_ref)))
    hid_ref[...] = small[0]
    a, b = iota((SITES, TAIL), 0), iota((SITES, TAIL), 1)
    pick = jnp.where(a == 32 * lax.axis_index("rep") + b, 1.0, 0.0).astype(F32)
    vis_ref[...] = dot(small[:, 0:SITES], pick, precision=HIGH)[1, 0:32]


def shape(dims, dtype=F32):
    return jax.ShapeDtypeStruct(dims, dtype)


def call(kernel, outs, name, n_in, scratch=()):
    vmem = pl.BlockSpec(memory_space=pltpu.VMEM)
    return pl.pallas_call(
        kernel,
        out_shape=outs,
        in_specs=[vmem] * n_in,
        out_specs=[vmem] * len(outs),
        scratch_shapes=list(scratch),
        name=name,
        compiler_params=pltpu.CompilerParams(vmem_limit_bytes=VMEM_LIMIT),
    )


def exchanged(blocks, axes):
    return lax.all_to_all(blocks, axes, split_axis=0, concat_axis=0, tiled=True)


def in_hbm(*arrays):
    return [pltpu.with_memory_space_constraint(a, pltpu.HBM) for a in arrays]


def per_device(spins, energies, counts, accepted, hidden_bias, weights):
    rows = shape((OWNERS, ROWS, WIDE), BF16)
    own = shape((ROWS, WIDE))
    vec_shape = shape((8, SLOTS))
    st0, turned = call(share_kernel, [shape((SIDE, OWN_SLOTS), BF16), shape((HIDDEN, SIDE), BF16)], "share", 6)(
        counts, *in_hbm(spins, energies, accepted, weights, hidden_bias)
    )
    st1 = lax.ppermute(st0, "chain_2", [(0, 1), (1, 0)])
    half_and_acts = [shape((n, OWN_SLOTS), BF16) for n in (HALF, HIDDEN)]
    half0, tt0 = call(acts_kernel, half_and_acts, "acts", 2)(st0, turned)
    half1, tt1, vec, blocks = call(
        setup_kernel, [*half_and_acts, vec_shape, shape((OWNERS, 2 * ROWS, WIDE), BF16)], "setup", 5
    )(st0, half0, tt0, st1, turned)
    operands = (st0, half0, tt0, st1, half1, tt1)
    res, ones, vec, copies = call(first_own_kernel, [own, own, vec_shape, rows], "first_own", 2)(
        exchanged(blocks, CHIPS), vec
    )

    def push(copies):
        parts, small = call(
            push_kernel, [shape((CORES * REPS, 2, OWN_SLOTS), BF16), shape((8, HIDDEN))], "push", 7,
            scratch=[pltpu.VMEM((HALF, HIDDEN), F32), pltpu.VMEM((SITES, TAIL), F32)],
        )(exchanged(copies, CHIPS), *operands)
        return exchanged(parts, UNITS), small

    state, smalls, residuals = (), [], [res]
    for iteration in range(2):
        parts, small = push(copies)
        vec, blocks = call(pull_kernel, [vec_shape, rows], "pull", 8)(parts, vec, *operands)
        first = iteration == 0
        sc, vec, res, *state, copies = call(
            lambda *refs, first=first: own_kernel(first, *refs),
            [shape((8, TAIL)), vec_shape, own, *([own, own] if first else []), rows], "own", 4 + len(state),
        )(exchanged(blocks, CHIPS), vec, res, ones, *state)
        state = (sc, *state)
        smalls.append(small)
        residuals.append(res)
    parts, small = push(copies)
    smalls.append(small)
    (sums,) = call(last_scalars_kernel, [shape((OWNERS, TAIL))], "last_scalars", 2)(parts, vec)
    return call(
        last_kernel, [shape((32,)), shape((HIDDEN,)), shape((ROWS, HIDDEN))], "last", 8
    )(exchanged(sums, CHIPS), sc, *residuals, *smalls)


def solution(mesh):
    split = Mesh(
        mesh.devices.reshape(4, 8, 2, mesh.shape["rep"]), ("chain_0", "chain_1", "chain_2", "rep")
    )
    in_specs = (P(CHAIN, None), P(CHAIN), P(CHAIN), P(CHAIN, None), P("rep"), P(None, "rep"))
    out_specs = (P("rep"), P("rep"), P(CHAIN, "rep"))
    return jax.shard_map(
        per_device, mesh=split, in_specs=in_specs, out_specs=out_specs, check_vma=False
    )
```

```python
import jax
import jax.numpy as jnp
from jax import lax
from jax.experimental import pallas as pl
from jax.experimental.pallas import tpu as pltpu
from jax.sharding import Mesh
from jax.sharding import PartitionSpec as P

KEEP_DEV = 768
SHIFT = 0.05
EPSILON = 1e-06
ENERGY_MID = -110.0
CHAIN = ("chain_0", "chain_1", "chain_2")
CHIPS = ("chain_0", "chain_1")
UNITS = ("chain_2", "rep")
F32 = jnp.float32
BF16 = jnp.bfloat16
HIGH = lax.Precision.HIGHEST

SITES = 256
CORES = 2
REPS = 8
HIDDEN = 512
OWNERS = 32
ROWS = 4
HALF = OWNERS * ROWS
TAIL = 128
WIDE = HIDDEN + TAIL
FIRST = 40
OWN_SLOTS = 1536
SLOTS = CORES * OWN_SLOTS
SIDE = SITES + 16
TOTAL = float(KEEP_DEV * OWNERS * CORES)
SCALARS = 8
VMEM_LIMIT = 24 * 2**20


def iota(shape, dim):
    return lax.broadcasted_iota(jnp.int32, shape, dim)


def dot(a, b, dims=((1,), (0,)), precision=None):
    return lax.dot_general(a, b, (dims, ((), ())), precision=precision, preferred_element_type=F32)


def by_lanes(a, b):
    return dot(a, b, ((1,), (1,)))


def eye(n):
    return jnp.where(iota((n, n), 0) == iota((n, n), 1), 1.0, 0.0).astype(BF16)


def two(x):
    high = x.astype(BF16)
    return high, (x - high.astype(F32)).astype(BF16)


def total(x):
    return jnp.sum(x, keepdims=True)


def scalar_lanes(scalars):
    lane = iota((1, TAIL), 1)
    out = jnp.zeros((1, TAIL), F32)
    for i, value in enumerate(scalars):
        one = value.astype(BF16).astype(F32)
        second = (value - one).astype(BF16).astype(F32)
        third = value - one - second
        for k, piece in enumerate((one, second, third)):
            out = jnp.where(lane == FIRST + 3 * i + k, piece, out)
    return out


def own_hidden(shape):
    row, col = iota(shape, 0), iota(shape, 1)
    return row == 8 * (col >> 4)


def row_pair(high, low):
    sub = iota((16, high.shape[1]), 0)
    return jnp.where(sub == 0, high.astype(F32), jnp.where(sub == 1, low.astype(F32), 0.0)).astype(BF16)


def part_of(core):
    return slice(core * OWN_SLOTS, (core + 1) * OWN_SLOTS)


def pull(weights, operands):
    grad, visible = 0.0, 0.0
    for core, (st_ref, half_ref, tt_ref) in enumerate(operands):
        high, low = two(weights[:, part_of(core)])
        spins = half_ref[...].astype(F32)
        pair = row_pair(high, low)
        rows = [(spins * high.astype(F32)).astype(BF16), (spins * low.astype(F32)).astype(BF16), pair]
        grad = grad + by_lanes(jnp.concatenate(rows, axis=0), tt_ref[...])
        visible = visible + by_lanes(st_ref[0:SITES, :], pair)
    hidden = grad[2 * HALF : 2 * HALF + 1] + grad[2 * HALF + 1 : 2 * HALF + 2]
    return grad[:HALF] + grad[HALF : 2 * HALF], visible[:, 0:1] + visible[:, 1:2], hidden


def tail_of(visible, hidden, scalars):
    v_high = visible.astype(BF16).astype(F32)
    lane, row = iota((SITES, TAIL), 1), iota((SITES, TAIL), 0)
    first = (row & 4) >> 1
    tail = jnp.where(lane == first, v_high, jnp.where(lane == first + 1, visible - v_high, 0.0))
    h_high, h_low = two(hidden)
    mine = own_hidden((SITES, HIDDEN))
    j, l = iota((HIDDEN, TAIL), 0) & 15, iota((HIDDEN, TAIL), 1)
    for piece, base in ((h_high, 8), (h_low, 24)):
        spread = jnp.where(mine, piece.astype(F32), 0.0).astype(BF16)
        tail = tail + dot(spread, jnp.where(l == base + j, 1.0, 0.0).astype(BF16))
    return tail + jnp.where((row & 7) == 1, scalar_lanes(scalars), 0.0)


def store_rows(out_ref, first, grad, tail):
    for c in range(OWNERS):
        near, far = slice(8 * c, 8 * c + ROWS), slice(8 * c + ROWS, 8 * c + 8)
        out_ref[c, first : first + ROWS, 0:HIDDEN] = grad[ROWS * c : ROWS * (c + 1), :].astype(BF16)
        out_ref[c, first : first + ROWS, HIDDEN:WIDE] = (tail[near, :] + tail[far, :]).astype(BF16)


def to_left(x, count):
    return pltpu.roll(x, TAIL - count, 1)


def combined(tail):
    lane = iota((ROWS, TAIL), 1)
    one = to_left(tail, 1)
    second = jnp.where(lane >= FIRST, one + to_left(tail, 2), jnp.where(lane >= 8, to_left(tail, 16), one))
    return tail + second


def store_copies(out_ref, rows, ones):
    lane = iota((ROWS, TAIL), 1)
    tail = rows[:, HIDDEN:WIDE]
    tail = jnp.where((lane == 0) | (lane == 2), tail * (1.0 / (CORES * REPS)), jnp.where((lane >= 8) & (lane < 24), tail * (1.0 / CORES), 0.0))
    high = tail.astype(BF16).astype(F32)
    low = tail - high
    packed = high + jnp.where(lane < 8, pltpu.roll(low, 1, 1), jnp.where(lane >= 24, pltpu.roll(low, 16, 1), 0.0))
    mean = total(rows[:, 0:HIDDEN] * ones[:, 0:HIDDEN]) * (1.0 / (TOTAL * TOTAL))
    packed = packed + jnp.where(iota((ROWS, TAIL), 0) == 1, scalar_lanes((mean,)), 0.0)
    packed = packed.astype(BF16)
    coupling = rows[:, 0:HIDDEN].astype(BF16)
    for c in range(OWNERS):
        out_ref[c, :, 0:HIDDEN] = coupling
        out_ref[c, :, HIDDEN:WIDE] = packed


def share_kernel(
    count_ref, spins_ref, energy_ref, accepted_ref, weights_ref, bias_ref, st_ref, turned_ref
):
    accepted = accepted_ref[...]
    live = iota((16, OWN_SLOTS), 1) < count_ref[...].reshape(1, 1)
    major = jnp.where((iota((16, OWN_SLOTS), 0) == (accepted >> 7)) & live, 1.0, 0.0).astype(BF16)
    minor = jnp.where(iota((TAIL, OWN_SLOTS), 0) == (accepted & 127), 1.0, 0.0).astype(BF16)
    table = by_lanes(major, minor)
    mask = jnp.concatenate([table[h : h + 1, :] for h in range(OWN_SLOTS // TAIL)], axis=1)
    energy = (energy_ref[...].astype(F32).reshape(1, OWN_SLOTS) - ENERGY_MID) * mask
    st_ref[0:SITES, :] = by_lanes(eye(SITES), spins_ref[...]).astype(BF16)
    st_ref[SITES:SIDE, :] = row_pair(energy.astype(BF16), mask.astype(BF16))
    bias_row = jnp.broadcast_to(bias_ref[...].astype(F32).reshape(1, HIDDEN), (16, HIDDEN))
    turned_ref[:, 0:SITES] = by_lanes(eye(HIDDEN), weights_ref[...]).astype(BF16)
    turned_ref[:, SITES:SIDE] = by_lanes(eye(HIDDEN), bias_row.astype(BF16)).astype(BF16)


def acts_kernel(st_ref, turned_ref, half_ref, tt_ref):
    sites = st_ref[0:SITES, :]
    row, site = iota((HALF, SITES), 0), iota((HALF, SITES), 1)
    mine = jnp.where(site == 8 * (row >> 2) + 4 * lax.axis_index("chain_2") + (row & 3), 1.0, 0.0).astype(BF16)
    half_ref[...] = dot(mine, sites).astype(BF16)
    preact = turned_ref[:, SITES : SITES + 1].astype(F32) + dot(turned_ref[:, 0:SITES], sites)
    tt_ref[...] = jnp.tanh(preact).astype(BF16)


def setup_kernel(st0_ref, half0_ref, tt0_ref, st1_ref, turned_ref, half1_ref, tt1_ref, vec_ref, out_ref):
    acts_kernel(st1_ref, turned_ref, half1_ref, tt1_ref)
    vec_ref[...] = jnp.zeros((8, SLOTS), F32)
    grad, visible, sums = 0.0, 0.0, 0.0
    for core, (st_ref, half_ref, tt_ref) in enumerate(((st0_ref, half0_ref, tt0_ref), (st1_ref, half1_ref, tt1_ref))):
        pair = st_ref[SITES:SIDE, :]
        extra = pair.astype(F32)
        energy, mask = extra[0:1, :], extra[1:2, :]
        vec_ref[0:1, part_of(core)] = mask
        vec_ref[1:2, part_of(core)] = energy
        spins = half_ref[...].astype(F32)
        rows = [(spins * energy).astype(BF16), (spins * mask).astype(BF16), pair]
        grad = grad + by_lanes(jnp.concatenate(rows, axis=0), tt_ref[...])
        visible = visible + by_lanes(st_ref[0:SITES, :], pair)
        sums = sums + total(energy)
    hidden = grad[2 * HALF :]
    for k, scalars in enumerate(((sums,), ())):
        tail = tail_of(visible[:, k : k + 1], hidden[k : k + 1], scalars)
        store_rows(out_ref, ROWS * k, grad[HALF * k : HALF * (k + 1)], tail)


def arrived(in_ref, first):
    rows = slice(first, first + ROWS)
    acc = [in_ref[c, rows, :].astype(F32) for c in range(4)]
    for c in range(4, OWNERS):
        acc[c % 4] = acc[c % 4] + in_ref[c, rows, :].astype(F32)
    acc = (acc[0] + acc[1]) + (acc[2] + acc[3])
    tail = combined(acc[:, HIDDEN:WIDE])
    scalars = [tail[1:2, FIRST + 3 * i : FIRST + 3 * i + 1] for i in range(SCALARS)]
    return acc[:, 0:HIDDEN], tail, scalars


def lanes_of(values):
    lane = iota((8, TAIL), 1)
    out = jnp.zeros((8, TAIL), F32)
    for i, value in enumerate(values):
        out = jnp.where(lane == i, value, out)
    return out


def first_own_kernel(in_ref, vec_ref, res_ref, ones_ref, vec_out_ref, copies_ref):
    energy, energy_tail, scalars = arrived(in_ref, 0)
    ones, ones_tail, _ = arrived(in_ref, ROWS)
    mean = scalars[0] / TOTAL
    res_ref[:, 0:HIDDEN] = energy - mean * ones
    res_ref[:, HIDDEN:WIDE] = energy_tail - mean * ones_tail
    ones_ref[:, 0:HIDDEN] = ones
    ones_ref[:, HIDDEN:WIDE] = ones_tail
    mask, raw = vec_ref[0:1, :], vec_ref[1:2, :]
    vec_out_ref[0:1, :] = mask
    vec_out_ref[1:2, :] = raw - mean * mask
    vec_out_ref[2:8, :] = jnp.zeros((6, SLOTS), F32)
    store_copies(copies_ref, res_ref[...], ones)


def push_kernel(in_ref, st0_ref, half0_ref, tt0_ref, st1_ref, half1_ref, tt1_ref, parts_ref, small_ref, rows_ref, tail_ref):
    for c in range(OWNERS):
        block = in_ref[c].astype(F32)
        rows_ref[ROWS * c : ROWS * (c + 1), :] = block[:, 0:HIDDEN]
        tail_ref[8 * c : 8 * c + ROWS, :] = block[:, HIDDEN:WIDE]
        tail_ref[8 * c + ROWS : 8 * c + 8, :] = block[:, HIDDEN:WIDE]
    lane, row = iota((SITES, TAIL), 1), iota((SITES, TAIL), 0)
    tail = tail_ref[...]
    l, j = iota((TAIL, HIDDEN), 0), iota((TAIL, HIDDEN), 1) & 15
    spread = dot(tail.astype(BF16), jnp.where((l == 8 + j) | (l == 24 + j), 1.0, 0.0).astype(BF16))
    hidden = jnp.sum(jnp.where(own_hidden((SITES, HIDDEN)), spread, 0.0), axis=0, keepdims=True)
    seen = jnp.where((lane < 4) & ((lane & 2) == ((row & 4) >> 1)), tail, 0.0).astype(BF16)
    a, b = iota((16, TAIL), 0), iota((16, TAIL), 1)
    pair = by_lanes(jnp.where((b < 4) & ((b & 1) == a), 1.0, 0.0).astype(BF16), seen)
    small_ref[...] = jnp.zeros((8, HIDDEN), F32)
    small_ref[0:1, :] = hidden * float(CORES)
    small_ref[1:2, 0:SITES] = (pair[0:1, :] + pair[1:2, :]) * float(CORES * REPS)
    mean = total(jnp.where(((row & 7) == 1) & (lane >= FIRST), tail, 0.0))
    rows = jnp.concatenate([rows_ref[...].astype(BF16), row_pair(*two(hidden))], axis=0)
    halves = []
    for st_ref, half_ref, tt_ref in ((st0_ref, half0_ref, tt0_ref), (st1_ref, half1_ref, tt1_ref)):
        mixture = dot(rows, tt_ref[...])
        side = dot(pair.astype(BF16), st_ref[0:SITES, :]) + mixture[HALF:, :]
        values = jnp.sum(mixture[0:HALF, :] * half_ref[...].astype(F32), axis=0, keepdims=True)
        halves.append((values + side[0:1, :] + side[1:2, :]) * (1.0 / TOTAL))
    own = lax.axis_index("chain_2")
    straight, swapped = jnp.concatenate(halves, axis=0), jnp.concatenate(halves[::-1], axis=0)
    extra = jnp.where(iota((2, TAIL), 0) == 0, scalar_lanes((mean,)), 0.0).astype(BF16)
    for core in range(CORES):
        packed = jnp.where(own == core, straight, swapped).astype(BF16)
        for y in range(REPS):
            parts_ref[core * REPS + y, :, 0:OWN_SLOTS] = packed
            parts_ref[core * REPS + y, :, OWN_SLOTS:] = extra


def row_sum(parts_ref, mask):
    values = parts_ref[0].astype(F32)
    for p in range(1, CORES * REPS):
        values = values + parts_ref[p].astype(F32)
    mean = total(values[0:1, OWN_SLOTS:])
    return (jnp.concatenate([values[0:1, 0:OWN_SLOTS], values[1:2, 0:OWN_SLOTS]], axis=1) - mean) * mask


def iteration_scalars(vec_ref, values):
    res, before, o_before, start = (vec_ref[i : i + 1, :] for i in (1, 2, 3, 4))
    return (
        total(res * values),
        total(values * values),
        total(values),
        total(values * o_before),
        total(values * before),
        total(res * o_before),
        total(values * start),
    )


def pull_kernel(parts_ref, vec_ref, st0_ref, half0_ref, tt0_ref, st1_ref, half1_ref, tt1_ref, vec_out_ref, out_ref):
    values = row_sum(parts_ref, vec_ref[0:1, :])
    vec_out_ref[...] = vec_ref[...]
    vec_out_ref[5:6, :] = values
    grad, visible, hidden = pull(values, ((st0_ref, half0_ref, tt0_ref), (st1_ref, half1_ref, tt1_ref)))
    store_rows(out_ref, 0, grad, tail_of(visible, hidden, iteration_scalars(vec_ref, values)))


def conjugate(scalars, past):
    r_zr, zr_zr, zr_sum, zr_zd, zr_d, r_zd, zr_start = scalars[:7]
    if past is None:
        beta, zd_sum, zd_zd, zd_d = None, zr_sum, zr_zr, r_zr
    else:
        rr, sum_before, zz_before, zd_before = past
        beta = r_zr / rr
        zd_sum = zr_sum + beta * sum_before
        zd_zd = zr_zr + 2.0 * beta * zr_zd + beta * beta * zz_before
        zd_d = r_zr + beta * (zr_d + r_zd) + beta * beta * zd_before
    step = r_zr / (zd_zd - zd_sum * zd_sum / TOTAL + SHIFT * zd_d)
    return beta, step, (r_zr, zd_sum, zd_zd, zd_d)


def own_kernel(first, *refs):
    if first:
        in_ref, vec_ref, res_ref, ones_ref, sc_out, vec_out, res_out, dir_out, img_out, copies_ref = refs
    else:
        (in_ref, vec_ref, res_ref, ones_ref, sc_ref, dir_ref, img_ref,
         sc_out, vec_out, res_out, copies_ref) = refs
    grad, tail, scalars = arrived(in_ref, 0)
    past = None if first else tuple(sc_ref[0:1, i : i + 1] for i in range(4))
    beta, step, now = conjugate(scalars, past)
    mean = scalars[2] / TOTAL
    zd_mean = now[1] / TOTAL
    if first:
        kept = (step, now[3])
    else:
        d0_zd1 = scalars[6] + beta * sc_ref[0:1, 5:6]
        kept = (sc_ref[0:1, 4:5], sc_ref[0:1, 5:6], step, now[3], d0_zd1, beta)
    sc_out[...] = lanes_of(now + kept)
    for part, new in ((slice(0, HIDDEN), grad), (slice(HIDDEN, WIDE), tail)):
        image, direction = new - mean * ones_ref[:, part], res_ref[:, part]
        if not first:
            image = image + beta * img_ref[:, part]
            direction = direction + beta * dir_ref[:, part]
        if first:
            img_out[:, part] = image
            dir_out[:, part] = direction
        res_out[:, part] = res_ref[:, part] - step * (image + SHIFT * direction)
    mask, res, o_res = vec_ref[0:1, :], vec_ref[1:2, :], vec_ref[5:6, :]
    direction, o_dir = res, o_res
    if not first:
        direction = direction + beta * vec_ref[2:3, :]
        o_dir = o_dir + beta * vec_ref[3:4, :]
    vec_out[0:1, :] = mask
    vec_out[1:2, :] = res - step * (o_dir - zd_mean * mask + SHIFT * direction)
    vec_out[2:3, :] = direction
    vec_out[3:4, :] = o_dir
    vec_out[4:5, :] = direction if first else vec_ref[4:5, :]
    vec_out[5:8, :] = jnp.zeros((3, SLOTS), F32)
    store_copies(copies_ref, res_out[...], ones_ref[...])


def last_scalars_kernel(parts_ref, vec_ref, out_ref):
    values = row_sum(parts_ref, vec_ref[0:1, :])
    lane = iota((OWNERS, TAIL), 1)
    out = jnp.zeros((OWNERS, TAIL), F32)
    for i, value in enumerate(iteration_scalars(vec_ref, values)):
        out = jnp.where(lane == i, value, out)
    out_ref[...] = out


def last_kernel(in_ref, sc_ref, r0_ref, r1_ref, r2_ref, v0_ref, v1_ref, v2_ref, vis_ref, hid_ref, mat_ref):
    summed = jnp.sum(in_ref[...], axis=0, keepdims=True)
    scalars = [summed[:, i : i + 1] for i in range(SCALARS)]
    keep = [sc_ref[0:1, i : i + 1] for i in range(10)]
    beta2, step2, now = conjugate(scalars, tuple(keep[0:4]))
    step0, d0_zd0, step1, d1_zd1, d0_zd1, beta1 = keep[4:10]
    d0_zd2 = scalars[6] + beta2 * d0_zd1
    d1_zd2 = scalars[4] + beta2 * d1_zd1
    norm = step0 * step0 * d0_zd0 + step1 * step1 * d1_zd1 + step2 * step2 * now[3]
    norm = norm + 2.0 * (step0 * step1 * d0_zd1 + step0 * step2 * d0_zd2 + step1 * step2 * d1_zd2)
    params = float(SITES * HIDDEN * REPS + HIDDEN * REPS + SITES)
    scale = lax.rsqrt(norm / (TOTAL * params) + EPSILON) / TOTAL
    w1 = scale * (step1 + step2 * beta2)
    weights = (scale * step0 + w1 * beta1, w1, scale * step2)
    mat_ref[...] = sum(w * ref[:, 0:HIDDEN] for w, ref in zip(weights, (r0_ref, r1_ref, r2_ref)))
    small = sum(w * ref[...] for w, ref in zip(weights, (v0_ref, v1_ref, v2_ref)))
    hid_ref[...] = small[0]
    a, b = iota((SITES, TAIL), 0), iota((SITES, TAIL), 1)
    pick = jnp.where(a == 32 * lax.axis_index("rep") + b, 1.0, 0.0).astype(F32)
    vis_ref[...] = dot(small[:, 0:SITES], pick, precision=HIGH)[1, 0:32]


def shape(dims, dtype=F32):
    return jax.ShapeDtypeStruct(dims, dtype)


def call(kernel, outs, name, n_in, scratch=()):
    vmem = pl.BlockSpec(memory_space=pltpu.VMEM)
    return pl.pallas_call(
        kernel,
        out_shape=outs,
        in_specs=[vmem] * n_in,
        out_specs=[vmem] * len(outs),
        scratch_shapes=list(scratch),
        name=name,
        compiler_params=pltpu.CompilerParams(vmem_limit_bytes=VMEM_LIMIT),
    )


def exchanged(blocks, axes):
    return lax.all_to_all(blocks, axes, split_axis=0, concat_axis=0, tiled=True)


def in_hbm(*arrays):
    return [pltpu.with_memory_space_constraint(a, pltpu.HBM) for a in arrays]


def per_device(spins, energies, counts, accepted, hidden_bias, weights):
    rows = shape((OWNERS, ROWS, WIDE), BF16)
    own = shape((ROWS, WIDE))
    vec_shape = shape((8, SLOTS))
    st0, turned = call(share_kernel, [shape((SIDE, OWN_SLOTS), BF16), shape((HIDDEN, SIDE), BF16)], "share", 6)(
        counts, *in_hbm(spins, energies, accepted, weights, hidden_bias)
    )
    st1 = lax.ppermute(st0, "chain_2", [(0, 1), (1, 0)])
    half_and_acts = [shape((n, OWN_SLOTS), BF16) for n in (HALF, HIDDEN)]
    half0, tt0 = call(acts_kernel, half_and_acts, "acts", 2)(st0, turned)
    half1, tt1, vec, blocks = call(
        setup_kernel, [*half_and_acts, vec_shape, shape((OWNERS, 2 * ROWS, WIDE), BF16)], "setup", 5
    )(st0, half0, tt0, st1, turned)
    operands = (st0, half0, tt0, st1, half1, tt1)
    res, ones, vec, copies = call(first_own_kernel, [own, own, vec_shape, rows], "first_own", 2)(
        exchanged(blocks, CHIPS), vec
    )

    def push(copies):
        parts, small = call(
            push_kernel, [shape((CORES * REPS, 2, OWN_SLOTS + TAIL), BF16), shape((8, HIDDEN))], "push", 7,
            scratch=[pltpu.VMEM((HALF, HIDDEN), F32), pltpu.VMEM((SITES, TAIL), F32)],
        )(exchanged(copies, CHIPS), *operands)
        return exchanged(parts, UNITS), small

    state, smalls, residuals = (), [], [res]
    for iteration in range(2):
        parts, small = push(copies)
        vec, blocks = call(pull_kernel, [vec_shape, rows], "pull", 8)(parts, vec, *operands)
        first = iteration == 0
        sc, vec, res, *state, copies = call(
            lambda *refs, first=first: own_kernel(first, *refs),
            [shape((8, TAIL)), vec_shape, own, *([own, own] if first else []), rows], "own", 4 + len(state),
        )(exchanged(blocks, CHIPS), vec, res, ones, *state)
        state = (sc, *state)
        smalls.append(small)
        residuals.append(res)
    parts, small = push(copies)
    smalls.append(small)
    (sums,) = call(last_scalars_kernel, [shape((OWNERS, TAIL))], "last_scalars", 2)(parts, vec)
    return call(
        last_kernel, [shape((32,)), shape((HIDDEN,)), shape((ROWS, HIDDEN))], "last", 8
    )(exchanged(sums, CHIPS), sc, *residuals, *smalls)


def solution(mesh):
    split = Mesh(
        mesh.devices.reshape(4, 8, 2, mesh.shape["rep"]), ("chain_0", "chain_1", "chain_2", "rep")
    )
    in_specs = (P(CHAIN, None), P(CHAIN), P(CHAIN), P(CHAIN, None), P("rep"), P(None, "rep"))
    out_specs = (P("rep"), P("rep"), P(CHAIN, "rep"))
    return jax.shard_map(
        per_device, mesh=split, in_specs=in_specs, out_specs=out_specs, check_vma=False
    )
```

```python
import jax
import jax.numpy as jnp
from jax import lax
from jax.experimental import pallas as pl
from jax.experimental.pallas import tpu as pltpu
from jax.sharding import Mesh
from jax.sharding import PartitionSpec as P

KEEP_DEV = 768
SHIFT = 0.05
EPSILON = 1e-06
ENERGY_MID = -110.0
CHAIN = ("chain_0", "chain_1", "chain_2")
CHIPS = ("chain_0", "chain_1")
UNITS = ("chain_2", "rep")
F32 = jnp.float32
BF16 = jnp.bfloat16
HIGH = lax.Precision.HIGHEST

SITES = 256
CORES = 2
REPS = 8
HIDDEN = 512
OWNERS = 32
ROWS = 4
HALF = OWNERS * ROWS
TAIL = 128
WIDE = HIDDEN + TAIL
FIRST = 40
OWN_SLOTS = 1536
SLOTS = CORES * OWN_SLOTS
SIDE = SITES + 16
TOTAL = float(KEEP_DEV * OWNERS * CORES)
SCALARS = 8
VMEM_LIMIT = 24 * 2**20


def iota(shape, dim):
    return lax.broadcasted_iota(jnp.int32, shape, dim)


def dot(a, b, dims=((1,), (0,)), precision=None):
    return lax.dot_general(a, b, (dims, ((), ())), precision=precision, preferred_element_type=F32)


def by_lanes(a, b):
    return dot(a, b, ((1,), (1,)))


def eye(n):
    return jnp.where(iota((n, n), 0) == iota((n, n), 1), 1.0, 0.0).astype(BF16)


def two(x):
    high = x.astype(BF16)
    return high, (x - high.astype(F32)).astype(BF16)


def total(x):
    return jnp.sum(x, keepdims=True)


def scalar_lanes(scalars):
    lane = iota((1, TAIL), 1)
    out = jnp.zeros((1, TAIL), F32)
    for i, value in enumerate(scalars):
        one = value.astype(BF16).astype(F32)
        second = (value - one).astype(BF16).astype(F32)
        third = value - one - second
        for k, piece in enumerate((one, second, third)):
            out = jnp.where(lane == FIRST + 3 * i + k, piece, out)
    return out


def own_hidden(shape):
    row, col = iota(shape, 0), iota(shape, 1)
    return row == 8 * (col >> 4)


def row_pair(high, low):
    sub = iota((16, high.shape[1]), 0)
    return jnp.where(sub == 0, high.astype(F32), jnp.where(sub == 1, low.astype(F32), 0.0)).astype(BF16)


def part_of(core):
    return slice(core * OWN_SLOTS, (core + 1) * OWN_SLOTS)


def pull(weights, operands):
    grad, visible = 0.0, 0.0
    for core, (st_ref, half_ref, tt_ref) in enumerate(operands):
        high, low = two(weights[:, part_of(core)])
        spins = half_ref[...].astype(F32)
        pair = row_pair(high, low)
        rows = [(spins * high.astype(F32)).astype(BF16), (spins * low.astype(F32)).astype(BF16), pair]
        grad = grad + by_lanes(jnp.concatenate(rows, axis=0), tt_ref[...])
        visible = visible + by_lanes(st_ref[0:SITES, :], pair)
    hidden = grad[2 * HALF : 2 * HALF + 1] + grad[2 * HALF + 1 : 2 * HALF + 2]
    return grad[:HALF] + grad[HALF : 2 * HALF], visible[:, 0:1] + visible[:, 1:2], hidden


def tail_of(visible, hidden, scalars):
    v_high = visible.astype(BF16).astype(F32)
    lane, row = iota((SITES, TAIL), 1), iota((SITES, TAIL), 0)
    first = (row & 4) >> 1
    tail = jnp.where(lane == first, v_high, jnp.where(lane == first + 1, visible - v_high, 0.0))
    h_high, h_low = two(hidden)
    mine = own_hidden((SITES, HIDDEN))
    j, l = iota((HIDDEN, TAIL), 0) & 15, iota((HIDDEN, TAIL), 1)
    for piece, base in ((h_high, 8), (h_low, 24)):
        spread = jnp.where(mine, piece.astype(F32), 0.0).astype(BF16)
        tail = tail + dot(spread, jnp.where(l == base + j, 1.0, 0.0).astype(BF16))
    return tail + jnp.where((row & 7) == 1, scalar_lanes(scalars), 0.0)


def store_rows(out_ref, first, grad, tail):
    for c in range(OWNERS):
        near, far = slice(8 * c, 8 * c + ROWS), slice(8 * c + ROWS, 8 * c + 8)
        out_ref[c, first : first + ROWS, 0:HIDDEN] = grad[ROWS * c : ROWS * (c + 1), :].astype(BF16)
        out_ref[c, first : first + ROWS, HIDDEN:WIDE] = (tail[near, :] + tail[far, :]).astype(BF16)


def to_left(x, count):
    return pltpu.roll(x, TAIL - count, 1)


def combined(tail):
    lane = iota((ROWS, TAIL), 1)
    one = to_left(tail, 1)
    second = jnp.where(lane >= FIRST, one + to_left(tail, 2), jnp.where(lane >= 8, to_left(tail, 16), one))
    return tail + second


def store_copies(out_ref, rows, ones):
    lane = iota((ROWS, TAIL), 1)
    tail = rows[:, HIDDEN:WIDE]
    tail = jnp.where((lane == 0) | (lane == 2), tail * (1.0 / (CORES * REPS)), jnp.where((lane >= 8) & (lane < 24), tail * (1.0 / CORES), 0.0))
    high = tail.astype(BF16).astype(F32)
    low = tail - high
    packed = high + jnp.where(lane < 8, pltpu.roll(low, 1, 1), jnp.where(lane >= 24, pltpu.roll(low, 16, 1), 0.0))
    mean = total(rows[:, 0:HIDDEN] * ones[:, 0:HIDDEN]) * (1.0 / (TOTAL * TOTAL))
    packed = packed + jnp.where(iota((ROWS, TAIL), 0) == 1, scalar_lanes((mean,)), 0.0)
    packed = packed.astype(BF16)
    coupling = rows[:, 0:HIDDEN].astype(BF16)
    for c in range(OWNERS):
        out_ref[c, :, 0:HIDDEN] = coupling
        out_ref[c, :, HIDDEN:WIDE] = packed


def share_kernel(
    count_ref, spins_ref, energy_ref, accepted_ref, weights_ref, bias_ref, st_ref, turned_ref
):
    accepted = accepted_ref[...]
    live = iota((16, OWN_SLOTS), 1) < count_ref[...].reshape(1, 1)
    major = jnp.where((iota((16, OWN_SLOTS), 0) == (accepted >> 7)) & live, 1.0, 0.0).astype(BF16)
    minor = jnp.where(iota((TAIL, OWN_SLOTS), 0) == (accepted & 127), 1.0, 0.0).astype(BF16)
    table = by_lanes(major, minor)
    mask = jnp.concatenate([table[h : h + 1, :] for h in range(OWN_SLOTS // TAIL)], axis=1)
    energy = (energy_ref[...].astype(F32).reshape(1, OWN_SLOTS) - ENERGY_MID) * mask
    st_ref[0:SITES, :] = by_lanes(eye(SITES), spins_ref[...]).astype(BF16)
    st_ref[SITES:SIDE, :] = row_pair(energy.astype(BF16), mask.astype(BF16))
    bias_row = jnp.broadcast_to(bias_ref[...].astype(F32).reshape(1, HIDDEN), (16, HIDDEN))
    turned_ref[:, 0:SITES] = by_lanes(eye(HIDDEN), weights_ref[...]).astype(BF16)
    turned_ref[:, SITES:SIDE] = by_lanes(eye(HIDDEN), bias_row.astype(BF16)).astype(BF16)


def acts_kernel(st_ref, turned_ref, half_ref, tt_ref):
    sites = st_ref[0:SITES, :]
    row, site = iota((HALF, SITES), 0), iota((HALF, SITES), 1)
    mine = jnp.where(site == 8 * (row >> 2) + 4 * lax.axis_index("chain_2") + (row & 3), 1.0, 0.0).astype(BF16)
    half_ref[...] = dot(mine, sites).astype(BF16)
    preact = turned_ref[:, SITES : SITES + 1].astype(F32) + dot(turned_ref[:, 0:SITES], sites)
    tt_ref[...] = jnp.tanh(preact).astype(BF16)


def setup_kernel(st0_ref, half0_ref, tt0_ref, st1_ref, turned_ref, half1_ref, tt1_ref, vec_ref, out_ref):
    acts_kernel(st1_ref, turned_ref, half1_ref, tt1_ref)
    vec_ref[...] = jnp.zeros((8, SLOTS), F32)
    grad, visible, sums = 0.0, 0.0, 0.0
    for core, (st_ref, half_ref, tt_ref) in enumerate(((st0_ref, half0_ref, tt0_ref), (st1_ref, half1_ref, tt1_ref))):
        pair = st_ref[SITES:SIDE, :]
        extra = pair.astype(F32)
        energy, mask = extra[0:1, :], extra[1:2, :]
        vec_ref[0:1, part_of(core)] = mask
        vec_ref[1:2, part_of(core)] = energy
        spins = half_ref[...].astype(F32)
        rows = [(spins * energy).astype(BF16), (spins * mask).astype(BF16), pair]
        grad = grad + by_lanes(jnp.concatenate(rows, axis=0), tt_ref[...])
        visible = visible + by_lanes(st_ref[0:SITES, :], pair)
        sums = sums + total(energy)
    hidden = grad[2 * HALF :]
    for k, scalars in enumerate(((sums,), ())):
        tail = tail_of(visible[:, k : k + 1], hidden[k : k + 1], scalars)
        store_rows(out_ref, ROWS * k, grad[HALF * k : HALF * (k + 1)], tail)


def arrived(in_ref, first):
    rows = slice(first, first + ROWS)
    acc = [in_ref[c, rows, :].astype(F32) for c in range(4)]
    for c in range(4, OWNERS):
        acc[c % 4] = acc[c % 4] + in_ref[c, rows, :].astype(F32)
    acc = (acc[0] + acc[1]) + (acc[2] + acc[3])
    tail = combined(acc[:, HIDDEN:WIDE])
    scalars = [tail[1:2, FIRST + 3 * i : FIRST + 3 * i + 1] for i in range(SCALARS)]
    return acc[:, 0:HIDDEN], tail, scalars


def lanes_of(values):
    lane = iota((8, TAIL), 1)
    out = jnp.zeros((8, TAIL), F32)
    for i, value in enumerate(values):
        out = jnp.where(lane == i, value, out)
    return out


def first_own_kernel(in_ref, vec_ref, res_ref, ones_ref, vec_out_ref, copies_ref):
    energy, energy_tail, scalars = arrived(in_ref, 0)
    ones, ones_tail, _ = arrived(in_ref, ROWS)
    mean = scalars[0] / TOTAL
    res_ref[:, 0:HIDDEN] = energy - mean * ones
    res_ref[:, HIDDEN:WIDE] = energy_tail - mean * ones_tail
    ones_ref[:, 0:HIDDEN] = ones
    ones_ref[:, HIDDEN:WIDE] = ones_tail
    mask, raw = vec_ref[0:1, :], vec_ref[1:2, :]
    vec_out_ref[0:1, :] = mask
    vec_out_ref[1:2, :] = raw - mean * mask
    vec_out_ref[2:8, :] = jnp.zeros((6, SLOTS), F32)
    store_copies(copies_ref, res_ref[...], ones)


def push_kernel(in_ref, st0_ref, half0_ref, tt0_ref, st1_ref, half1_ref, tt1_ref, parts_ref, small_ref, rows_ref, tail_ref):
    for c in range(OWNERS):
        block = in_ref[c].astype(F32)
        rows_ref[ROWS * c : ROWS * (c + 1), :] = block[:, 0:HIDDEN]
        tail_ref[8 * c : 8 * c + ROWS, :] = block[:, HIDDEN:WIDE]
        tail_ref[8 * c + ROWS : 8 * c + 8, :] = block[:, HIDDEN:WIDE]
    lane, row = iota((SITES, TAIL), 1), iota((SITES, TAIL), 0)
    tail = tail_ref[...]
    l, j = iota((TAIL, HIDDEN), 0), iota((TAIL, HIDDEN), 1) & 15
    spread = dot(tail.astype(BF16), jnp.where((l == 8 + j) | (l == 24 + j), 1.0, 0.0).astype(BF16))
    hidden = jnp.sum(jnp.where(own_hidden((SITES, HIDDEN)), spread, 0.0), axis=0, keepdims=True)
    seen = jnp.where((lane < 4) & ((lane & 2) == ((row & 4) >> 1)), tail, 0.0).astype(BF16)
    a, b = iota((16, TAIL), 0), iota((16, TAIL), 1)
    pair = by_lanes(jnp.where((b < 4) & ((b & 1) == a), 1.0, 0.0).astype(BF16), seen)
    small_ref[...] = jnp.zeros((8, HIDDEN), F32)
    small_ref[0:1, :] = hidden * float(CORES)
    small_ref[1:2, 0:SITES] = (pair[0:1, :] + pair[1:2, :]) * float(CORES * REPS)
    mean = total(jnp.where(((row & 7) == 1) & (lane >= FIRST), tail, 0.0))
    rows = jnp.concatenate([rows_ref[...].astype(BF16), row_pair(*two(hidden))], axis=0)
    halves = []
    for st_ref, half_ref, tt_ref in ((st0_ref, half0_ref, tt0_ref), (st1_ref, half1_ref, tt1_ref)):
        mixture = dot(rows, tt_ref[...])
        side = dot(pair.astype(BF16), st_ref[0:SITES, :]) + mixture[HALF:, :]
        values = jnp.sum(mixture[0:HALF, :] * half_ref[...].astype(F32), axis=0, keepdims=True)
        halves.append((values + side[0:1, :] + side[1:2, :]) * (1.0 / TOTAL) - mean)
    own = lax.axis_index("chain_2")
    straight, swapped = jnp.concatenate(halves, axis=0), jnp.concatenate(halves[::-1], axis=0)
    for core in range(CORES):
        packed = jnp.where(own == core, straight, swapped).astype(BF16)
        for y in range(REPS):
            parts_ref[core * REPS + y] = packed


def row_sum(parts_ref, mask):
    values = parts_ref[0].astype(F32)
    for p in range(1, CORES * REPS):
        values = values + parts_ref[p].astype(F32)
    return jnp.concatenate([values[0:1, :], values[1:2, :]], axis=1) * mask


def iteration_scalars(vec_ref, values):
    res, before, o_before, start = (vec_ref[i : i + 1, :] for i in (1, 2, 3, 4))
    return (
        total(res * values),
        total(values * values),
        total(values),
        total(values * o_before),
        total(values * before),
        total(res * o_before),
        total(values * start),
    )


def pull_kernel(parts_ref, vec_ref, st0_ref, half0_ref, tt0_ref, st1_ref, half1_ref, tt1_ref, vec_out_ref, out_ref):
    values = row_sum(parts_ref, vec_ref[0:1, :])
    vec_out_ref[...] = vec_ref[...]
    vec_out_ref[5:6, :] = values
    grad, visible, hidden = pull(values, ((st0_ref, half0_ref, tt0_ref), (st1_ref, half1_ref, tt1_ref)))
    store_rows(out_ref, 0, grad, tail_of(visible, hidden, iteration_scalars(vec_ref, values)))


def conjugate(scalars, past):
    r_zr, zr_zr, zr_sum, zr_zd, zr_d, r_zd, zr_start = scalars[:7]
    if past is None:
        beta, zd_sum, zd_zd, zd_d = None, zr_sum, zr_zr, r_zr
    else:
        rr, sum_before, zz_before, zd_before = past
        beta = r_zr / rr
        zd_sum = zr_sum + beta * sum_before
        zd_zd = zr_zr + 2.0 * beta * zr_zd + beta * beta * zz_before
        zd_d = r_zr + beta * (zr_d + r_zd) + beta * beta * zd_before
    step = r_zr / (zd_zd - zd_sum * zd_sum / TOTAL + SHIFT * zd_d)
    return beta, step, (r_zr, zd_sum, zd_zd, zd_d)


def own_kernel(first, *refs):
    if first:
        in_ref, vec_ref, res_ref, ones_ref, sc_out, vec_out, res_out, dir_out, img_out, copies_ref = refs
    else:
        (in_ref, vec_ref, res_ref, ones_ref, sc_ref, dir_ref, img_ref,
         sc_out, vec_out, res_out, copies_ref) = refs
    grad, tail, scalars = arrived(in_ref, 0)
    past = None if first else tuple(sc_ref[0:1, i : i + 1] for i in range(4))
    beta, step, now = conjugate(scalars, past)
    mean = scalars[2] / TOTAL
    zd_mean = now[1] / TOTAL
    if first:
        kept = (step, now[3])
    else:
        d0_zd1 = scalars[6] + beta * sc_ref[0:1, 5:6]
        kept = (sc_ref[0:1, 4:5], sc_ref[0:1, 5:6], step, now[3], d0_zd1, beta)
    sc_out[...] = lanes_of(now + kept)
    for part, new in ((slice(0, HIDDEN), grad), (slice(HIDDEN, WIDE), tail)):
        image, direction = new - mean * ones_ref[:, part], res_ref[:, part]
        if not first:
            image = image + beta * img_ref[:, part]
            direction = direction + beta * dir_ref[:, part]
        if first:
            img_out[:, part] = image
            dir_out[:, part] = direction
        res_out[:, part] = res_ref[:, part] - step * (image + SHIFT * direction)
    mask, res, o_res = vec_ref[0:1, :], vec_ref[1:2, :], vec_ref[5:6, :]
    direction, o_dir = res, o_res
    if not first:
        direction = direction + beta * vec_ref[2:3, :]
        o_dir = o_dir + beta * vec_ref[3:4, :]
    vec_out[0:1, :] = mask
    vec_out[1:2, :] = res - step * (o_dir - zd_mean * mask + SHIFT * direction)
    vec_out[2:3, :] = direction
    vec_out[3:4, :] = o_dir
    vec_out[4:5, :] = direction if first else vec_ref[4:5, :]
    vec_out[5:8, :] = jnp.zeros((3, SLOTS), F32)
    store_copies(copies_ref, res_out[...], ones_ref[...])


def last_scalars_kernel(parts_ref, vec_ref, out_ref):
    values = row_sum(parts_ref, vec_ref[0:1, :])
    lane = iota((OWNERS, TAIL), 1)
    out = jnp.zeros((OWNERS, TAIL), F32)
    for i, value in enumerate(iteration_scalars(vec_ref, values)):
        out = jnp.where(lane == i, value, out)
    out_ref[...] = out


def last_kernel(in_ref, sc_ref, r0_ref, r1_ref, r2_ref, v0_ref, v1_ref, v2_ref, vis_ref, hid_ref, mat_ref):
    summed = jnp.sum(in_ref[...], axis=0, keepdims=True)
    scalars = [summed[:, i : i + 1] for i in range(SCALARS)]
    keep = [sc_ref[0:1, i : i + 1] for i in range(10)]
    beta2, step2, now = conjugate(scalars, tuple(keep[0:4]))
    step0, d0_zd0, step1, d1_zd1, d0_zd1, beta1 = keep[4:10]
    d0_zd2 = scalars[6] + beta2 * d0_zd1
    d1_zd2 = scalars[4] + beta2 * d1_zd1
    norm = step0 * step0 * d0_zd0 + step1 * step1 * d1_zd1 + step2 * step2 * now[3]
    norm = norm + 2.0 * (step0 * step1 * d0_zd1 + step0 * step2 * d0_zd2 + step1 * step2 * d1_zd2)
    params = float(SITES * HIDDEN * REPS + HIDDEN * REPS + SITES)
    scale = lax.rsqrt(norm / (TOTAL * params) + EPSILON) / TOTAL
    w1 = scale * (step1 + step2 * beta2)
    weights = (scale * step0 + w1 * beta1, w1, scale * step2)
    mat_ref[...] = sum(w * ref[:, 0:HIDDEN] for w, ref in zip(weights, (r0_ref, r1_ref, r2_ref)))
    small = sum(w * ref[...] for w, ref in zip(weights, (v0_ref, v1_ref, v2_ref)))
    hid_ref[...] = small[0]
    a, b = iota((SITES, TAIL), 0), iota((SITES, TAIL), 1)
    pick = jnp.where(a == 32 * lax.axis_index("rep") + b, 1.0, 0.0).astype(F32)
    vis_ref[...] = dot(small[:, 0:SITES], pick, precision=HIGH)[1, 0:32]


def shape(dims, dtype=F32):
    return jax.ShapeDtypeStruct(dims, dtype)


def call(kernel, outs, name, n_in, scratch=()):
    vmem = pl.BlockSpec(memory_space=pltpu.VMEM)
    return pl.pallas_call(
        kernel,
        out_shape=outs,
        in_specs=[vmem] * n_in,
        out_specs=[vmem] * len(outs),
        scratch_shapes=list(scratch),
        name=name,
        compiler_params=pltpu.CompilerParams(vmem_limit_bytes=VMEM_LIMIT),
    )


def exchanged(blocks, axes):
    return lax.all_to_all(blocks, axes, split_axis=0, concat_axis=0, tiled=True)


def in_hbm(*arrays):
    return [pltpu.with_memory_space_constraint(a, pltpu.HBM) for a in arrays]


def per_device(spins, energies, counts, accepted, hidden_bias, weights):
    rows = shape((OWNERS, ROWS, WIDE), BF16)
    own = shape((ROWS, WIDE))
    vec_shape = shape((8, SLOTS))
    st0, turned = call(share_kernel, [shape((SIDE, OWN_SLOTS), BF16), shape((HIDDEN, SIDE), BF16)], "share", 6)(
        counts, *in_hbm(spins, energies, accepted, weights, hidden_bias)
    )
    st1 = lax.ppermute(st0, "chain_2", [(0, 1), (1, 0)])
    half_and_acts = [shape((n, OWN_SLOTS), BF16) for n in (HALF, HIDDEN)]
    half0, tt0 = call(acts_kernel, half_and_acts, "acts", 2)(st0, turned)
    half1, tt1, vec, blocks = call(
        setup_kernel, [*half_and_acts, vec_shape, shape((OWNERS, 2 * ROWS, WIDE), BF16)], "setup", 5
    )(st0, half0, tt0, st1, turned)
    operands = (st0, half0, tt0, st1, half1, tt1)
    res, ones, vec, copies = call(first_own_kernel, [own, own, vec_shape, rows], "first_own", 2)(
        exchanged(blocks, CHIPS), vec
    )

    def push(copies):
        parts, small = call(
            push_kernel, [shape((CORES * REPS, 2, OWN_SLOTS), BF16), shape((8, HIDDEN))], "push", 7,
            scratch=[pltpu.VMEM((HALF, HIDDEN), F32), pltpu.VMEM((SITES, TAIL), F32)],
        )(exchanged(copies, CHIPS), *operands)
        return exchanged(parts, UNITS), small

    state, smalls, residuals = (), [], [res]
    for iteration in range(2):
        parts, small = push(copies)
        vec, blocks = call(pull_kernel, [vec_shape, rows], "pull", 8)(parts, vec, *operands)
        first = iteration == 0
        sc, vec, res, *state, copies = call(
            lambda *refs, first=first: own_kernel(first, *refs),
            [shape((8, TAIL)), vec_shape, own, *([own, own] if first else []), rows], "own", 4 + len(state),
        )(exchanged(blocks, CHIPS), vec, res, ones, *state)
        state = (sc, *state)
        smalls.append(small)
        residuals.append(res)
    parts, small = push(copies)
    smalls.append(small)
    (sums,) = call(last_scalars_kernel, [shape((OWNERS, TAIL))], "last_scalars", 2)(parts, vec)
    return call(
        last_kernel, [shape((32,)), shape((HIDDEN,)), shape((ROWS, HIDDEN))], "last", 8
    )(exchanged(sums, CHIPS), sc, *residuals, *smalls)


def solution(mesh):
    split = Mesh(
        mesh.devices.reshape(4, 8, 2, mesh.shape["rep"]), ("chain_0", "chain_1", "chain_2", "rep")
    )
    in_specs = (P(CHAIN, None), P(CHAIN), P(CHAIN), P(CHAIN, None), P("rep"), P(None, "rep"))
    out_specs = (P("rep"), P("rep"), P(CHAIN, "rep"))
    return jax.shard_map(
        per_device, mesh=split, in_specs=in_specs, out_specs=out_specs, check_vma=False
    )
```
